32 devices in a mesh: gx: 8 (over z, core), gy: 4 (over y, x).
Axes of the slice: x: 2, y: 2, z: 4, core: 2. Of those that a mesh axis runs over, the one named last changes fastest.
Arguments:
- velocity: float32 [3, 32, 32, 128], P(None, 'gx', 'gy'), may hold values from -4 to 4
- forcing: float32 [3, 32, 32, 128], P(None, 'gx', 'gy'), may hold values from -6 to 6
- viscosity: float32 [32, 32, 128], P('gx', 'gy'), may hold values from 0.05 to 0.5
- residual_prev: float32 [3, 32, 32, 128], P(None, 'gx', 'gy'), may hold values from -4 to 4
- value_prev: float32 [3, 32, 32, 128], P(None, 'gx', 'gy'), may hold values from -4 to 4
- hist_res: float32 [5, 3, 32, 32, 128], P(None, None, 'gx', 'gy'), may hold values from -16 to 16
- hist_val: float32 [5, 3, 32, 32, 128], P(None, None, 'gx', 'gy'), may hold values from -4 to 4
Outputs:
- velocity_out: float32 [3, 32, 32, 128], P(None, 'gx', 'gy')
- residual_out: float32 [3, 32, 32, 128], P(None, 'gx', 'gy')
The draws below stay inside these ranges and needn't reach their ends.
All inputs are finite; a program needn't handle non-finite values.
Results may differ from the reference program's by a relative error of at most 0.0003.
Values sent between devices are 32-bit elements; how exact they have to be, the bound alone decides.
A program may use at most 64 MiB of HBM per device.

```python
import math
import jax
import jax.numpy as jnp
from jax import lax

CX = 4
CY = 8
NZ = 128
M = 5
SWEEPS = 3
ITERS = 2
NX = 32
NY = 32


def shared_forcing(key):
    base = jax.random.truncated_normal(jax.random.fold_in(key, 7), -5.0, 5.0, (3, NX, NY, NZ), jnp.float32)
    return base


def draw_forcing(key, part):
    return shared_forcing(key)


def draw_hist_res(key, part):
    forcing = shared_forcing(key)
    keys = jax.random.split(jax.random.fold_in(key, 11), 4)
    magnitude = jax.random.uniform(keys[0], (M,), jnp.float32, 0.4, 1.0)
    signs = jnp.where(jax.random.bernoulli(keys[1], 0.5, (M,)), 1.0, -1.0)
    coef = magnitude * signs
    blocks = jnp.exp(jax.random.uniform(keys[2], (M, 1, NX // CX, 1, NY // CY, 1, 1), jnp.float32, math.log(0.25), math.log(4.0)))
    noise = jax.random.truncated_normal(keys[3], -5.0, 5.0, (M, 3, NX, NY, NZ), jnp.float32)
    noise = (noise.reshape(M, 3, NX // CX, CX, NY // CY, CY, NZ) * blocks).reshape(M, 3, NX, NY, NZ)
    return coef[:, None, None, None, None] * forcing[None] + 0.5 * noise


def shard_levels(rng, extent, pieces, smallest, high):
    loudness = 1.0
    for dim, blocks in pieces:
        draws = jax.random.uniform(jax.random.fold_in(jax.random.fold_in(rng, 6), dim), (blocks,), jnp.float32, smallest / len(pieces), high / len(pieces))
        loudness = loudness * jnp.repeat(jnp.exp(draws), extent[dim] // blocks).reshape((-1,) + (1,) * (len(extent) - 1 - dim))
    return loudness


def centred(key, extent, deviation, limit, pieces=(), kind=jnp.bfloat16):
    result = jax.random.normal(key, extent, jnp.float32) * deviation
    if len(pieces) > 0:
        result = shard_levels(key, extent, pieces, -0.22, 0.18) * result
    return jnp.clip(result, min=-limit, max=limit).astype(kind)


def setup_inputs(seed: int = 0) -> dict:
    seeds = jax.random.split(jax.random.key(seed), 8)
    return {
        "velocity": centred(seeds[0], (3, NX, NY, NZ), 0.5, 4.0, ((1, 8), (2, 4)), jnp.float32),
        "forcing": draw_forcing(jax.random.fold_in(seeds[7], 71), 0),
        "viscosity": jnp.clip(jnp.exp(math.log(0.5) - 2.3025851 * jax.random.uniform(seeds[2], (NX, NY, NZ), jnp.float32) ** shard_levels(seeds[2], (NX, NY, NZ), ((0, 8), (1, 4)), -0.2, 0.2)), 0.05, 0.5),
        "residual_prev": centred(seeds[3], (3, NX, NY, NZ), 0.5, 4.0, ((1, 8), (2, 4)), jnp.float32),
        "value_prev": centred(seeds[4], (3, NX, NY, NZ), 0.5, 4.0, ((1, 8), (2, 4)), jnp.float32),
        "hist_res": draw_hist_res(jax.random.fold_in(seeds[7], 71), 0),
        "hist_val": centred(seeds[6], (M, 3, NX, NY, NZ), 0.5, 4.0, ((2, 8), (3, 4)), jnp.float32),
    }


REG = 0.05
FLOOR = 0.001

def relax(wide, vel, forcing, visc):
    deep = jnp.pad(wide, ((0, 0), (0, 0), (0, 0), (1, 1)))
    west = deep[:, :-2, 1:-1, 1:-1]
    east = deep[:, 2:, 1:-1, 1:-1]
    south = deep[:, 1:-1, :-2, 1:-1]
    north = deep[:, 1:-1, 2:, 1:-1]
    below = deep[:, 1:-1, 1:-1, :-2]
    above = deep[:, 1:-1, 1:-1, 2:]
    upward = jnp.maximum(vel, 0.0)
    downward = jnp.minimum(vel, 0.0)
    diag = 1.0 + 6.0 * visc + jnp.sum(jnp.abs(vel), axis=0)
    total = forcing + vel + visc * (west + east + south + north + below + above)
    total = total + upward[0] * west - downward[0] * east
    total = total + upward[1] * south - downward[1] * north
    total = total + upward[2] * below - downward[2] * above
    return total / diag

def picard(field, forcing, visc):
    state = field
    for sweep in range(SWEEPS):
        state = relax(jnp.pad(state, ((0, 0), (1, 1), (1, 1), (0, 0))), field, forcing, visc)
    return state

def reference(velocity, forcing, viscosity, residual_prev, value_prev, hist_res, hist_val):
    entries = 3.0 * NX * NY * NZ
    field = velocity
    res_last = residual_prev
    val_last = value_prev
    hist_f = hist_res
    hist_g = hist_val
    for step in range(ITERS):
        value = picard(field, forcing, viscosity)
        resid = value - field
        flat = hist_f.reshape(M, -1)
        gram = jnp.dot(flat, flat.T, precision=lax.Precision.HIGHEST)
        rhs = jnp.dot(flat, resid.reshape(-1), precision=lax.Precision.HIGHEST)
        shift = REG * jnp.trace(gram) / M + FLOOR * entries
        gamma = jnp.linalg.solve(gram + shift * jnp.eye(M, dtype=jnp.float32), rhs)
        field = value - jnp.tensordot(gamma, hist_g, axes=1, precision=lax.Precision.HIGHEST)
        hist_f = jnp.concatenate([hist_f[1:], (resid - res_last)[None]], 0)
        hist_g = jnp.concatenate([hist_g[1:], (value - val_last)[None]], 0)
        res_last = resid
        val_last = value
    return (field, res_last)
```

```python
import functools

import jax
import jax.numpy as jnp
from jax import lax
from jax.experimental import pallas as pl
from jax.experimental.pallas import tpu as pltpu
from jax.sharding import PartitionSpec as P

SWEEPS = 3
REG = 0.05
FLOOR = 0.001
MESH = pl.DeviceIdType.MESH
DIRS = ((-1, 0), (1, 0), (0, -1), (0, 1), (-1, -1), (-1, 1), (1, -1), (1, 1))
HALO = SWEEPS


def both(a, b):
    return jnp.logical_and(a, b)


def kernel(
    counts,
    direct,
    entries,
    vel_hbm, forc_hbm, visc_hbm, rp_hbm, gp_hbm, hres_hbm, hval_hbm,
    out_ref, res_ref,
    wide, static, hist, late, ahead, past_res, past_val, coef, first, second, fres, delta,
    slots_y, slots_x, slots_all, ruler,
    in_sem, send_sem, recv_sem, ysend, yrecv, xsend, xrecv, asend, arecv, gate,
):
    depth, _, cells_x, cells_y, lanes = hres_hbm.shape
    count_x, count_y = counts
    me_x, me_y = lax.axis_index("gx"), lax.axis_index("gy")
    rows = 2 * cells_y

    def exists(sx, sy):
        ok = None
        for step, me, count in ((sx, me_x, count_x), (sy, me_y, count_y)):
            if step != 0:
                here = me > 0 if step < 0 else me < count - 1
                ok = here if ok is None else both(ok, here)
        return ok

    loads = [
        pltpu.make_async_copy(vel_hbm, wide.at[:, HALO : HALO + cells_x, 0:cells_y], in_sem.at[0]),
        pltpu.make_async_copy(forc_hbm, static.at[0:3, 2 : 2 + cells_x, 0:cells_y], in_sem.at[1]),
        pltpu.make_async_copy(visc_hbm, static.at[3, 2 : 2 + cells_x, 0:cells_y], in_sem.at[2]),
        pltpu.make_async_copy(hval_hbm, hist.at[:, :, HALO : HALO + cells_x, 0:cells_y], in_sem.at[3]),
        pltpu.make_async_copy(hres_hbm, fres, in_sem.at[4]),
        pltpu.make_async_copy(rp_hbm, past_res, in_sem.at[5]),
        pltpu.make_async_copy(gp_hbm, past_val, in_sem.at[6]),
    ]
    barrier = pltpu.get_barrier_semaphore()
    for k in range(1, count_y):
        pl.semaphore_signal(
            barrier, inc=1, device_id=(me_x, lax.rem(me_y + k, count_y)), device_id_type=MESH
        )
    for k in range(1, count_x):
        pl.semaphore_signal(
            barrier, inc=1, device_id=(lax.rem(me_x + k, count_x), me_y), device_id_type=MESH
        )
    total = jnp.int32(count_x + count_y - 2)
    for sx, sy in DIRS[4:]:
        here = exists(sx, sy)
        total = total + jnp.where(here, 1, 0)

        @pl.when(here)
        def _():
            pl.semaphore_signal(
                barrier, inc=1, device_id=(me_x + sx, me_y + sy), device_id_type=MESH
            )

    for load in loads:
        load.start()

    def clear(ref, off):
        lead = (slice(None),) * (len(ref.shape) - 3)
        for (sx, sy), part in (
            ((-1, 0), (slice(0, off), slice(None))),
            ((1, 0), (slice(off + cells_x, 2 * off + cells_x), slice(None))),
            ((0, -1), (slice(None), slice(rows - off, rows))),
            ((0, 1), (slice(None), slice(cells_y, cells_y + off))),
        ):

            @pl.when(jnp.logical_not(exists(sx, sy)))
            def _():
                where = lead + part
                ref[where] = jnp.zeros(ref.at[where].shape, jnp.float32)

    clear(wide, HALO)
    clear(static, HALO - 1)
    pl.semaphore_wait(barrier, total)

    def halo(ref, which, d, off):
        sx, sy = DIRS[d]
        wide_by = off if sx == 0 or sy == 0 else off - 1
        if sx == 0:
            src_x = dst_x = slice(off, off + cells_x)
        elif sx < 0:
            src_x = slice(off, off + wide_by)
            dst_x = slice(off + cells_x, off + cells_x + wide_by)
        else:
            src_x = slice(off + cells_x - wide_by, off + cells_x)
            dst_x = slice(off - wide_by, off)
        if sy == 0:
            src_y = dst_y = slice(0, cells_y)
        elif sy < 0:
            src_y = slice(0, wide_by)
            dst_y = slice(cells_y, cells_y + wide_by)
        else:
            src_y = slice(cells_y - wide_by, cells_y)
            dst_y = slice(rows - wide_by, rows)
        lead = (slice(None),) * (len(ref.shape) - 3)
        return pltpu.make_async_remote_copy(
            src_ref=ref.at[lead + (src_x, src_y)],
            dst_ref=ref.at[lead + (dst_x, dst_y)],
            send_sem=send_sem.at[which],
            recv_sem=recv_sem.at[which],
            device_id=(me_x + sx, me_y + sy),
            device_id_type=MESH,
        )

    fields = ((wide, 0, HALO), (static, 1, HALO - 1), (hist, 2, HALO), (late, 3, HALO))

    def send(field):
        ref, which, off = field
        for d, (sx, sy) in enumerate(DIRS):

            @pl.when(exists(sx, sy))
            def _():
                halo(ref, which, d, off).start()

    def places(me, count):
        inner = both(me > 0, me < count - 1)
        if count == 1:
            return [((0, 0), None)]
        ends = [((0, 1), me == 0), ((1, 0), me == count - 1)]
        return ends + [((1, 1), inner)] if count > 2 else ends

    def moved(field, act):
        ref, which, off = field
        lead = 1
        for extent in ref.shape[:-3]:
            lead = lead * extent
        for sides_x, here_x in places(me_x, count_x):
            for sides_y, here_y in places(me_y, count_y):
                size = 0
                for sx, sy in DIRS:
                    deep = off if sx == 0 or sy == 0 else off - 1
                    part = lead * (cells_x if sx == 0 else deep) * (cells_y if sy == 0 else deep)
                    for step, sides in ((sx, sides_x), (sy, sides_y)):
                        part = part * (sides[(step + 1) // 2] if step != 0 else 1)
                    size = size + part
                if size == 0:
                    continue
                rows_all = ruler.at[0:size]
                copy = pltpu.make_async_remote_copy(
                    src_ref=rows_all,
                    dst_ref=rows_all,
                    send_sem=send_sem.at[which],
                    recv_sem=recv_sem.at[which],
                    device_id={"gx": lax.rem(me_x + 1, count_x)},
                    device_id_type=MESH,
                )
                here = [h for h in (here_x, here_y) if h is not None]

                @pl.when(functools.reduce(both, here))
                def _():
                    act(copy)

    def receive(field):
        moved(field, lambda copy: copy.wait_recv())

    def sent(field):
        moved(field, lambda copy: copy.wait_send())

    def along(slots, idx, k, sends, recvs, me, count, axis):
        return pltpu.make_async_remote_copy(
            src_ref=slots.at[idx, me],
            dst_ref=slots.at[idx, me],
            send_sem=sends.at[idx],
            recv_sem=recvs.at[idx],
            device_id={axis: lax.rem(me + k, count)},
            device_id_type=MESH,
        )

    lines = (
        (slots_y, ysend, yrecv, me_y, count_y, "gy"),
        (slots_x, xsend, xrecv, me_x, count_x, "gx"),
    )

    def spread(line, idx, row):
        slots, sends, recvs, me, count, axis = line
        slots[idx, me] = row
        for k in range(1, count):
            along(slots, idx, k, sends, recvs, me, count, axis).start()

    def whole(line, idx):
        slots, sends, recvs, me, count, axis = line
        part = slots.at[idx, 0 : count - 1]
        return pltpu.make_async_remote_copy(
            src_ref=part,
            dst_ref=part,
            send_sem=sends.at[idx],
            recv_sem=recvs.at[idx],
            device_id={axis: lax.rem(me + 1, count)},
            device_id_type=MESH,
        )

    def gather(line, idx):
        slots, sends, recvs, me, count, axis = line
        whole(line, idx).wait_recv()
        total = slots[idx, 0]
        for k in range(1, count):
            total = total + slots[idx, k]
        return total

    def spent(line, idx):
        whole(line, idx).wait_send()

    count_all = count_x * count_y
    me_all = me_x * count_y + me_y

    def straight(k):
        peer = lax.rem(me_all + k, count_all)
        return pltpu.make_async_remote_copy(
            src_ref=slots_all.at[me_all],
            dst_ref=slots_all.at[me_all],
            send_sem=asend,
            recv_sem=arecv,
            device_id=(lax.div(peer, count_y), lax.rem(peer, count_y)),
            device_id_type=MESH,
        )

    def all_straight():
        part = slots_all.at[0 : count_all - 1]
        return pltpu.make_async_remote_copy(
            src_ref=part,
            dst_ref=part,
            send_sem=asend,
            recv_sem=arecv,
            device_id={"gx": lax.rem(me_x + 1, count_x)},
            device_id_type=MESH,
        )

    lane = lax.broadcasted_iota(jnp.int32, (cells_y, lanes), 1)

    def packed(parts):
        row = jnp.zeros((cells_y, lanes), jnp.float32)
        for j, part in enumerate(parts):
            row = jnp.where(lane == j, jnp.sum(part, axis=1, keepdims=True), row)
        return jnp.sum(row, axis=0, keepdims=True)

    def unpacked(row, count):
        return [jnp.broadcast_to(row[:, j : j + 1], (cells_y, lanes)) for j in range(count)]

    own = [(c, x) for c in range(3) for x in range(cells_x)]

    def factored(gram):
        trace = gram[0][0]
        for j in range(1, depth):
            trace = trace + gram[j][j]
        shift = (REG / depth) * trace + FLOOR * entries
        lower = [[None] * depth for _ in range(depth)]
        inverse = [None] * depth
        scaled = [[None] * depth for _ in range(depth)]
        for j in range(depth):
            pivot = gram[j][j] + shift
            for k in range(j):
                pivot = pivot - lower[j][k] * scaled[j][k]
            inverse[j] = 1.0 / pivot
            for i in range(j + 1, depth):
                value = gram[i][j]
                for k in range(j):
                    value = value - scaled[i][k] * lower[j][k]
                scaled[i][j] = value
                lower[i][j] = value * inverse[j]
        return lower, inverse

    def solved(factors, rhs):
        lower, inverse = factors
        part = list(rhs)
        for j in range(depth):
            for i in range(j + 1, depth):
                part[i] = part[i] - lower[i][j] * part[j]
        part = [p * inv for p, inv in zip(part, inverse)]
        for j in reversed(range(depth)):
            for i in range(j):
                part[i] = part[i] - lower[j][i] * part[j]
        return part

    zlane = lax.broadcasted_iota(jnp.int32, (rows, lanes), 1)
    has_below = jnp.where(zlane == 0, 0.0, 1.0)
    has_above = jnp.where(zlane == lanes - 1, 0.0, 1.0)

    def relax(src, dst, off, x, cut):
        cs = [coef[j, x + off][0:cut] for j in range(6)]
        for c in range(3):
            here = src(c, x)
            total = coef[6 + c, x + off][0:cut]
            total = total + cs[0] * src(c, x - 1)[0:cut] + cs[1] * src(c, x + 1)[0:cut]
            total = total + cs[2] * pltpu.roll(here, 1, 0)[0:cut]
            total = total + cs[3] * pltpu.roll(here, rows - 1, 0)[0:cut]
            total = total + cs[4] * pltpu.roll(here[0:cut], 1, 1)
            total = total + cs[5] * pltpu.roll(here[0:cut], lanes - 1, 1)
            dst(c, x, total)

    def picard(field, dst):
        for x in range(-2, cells_x + 2):
            vel = [field[c, x + HALO] for c in range(3)]
            visc = static[3, x + 2]
            diag = 1.0 + 6.0 * visc + jnp.abs(vel[0]) + jnp.abs(vel[1]) + jnp.abs(vel[2])
            inv = 1.0 / diag
            for a in range(3):
                lo = (visc + jnp.maximum(vel[a], 0.0)) * inv
                hi = (visc - jnp.minimum(vel[a], 0.0)) * inv
                if a == 2:
                    lo, hi = lo * has_below, hi * has_above
                coef[2 * a, x + 2] = lo
                coef[2 * a + 1, x + 2] = hi
            for c in range(3):
                coef[6 + c, x + 2] = (static[c, x + 2] + vel[c]) * inv

        def put(ref, off):
            def store(c, x, value):
                ref[c, x + off] = value

            return store

        for x in range(-2, cells_x + 2):
            relax(lambda c, i: field[c, i + HALO], put(first, 2), 2, x, rows)
        for x in range(-1, cells_x + 1):
            relax(lambda c, i: first[c, i + 2], put(second, 1), 2, x, rows)
        for x in range(cells_x):
            relax(lambda c, i: second[c, i + 1], dst, 2, x, cells_y)

    for k in range(1, count_x if direct else 1):
        pl.semaphore_signal(
            gate, inc=1, device_id=(lax.rem(me_x + k, count_x), me_y), device_id_type=MESH
        )

    for load in loads[:3]:
        load.wait()
    send(fields[0])
    send(fields[1])
    loads[3].wait()
    send(fields[2])
    for load in loads[4:]:
        load.wait()

    pairs = [(i, j) for i in range(depth) for j in range(i + 1)]
    clear(hist, HALO)
    clear(late, HALO)
    sums = [None] * (len(pairs) + depth)

    def add(j, value):
        sums[j] = value if sums[j] is None else sums[j] + value

    for c, x in own:
        f = [fres[j, c, x] for j in range(depth)]
        r = past_res[c, x]
        for n, (i, j) in enumerate(pairs):
            add(n, f[i] * f[j])
        for j in range(depth):
            add(len(pairs) + j, f[j] * r)
    spread(lines[1], 0, packed(sums))

    receive(fields[0])
    receive(fields[1])

    def store_value(c, x, value):
        late[c, x + HALO, 0:cells_y] = value

    picard(wide, store_value)

    sums = [None] * (depth + 1)
    for c, x in own:
        resid = late[c, x + HALO, 0:cells_y] - wide[c, x + HALO, 0:cells_y]
        newest = resid - past_res[c, x]
        delta[c, x] = newest
        for j in range(depth):
            add(j, fres[j, c, x] * resid)
        add(depth, newest * newest)
    spread(lines[1], 1, packed(sums))
    send(fields[3])
    spread(lines[0], 0, gather(lines[1], 0))
    spread(lines[0], 1, gather(lines[1], 1))

    early = unpacked(gather(lines[0], 0), len(pairs) + depth)
    gram = [[None] * depth for _ in range(depth)]
    for n, (i, j) in enumerate(pairs):
        gram[i][j] = gram[j][i] = early[n]
    factors = factored(gram)
    receive(fields[2])
    receive(fields[3])
    for_rhs = unpacked(gather(lines[0], 1), depth + 1)
    rhs, newest_sq = for_rhs[:depth], for_rhs[depth]
    gamma = solved(factors, rhs)
    wide_gamma = [jnp.concatenate([g, g], 0) for g in gamma]
    for c in range(3):
        for x in range(cells_x + 2 * HALO):
            value = late[c, x]
            for j in range(depth):
                value = value - wide_gamma[j] * hist[j, c, x]
            ahead[c, x] = value

    def store_out(c, x, value):
        out_ref[c, x] = value

    picard(ahead, store_out)

    sums = [None] * depth
    for c, x in own:
        resid = out_ref[c, x] - ahead[c, x + HALO, 0:cells_y]
        res_ref[c, x] = resid
        for j in range(1, depth):
            add(j - 1, fres[j, c, x] * resid)
        add(depth - 1, delta[c, x] * resid)
    if direct:
        pl.semaphore_wait(gate, count_x - 1)
        slots_all[me_all] = packed(sums)
        for k in range(1, count_all):
            straight(k).start()
    else:
        spread(lines[1], 2, packed(sums))

    gram2 = [[None] * depth for _ in range(depth)]
    for i in range(depth - 1):
        for j in range(depth - 1):
            gram2[i][j] = gram[i + 1][j + 1]
        cross = rhs[i + 1] - early[len(pairs) + i + 1]
        gram2[i][depth - 1] = gram2[depth - 1][i] = cross
    gram2[depth - 1][depth - 1] = newest_sq
    factors = factored(gram2)

    if not direct:
        spread(lines[0], 2, gather(lines[1], 2))
    for field in fields:
        sent(field)
    for line in lines:
        for idx in range(2):
            spent(line, idx)
    if direct:
        all_straight().wait_recv()
        final = jnp.sum(slots_all[...], axis=0)
    else:
        final = gather(lines[0], 2)
    gamma = solved(factors, unpacked(final, depth))
    for c, x in own:
        value = out_ref[c, x]
        newest = late[c, x + HALO, 0:cells_y] - past_val[c, x]
        for j in range(1, depth):
            value = value - gamma[j - 1] * hist[j, c, x + HALO, 0:cells_y]
        out_ref[c, x] = value - gamma[depth - 1] * newest
    if direct:
        all_straight().wait_send()
    else:
        for line in lines:
            spent(line, 2)


def leave(vel_ref, res_ref, vel_hbm, res_hbm, sem):
    copies = [
        pltpu.make_async_copy(vel_ref, vel_hbm, sem.at[0]),
        pltpu.make_async_copy(res_ref, res_hbm, sem.at[1]),
    ]
    for copy in copies:
        copy.start()
    for copy in copies:
        copy.wait()


def local(velocity, forcing, viscosity, residual_prev, value_prev, hist_res, hist_val):
    depth, comps, cells_x, cells_y, lanes = hist_res.shape
    counts = (lax.axis_size("gx"), lax.axis_size("gy"))
    entries = 3.0 * cells_x * cells_y * lanes * counts[0] * counts[1]
    rows = 2 * cells_y
    count_all = counts[0] * counts[1]
    direct = count_all <= 64
    count_all = count_all if direct else 1

    def vmem(*shape):
        return pltpu.VMEM(shape + (lanes,), jnp.float32)

    results = pl.pallas_call(
        functools.partial(kernel, counts, direct, entries),
        name="anderson",
        out_shape=(pltpu.VMEM(velocity.shape, jnp.float32),) * 2,
        in_specs=[pl.BlockSpec(memory_space=pl.ANY)] * 7,
        out_specs=(pl.BlockSpec(memory_space=pltpu.VMEM),) * 2,
        scratch_shapes=[
            vmem(3, cells_x + 6, rows),
            vmem(4, cells_x + 4, rows),
            vmem(depth, 3, cells_x + 6, rows),
            vmem(3, cells_x + 6, rows),
            vmem(3, cells_x + 6, rows),
            vmem(3, cells_x, cells_y),
            vmem(3, cells_x, cells_y),
            vmem(9, cells_x + 4, rows),
            vmem(3, cells_x + 4, rows),
            vmem(3, cells_x + 2, rows),
            vmem(depth, 3, cells_x, cells_y),
            vmem(3, cells_x, cells_y),
            vmem(3, counts[1], 1),
            vmem(3, counts[0], 1),
            vmem(count_all, 1),
            vmem(depth * 3 * (6 * (cells_x + cells_y) + 16), 1),
            pltpu.SemaphoreType.DMA((7,)),
            pltpu.SemaphoreType.DMA((4,)),
            pltpu.SemaphoreType.DMA((4,)),
            pltpu.SemaphoreType.DMA((3,)),
            pltpu.SemaphoreType.DMA((3,)),
            pltpu.SemaphoreType.DMA((3,)),
            pltpu.SemaphoreType.DMA((3,)),
            pltpu.SemaphoreType.DMA,
            pltpu.SemaphoreType.DMA,
            pltpu.SemaphoreType.REGULAR,
        ],
        compiler_params=pltpu.CompilerParams(collective_id=0, has_side_effects=True),
    )(velocity, forcing, viscosity, residual_prev, value_prev, hist_res, hist_val)
    return pl.pallas_call(
        leave,
        name="leave",
        out_shape=(jax.ShapeDtypeStruct(velocity.shape, jnp.float32),) * 2,
        in_specs=[pl.BlockSpec(memory_space=pl.ANY)] * 2,
        out_specs=(pl.BlockSpec(memory_space=pl.ANY),) * 2,
        scratch_shapes=[pltpu.SemaphoreType.DMA((2,))],
    )(*(pltpu.with_memory_space_constraint(r, pltpu.VMEM) for r in results))


def solution(mesh):
    field = P(None, "gx", "gy", None)
    history = P(None, None, "gx", "gy", None)
    return jax.shard_map(
        local,
        mesh=mesh,
        in_specs=(field, field, P("gx", "gy", None), field, field, history, history),
        out_specs=(field, field),
        check_vma=False,
    )
```

```python
import functools

import jax
import jax.numpy as jnp
from jax import lax
from jax.experimental import pallas as pl
from jax.experimental.pallas import tpu as pltpu
from jax.sharding import PartitionSpec as P

SWEEPS = 3
REG = 0.05
FLOOR = 0.001
MESH = pl.DeviceIdType.MESH
DIRS = ((-1, 0), (1, 0), (0, -1), (0, 1), (-1, -1), (-1, 1), (1, -1), (1, 1))
HALO = SWEEPS


def both(a, b):
    return jnp.logical_and(a, b)


def kernel(
    counts,
    direct,
    entries,
    vel_hbm, forc_hbm, visc_hbm, rp_hbm, gp_hbm, hres_hbm, hval_hbm,
    out_ref, res_ref,
    wide, static, hist, late, ahead, past_res, past_val, coef, first, second, fres, delta,
    ruler, in_sem, send_sem, recv_sem, gate, *shared,
):
    depth, _, cells_x, cells_y, lanes = hres_hbm.shape
    count_x, count_y = counts
    me_x, me_y = lax.axis_index("gx"), lax.axis_index("gy")
    rows = 2 * cells_y

    def exists(sx, sy):
        ok = None
        for step, me, count in ((sx, me_x, count_x), (sy, me_y, count_y)):
            if step != 0:
                here = me > 0 if step < 0 else me < count - 1
                ok = here if ok is None else both(ok, here)
        return ok

    loads = [
        pltpu.make_async_copy(vel_hbm, wide.at[:, HALO : HALO + cells_x, 0:cells_y], in_sem.at[0]),
        pltpu.make_async_copy(forc_hbm, static.at[0:3, 2 : 2 + cells_x, 0:cells_y], in_sem.at[1]),
        pltpu.make_async_copy(visc_hbm, static.at[3, 2 : 2 + cells_x, 0:cells_y], in_sem.at[2]),
        pltpu.make_async_copy(hval_hbm, hist.at[:, :, HALO : HALO + cells_x, 0:cells_y], in_sem.at[3]),
        pltpu.make_async_copy(hres_hbm, fres, in_sem.at[4]),
        pltpu.make_async_copy(rp_hbm, past_res, in_sem.at[5]),
        pltpu.make_async_copy(gp_hbm, past_val, in_sem.at[6]),
    ]
    for load in loads:
        load.start()
    barrier = pltpu.get_barrier_semaphore()
    for k in range(1, count_y):
        pl.semaphore_signal(
            barrier, inc=1, device_id=(me_x, lax.rem(me_y + k, count_y)), device_id_type=MESH
        )
    for k in range(1, count_x):
        pl.semaphore_signal(
            barrier, inc=1, device_id=(lax.rem(me_x + k, count_x), me_y), device_id_type=MESH
        )
    total = jnp.int32(count_x + count_y - 2)
    for sx, sy in DIRS[4:]:
        here = exists(sx, sy)
        total = total + jnp.where(here, 1, 0)

        @pl.when(here)
        def _():
            pl.semaphore_signal(
                barrier, inc=1, device_id=(me_x + sx, me_y + sy), device_id_type=MESH
            )

    def clear(ref, off):
        lead = (slice(None),) * (len(ref.shape) - 3)
        for (sx, sy), part in (
            ((-1, 0), (slice(0, off), slice(None))),
            ((1, 0), (slice(off + cells_x, 2 * off + cells_x), slice(None))),
            ((0, -1), (slice(None), slice(rows - off, rows))),
            ((0, 1), (slice(None), slice(cells_y, cells_y + off))),
        ):

            @pl.when(jnp.logical_not(exists(sx, sy)))
            def _():
                where = lead + part
                ref[where] = jnp.zeros(ref.at[where].shape, jnp.float32)

    clear(wide, HALO)
    clear(static, HALO - 1)
    with jax.named_scope("barrier"):
        pl.semaphore_wait(barrier, total)

    def span_x(sx, off, deep, skip=0):
        if sx == 0:
            return (slice(off, off + cells_x),) * 2
        if sx < 0:
            return slice(off + skip, off + deep), slice(off + cells_x + skip, off + cells_x + deep)
        return slice(off + cells_x - deep, off + cells_x - skip), slice(off - deep, off - skip)

    def span_y(sy, deep, skip=0):
        if sy == 0:
            return (slice(0, cells_y),) * 2
        if sy < 0:
            return slice(skip, deep), slice(cells_y + skip, cells_y + deep)
        return slice(cells_y - deep, cells_y - skip), slice(rows - deep, rows - skip)

    def faces(ref, off, dirs):
        pieces = []
        for sx, sy in dirs:
            deep = off if sx == 0 or sy == 0 else off - 1
            pieces.append((ref, (sx, sy), 0, span_x(sx, off, deep), span_y(sy, deep)))
        return pieces

    def layers(ref, off, deep, skip):
        return [(ref, (0, sy), 0, span_x(0, off, 0), span_y(sy, deep, skip)) for sy in (-1, 1)]

    def corners(ref, off):
        deep = off - 1
        pieces = []
        for sx in (-1, 1):
            for side, part in ((1, slice(cells_y, cells_y + deep)), (-1, slice(rows - deep, rows))):
                pieces.append((ref, (sx, 0), side, span_x(sx, off, deep), (part, part)))
        return pieces

    def length(part):
        return part.stop - part.start

    def size_of(piece):
        ref, _, _, (src_x, _), (src_y, _) = piece
        size = length(src_x) * length(src_y)
        for extent in ref.shape[:-3]:
            size = size * extent
        return size

    def places(me, count):
        if count == 1:
            return [((0, 0), None)]
        ends = [((0, 1), me == 0), ((1, 0), me == count - 1)]
        return ends + [((1, 1), both(me > 0, me < count - 1))] if count > 2 else ends

    def settle(pieces, sem, sending, more=0):
        for sides_x, here_x in places(me_x, count_x):
            for sides_y, here_y in places(me_y, count_y):
                size = more
                for piece in pieces:
                    _, (sx, sy), side, _, _ = piece
                    there = 1
                    for step, sides in ((sx, sides_x), (sy, sides_y)):
                        if step != 0:
                            there = there * sides[step > 0 if sending else step < 0]
                    if side != 0:
                        there = there * sides_y[side > 0]
                    size = size + there * size_of(piece)
                if size == 0:
                    continue
                part = ruler.at[0:size]
                copy = pltpu.make_async_remote_copy(
                    src_ref=part,
                    dst_ref=part,
                    send_sem=sem,
                    recv_sem=sem,
                    device_id={"gx": lax.rem(me_x + 1, count_x)},
                    device_id_type=MESH,
                )
                here = [h for h in (here_x, here_y) if h is not None]

                @pl.when(functools.reduce(both, here))
                def _():
                    if sending:
                        copy.wait_send()
                    else:
                        copy.wait_recv()

    fields = {
        "wide": faces(wide, HALO, DIRS),
        "static": faces(static, HALO - 1, DIRS),
        "across": faces(hist, HALO, DIRS[:2]),
        "near": layers(hist, HALO, HALO - 1, 0),
        "far": layers(hist, HALO, HALO, HALO - 1),
        "turn": corners(hist, HALO),
        "late": faces(late, HALO, DIRS),
    }
    places_of = {name: n for n, name in enumerate(fields)}

    def send(name):
        for piece in fields[name]:
            ref, (sx, sy), side, (src_x, dst_x), (src_y, dst_y) = piece
            here = exists(sx, sy)
            if side != 0:
                here = both(here, exists(0, side))
            lead = (slice(None),) * (len(ref.shape) - 3)

            @pl.when(here)
            def _():
                pltpu.make_async_remote_copy(
                    src_ref=ref.at[lead + (src_x, src_y)],
                    dst_ref=ref.at[lead + (dst_x, dst_y)],
                    send_sem=send_sem,
                    recv_sem=recv_sem.at[places_of[name]],
                    device_id=(me_x + sx, me_y + sy),
                    device_id_type=MESH,
                ).start()

    def receive(name):
        with jax.named_scope(name):
            settle(fields[name], recv_sem.at[places_of[name]], False)

    def along(slots, idx, k, sends, recvs, me, count, axis):
        return pltpu.make_async_remote_copy(
            src_ref=slots.at[idx, me],
            dst_ref=slots.at[idx, me],
            send_sem=sends.at[idx],
            recv_sem=recvs.at[idx],
            device_id={axis: lax.rem(me + k, count)},
            device_id_type=MESH,
        )

    count_all = count_x * count_y
    me_all = me_x * count_y + me_y
    if direct:
        slots_all, all_sem = shared
    else:
        slots_y, slots_x, ysend, yrecv, xsend, xrecv = shared
        lines = (
            (slots_y, ysend, yrecv, me_y, count_y, "gy"),
            (slots_x, xsend, xrecv, me_x, count_x, "gx"),
        )

    def spread(line, idx, row):
        slots, sends, recvs, me, count, axis = line
        slots[idx, me] = row
        for k in range(1, count):
            along(slots, idx, k, sends, recvs, me, count, axis).start()

    def whole(line, idx):
        slots, sends, recvs, me, count, axis = line
        part = slots.at[idx, 0 : count - 1]
        return pltpu.make_async_remote_copy(
            src_ref=part,
            dst_ref=part,
            send_sem=sends.at[idx],
            recv_sem=recvs.at[idx],
            device_id={axis: lax.rem(me + 1, count)},
            device_id_type=MESH,
        )

    def gather(line, idx):
        slots, sends, recvs, me, count, axis = line
        whole(line, idx).wait_recv()
        total = slots[idx, 0]
        for k in range(1, count):
            total = total + slots[idx, k]
        return total

    def give(idx, row):
        if not direct:
            spread(lines[1], idx, row)
            return
        slots_all[idx, me_all] = row
        for k in range(1, count_all):
            peer = lax.rem(me_all + k, count_all)
            pltpu.make_async_remote_copy(
                src_ref=slots_all.at[idx, me_all],
                dst_ref=slots_all.at[idx, me_all],
                send_sem=send_sem,
                recv_sem=all_sem.at[idx],
                device_id=(lax.div(peer, count_y), lax.rem(peer, count_y)),
                device_id_type=MESH,
            ).start()

    def halfway(idx):
        if not direct:
            spread(lines[0], idx, gather(lines[1], idx))

    def take(idx):
        if not direct:
            return gather(lines[0], idx)
        part = ruler.at[0 : count_all - 1]
        with jax.named_scope("take" + str(idx)):
            pltpu.make_async_remote_copy(
                src_ref=part,
                dst_ref=part,
                send_sem=all_sem.at[idx],
                recv_sem=all_sem.at[idx],
                device_id={"gx": lax.rem(me_x + 1, count_x)},
                device_id_type=MESH,
            ).wait_recv()
        return jnp.sum(slots_all[idx], axis=0)

    lane = lax.broadcasted_iota(jnp.int32, (cells_y, lanes), 1)

    def packed(parts):
        row = jnp.zeros((cells_y, lanes), jnp.float32)
        for j, part in enumerate(parts):
            row = jnp.where(lane == j, jnp.sum(part, axis=1, keepdims=True), row)
        return jnp.sum(row, axis=0, keepdims=True)

    def unpacked(row, count):
        return [jnp.broadcast_to(row[:, j : j + 1], (cells_y, lanes)) for j in range(count)]

    own = [(c, x) for c in range(3) for x in range(cells_x)]

    def factored(gram):
        trace = gram[0][0]
        for j in range(1, depth):
            trace = trace + gram[j][j]
        shift = (REG / depth) * trace + FLOOR * entries
        lower = [[None] * depth for _ in range(depth)]
        inverse = [None] * depth
        scaled = [[None] * depth for _ in range(depth)]
        for j in range(depth):
            pivot = gram[j][j] + shift
            for k in range(j):
                pivot = pivot - lower[j][k] * scaled[j][k]
            inverse[j] = 1.0 / pivot
            for i in range(j + 1, depth):
                value = gram[i][j]
                for k in range(j):
                    value = value - scaled[i][k] * lower[j][k]
                scaled[i][j] = value
                lower[i][j] = value * inverse[j]
        return lower, inverse

    def solved(factors, rhs):
        lower, inverse = factors
        part = list(rhs)
        for j in range(depth):
            for i in range(j + 1, depth):
                part[i] = part[i] - lower[i][j] * part[j]
        part = [p * inv for p, inv in zip(part, inverse)]
        for j in reversed(range(depth)):
            for i in range(j):
                part[i] = part[i] - lower[j][i] * part[j]
        return part

    zlane = lax.broadcasted_iota(jnp.int32, (rows, lanes), 1)
    has_below = jnp.where(zlane == 0, 0.0, 1.0)
    has_above = jnp.where(zlane == lanes - 1, 0.0, 1.0)

    def relax(src, dst, off, x, cut):
        cs = [coef[j, x + off][0:cut] for j in range(6)]
        for c in range(3):
            here = src(c, x)
            total = coef[6 + c, x + off][0:cut]
            total = total + cs[0] * src(c, x - 1)[0:cut] + cs[1] * src(c, x + 1)[0:cut]
            total = total + cs[2] * pltpu.roll(here, 1, 0)[0:cut]
            total = total + cs[3] * pltpu.roll(here, rows - 1, 0)[0:cut]
            total = total + cs[4] * pltpu.roll(here[0:cut], 1, 1)
            total = total + cs[5] * pltpu.roll(here[0:cut], lanes - 1, 1)
            dst(c, x, total)

    def picard(field, dst):
        for x in range(-2, cells_x + 2):
            vel = [field[c, x + HALO] for c in range(3)]
            visc = static[3, x + 2]
            diag = 1.0 + 6.0 * visc + jnp.abs(vel[0]) + jnp.abs(vel[1]) + jnp.abs(vel[2])
            inv = 1.0 / diag
            for a in range(3):
                lo = (visc + jnp.maximum(vel[a], 0.0)) * inv
                hi = (visc - jnp.minimum(vel[a], 0.0)) * inv
                if a == 2:
                    lo, hi = lo * has_below, hi * has_above
                coef[2 * a, x + 2] = lo
                coef[2 * a + 1, x + 2] = hi
            for c in range(3):
                coef[6 + c, x + 2] = (static[c, x + 2] + vel[c]) * inv

        def put(ref, off):
            def store(c, x, value):
                ref[c, x + off] = value

            return store

        for x in range(-2, cells_x + 2):
            relax(lambda c, i: field[c, i + HALO], put(first, 2), 2, x, rows)
        for x in range(-1, cells_x + 1):
            relax(lambda c, i: first[c, i + 2], put(second, 1), 2, x, rows)
        for x in range(cells_x):
            relax(lambda c, i: second[c, i + 1], dst, 2, x, cells_y)

    for k in range(1, count_x if direct else 1):
        pl.semaphore_signal(
            gate, inc=1, device_id=(lax.rem(me_x + k, count_x), me_y), device_id_type=MESH
        )

    for load in loads[:3]:
        load.wait()
    send("wide")
    send("static")
    loads[3].wait()
    send("near")
    send("far")
    send("across")
    for load in loads[4:]:
        load.wait()

    pairs = [(i, j) for i in range(depth) for j in range(i + 1)]
    clear(hist, HALO)
    clear(late, HALO)
    sums = [None] * (len(pairs) + depth)

    def add(j, value):
        sums[j] = value if sums[j] is None else sums[j] + value

    for c, x in own:
        f = [fres[j, c, x] for j in range(depth)]
        r = past_res[c, x]
        for n, (i, j) in enumerate(pairs):
            add(n, f[i] * f[j])
        for j in range(depth):
            add(len(pairs) + j, f[j] * r)
    row = packed(sums)
    if direct:
        with jax.named_scope("gate"):
            pl.semaphore_wait(gate, count_x - 1)
    give(0, row)

    receive("wide")
    receive("static")

    def store_value(c, x, value):
        late[c, x + HALO, 0:cells_y] = value

    picard(wide, store_value)

    sums = [None] * (depth + 1)
    for c, x in own:
        resid = late[c, x + HALO, 0:cells_y] - wide[c, x + HALO, 0:cells_y]
        newest = resid - past_res[c, x]
        delta[c, x] = newest
        for j in range(depth):
            add(j, fres[j, c, x] * resid)
        add(depth, newest * newest)
    give(1, packed(sums))
    send("late")
    receive("near")
    send("turn")
    halfway(0)
    halfway(1)

    early = unpacked(take(0), len(pairs) + depth)
    gram = [[None] * depth for _ in range(depth)]
    for n, (i, j) in enumerate(pairs):
        gram[i][j] = gram[j][i] = early[n]
    factors = factored(gram)
    for name in ("across", "far", "turn", "late"):
        receive(name)
    for_rhs = unpacked(take(1), depth + 1)
    rhs, newest_sq = for_rhs[:depth], for_rhs[depth]
    gamma = solved(factors, rhs)
    wide_gamma = [jnp.concatenate([g, g], 0) for g in gamma]
    for c in range(3):
        for x in range(cells_x + 2 * HALO):
            value = late[c, x]
            for j in range(depth):
                value = value - wide_gamma[j] * hist[j, c, x]
            ahead[c, x] = value

    def store_out(c, x, value):
        out_ref[c, x] = value

    picard(ahead, store_out)

    sums = [None] * depth
    for c, x in own:
        resid = out_ref[c, x] - ahead[c, x + HALO, 0:cells_y]
        res_ref[c, x] = resid
        for j in range(1, depth):
            add(j - 1, fres[j, c, x] * resid)
        add(depth - 1, delta[c, x] * resid)
    give(2, packed(sums))

    gram2 = [[None] * depth for _ in range(depth)]
    for i in range(depth - 1):
        for j in range(depth - 1):
            gram2[i][j] = gram[i + 1][j + 1]
        cross = rhs[i + 1] - early[len(pairs) + i + 1]
        gram2[i][depth - 1] = gram2[depth - 1][i] = cross
    gram2[depth - 1][depth - 1] = newest_sq
    factors = factored(gram2)

    halfway(2)
    final = take(2)
    gamma = solved(factors, unpacked(final, depth))
    for c, x in own:
        value = out_ref[c, x]
        newest = late[c, x + HALO, 0:cells_y] - past_val[c, x]
        for j in range(1, depth):
            value = value - gamma[j - 1] * hist[j, c, x + HALO, 0:cells_y]
        out_ref[c, x] = value - gamma[depth - 1] * newest
    pieces = [piece for name in fields for piece in fields[name]]
    settle(pieces, send_sem, True, 3 * (count_all - 1) if direct else 0)
    if not direct:
        for line in lines:
            for idx in range(3):
                whole(line, idx).wait_send()


def leave(vel_ref, res_ref, vel_hbm, res_hbm, sem):
    copies = [
        pltpu.make_async_copy(vel_ref, vel_hbm, sem.at[0]),
        pltpu.make_async_copy(res_ref, res_hbm, sem.at[1]),
    ]
    for copy in copies:
        copy.start()
    for copy in copies:
        copy.wait()


def local(velocity, forcing, viscosity, residual_prev, value_prev, hist_res, hist_val):
    depth, comps, cells_x, cells_y, lanes = hist_res.shape
    counts = (lax.axis_size("gx"), lax.axis_size("gy"))
    entries = 3.0 * cells_x * cells_y * lanes * counts[0] * counts[1]
    rows = 2 * cells_y
    count_all = counts[0] * counts[1]
    direct = count_all <= 64
    def vmem(*shape):
        return pltpu.VMEM(shape + (lanes,), jnp.float32)

    if direct:
        shared = [vmem(3, count_all, 1), pltpu.SemaphoreType.DMA((3,))]
    else:
        shared = [vmem(3, counts[1], 1), vmem(3, counts[0], 1)]
        shared += [pltpu.SemaphoreType.DMA((3,))] * 4
    length = 9 * (depth + 3) * (6 * (cells_x + cells_y) + 16) + 3 * count_all
    results = pl.pallas_call(
        functools.partial(kernel, counts, direct, entries),
        name="anderson",
        out_shape=(pltpu.VMEM(velocity.shape, jnp.float32),) * 2,
        in_specs=[pl.BlockSpec(memory_space=pl.ANY)] * 7,
        out_specs=(pl.BlockSpec(memory_space=pltpu.VMEM),) * 2,
        scratch_shapes=[
            vmem(3, cells_x + 6, rows),
            vmem(4, cells_x + 4, rows),
            vmem(depth, 3, cells_x + 6, rows),
            vmem(3, cells_x + 6, rows),
            vmem(3, cells_x + 6, rows),
            vmem(3, cells_x, cells_y),
            vmem(3, cells_x, cells_y),
            vmem(9, cells_x + 4, rows),
            vmem(3, cells_x + 4, rows),
            vmem(3, cells_x + 2, rows),
            vmem(depth, 3, cells_x, cells_y),
            vmem(3, cells_x, cells_y),
            vmem(length, 1),
            pltpu.SemaphoreType.DMA((7,)),
            pltpu.SemaphoreType.DMA,
            pltpu.SemaphoreType.DMA((7,)),
            pltpu.SemaphoreType.REGULAR,
            *shared,
        ],
        compiler_params=pltpu.CompilerParams(collective_id=0, has_side_effects=True),
    )(velocity, forcing, viscosity, residual_prev, value_prev, hist_res, hist_val)
    return pl.pallas_call(
        leave,
        name="leave",
        out_shape=(jax.ShapeDtypeStruct(velocity.shape, jnp.float32),) * 2,
        in_specs=[pl.BlockSpec(memory_space=pl.ANY)] * 2,
        out_specs=(pl.BlockSpec(memory_space=pl.ANY),) * 2,
        scratch_shapes=[pltpu.SemaphoreType.DMA((2,))],
    )(*(pltpu.with_memory_space_constraint(r, pltpu.VMEM) for r in results))


def solution(mesh):
    field = P(None, "gx", "gy", None)
    history = P(None, None, "gx", "gy", None)
    return jax.shard_map(
        local,
        mesh=mesh,
        in_specs=(field, field, P("gx", "gy", None), field, field, history, history),
        out_specs=(field, field),
        check_vma=False,
    )
```

```python
import functools

import jax
import jax.numpy as jnp
from jax import lax
from jax.experimental import pallas as pl
from jax.experimental.pallas import tpu as pltpu
from jax.sharding import PartitionSpec as P

SWEEPS = 3
REG = 0.05
FLOOR = 0.001
MESH = pl.DeviceIdType.MESH
DIRS = ((-1, 0), (1, 0), (0, -1), (0, 1), (-1, -1), (-1, 1), (1, -1), (1, 1))
HALO = SWEEPS


def both(a, b):
    return jnp.logical_and(a, b)


def kernel(
    counts,
    direct,
    entries,
    vel_hbm, forc_hbm, visc_hbm, rp_hbm, gp_hbm, hres_hbm, hval_hbm,
    out_ref, res_ref,
    wide, static, hist, late, ahead, past_res, past_val, coef, first, second, fres, delta,
    passing, ruler, in_sem, send_sem, recv_sem, gate, *shared,
):
    depth, _, cells_x, cells_y, lanes = hres_hbm.shape
    count_x, count_y = counts
    me_x, me_y = lax.axis_index("gx"), lax.axis_index("gy")
    rows = 2 * cells_y

    def exists(sx, sy):
        ok = None
        for step, me, count in ((sx, me_x, count_x), (sy, me_y, count_y)):
            if step != 0:
                here = me > 0 if step < 0 else me < count - 1
                ok = here if ok is None else both(ok, here)
        return ok

    loads = [
        pltpu.make_async_copy(vel_hbm, wide.at[:, HALO : HALO + cells_x, 0:cells_y], in_sem.at[0]),
        pltpu.make_async_copy(forc_hbm, static.at[0:3, 2 : 2 + cells_x, 0:cells_y], in_sem.at[0]),
        pltpu.make_async_copy(visc_hbm, static.at[3, 2 : 2 + cells_x, 0:cells_y], in_sem.at[0]),
        pltpu.make_async_copy(hval_hbm, hist.at[:, :, HALO : HALO + cells_x, 0:cells_y], in_sem.at[1]),
        pltpu.make_async_copy(hres_hbm, fres, in_sem.at[2]),
        pltpu.make_async_copy(rp_hbm, past_res, in_sem.at[2]),
        pltpu.make_async_copy(gp_hbm, past_val, in_sem.at[2]),
    ]
    for load in loads:
        load.start()
    barrier = pltpu.get_barrier_semaphore()
    for k in range(1, count_y):
        pl.semaphore_signal(
            barrier, inc=1, device_id=(me_x, lax.rem(me_y + k, count_y)), device_id_type=MESH
        )
    for k in range(2, count_x):

        @pl.when(me_x + k < count_x)
        def _():
            pl.semaphore_signal(barrier, inc=1, device_id=(me_x + k, me_y), device_id_type=MESH)

    total = count_y - 1 + jnp.maximum(me_x - 1, 0)
    for sx, sy in DIRS[:2] + DIRS[4:]:
        here = exists(sx, sy)
        total = total + jnp.where(here, 1, 0)

        @pl.when(here)
        def _():
            pl.semaphore_signal(
                barrier, inc=1, device_id=(me_x + sx, me_y + sy), device_id_type=MESH
            )

    def clear(ref, off):
        lead = (slice(None),) * (len(ref.shape) - 3)
        for (sx, sy), part in (
            ((-1, 0), (slice(0, off), slice(None))),
            ((1, 0), (slice(off + cells_x, 2 * off + cells_x), slice(None))),
            ((0, -1), (slice(None), slice(rows - off, rows))),
            ((0, 1), (slice(None), slice(cells_y, cells_y + off))),
        ):

            @pl.when(jnp.logical_not(exists(sx, sy)))
            def _():
                where = lead + part
                ref[where] = jnp.zeros(ref.at[where].shape, jnp.float32)

    clear(wide, HALO)
    clear(static, HALO - 1)
    with jax.named_scope("barrier"):
        pl.semaphore_wait(barrier, total)

    def span_x(sx, off, deep, skip=0):
        if sx == 0:
            return (slice(off, off + cells_x),) * 2
        if sx < 0:
            return slice(off + skip, off + deep), slice(off + cells_x + skip, off + cells_x + deep)
        return slice(off + cells_x - deep, off + cells_x - skip), slice(off - deep, off - skip)

    def span_y(sy, deep, skip=0):
        if sy == 0:
            return (slice(0, cells_y),) * 2
        if sy < 0:
            return slice(skip, deep), slice(cells_y + skip, cells_y + deep)
        return slice(cells_y - deep, cells_y - skip), slice(rows - deep, rows - skip)

    def faces(ref, off, dirs):
        pieces = []
        for sx, sy in dirs:
            deep = off if sx == 0 or sy == 0 else off - 1
            pieces.append((ref, (sx, sy), 0, span_x(sx, off, deep), span_y(sy, deep)))
        return pieces

    def layer(ref, off, deep, skip, sy):
        return [(ref, (0, sy), 0, span_x(0, off, 0), span_y(sy, deep, skip))]

    def corners(ref, off, side):
        deep = off - 1
        part = slice(cells_y, cells_y + deep) if side > 0 else slice(rows - deep, rows)
        return [(ref, (sx, 0), side, span_x(sx, off, deep), (part, part)) for sx in (-1, 1)]

    def length(part):
        return part.stop - part.start

    def size_of(piece):
        ref, _, _, (src_x, _), (src_y, _) = piece
        size = length(src_x) * length(src_y)
        for extent in ref.shape[:-3]:
            size = size * extent
        return size

    def places(me, count):
        if count == 1:
            return [((0, 0), None)]
        ends = [((0, 1), me == 0), ((1, 0), me == count - 1)]
        return ends + [((1, 1), both(me > 0, me < count - 1))] if count > 2 else ends

    def settle(pieces, sem, sending, more=0):
        for sides_x, here_x in places(me_x, count_x):
            for sides_y, here_y in places(me_y, count_y):
                size = more
                for piece in pieces:
                    _, (sx, sy), side, _, _ = piece
                    there = 1
                    for step, sides in ((sx, sides_x), (sy, sides_y)):
                        if step != 0:
                            there = there * sides[step > 0 if sending else step < 0]
                    if side != 0:
                        there = there * sides_y[side > 0]
                    size = size + there * size_of(piece)
                if sending and relayed and sides_y != (1, 1):
                    near, far = fields["north"][1][0], fields["far"][1][0]
                    size = size + size_of(near) * (depth - straight) // depth + size_of(far)
                if size == 0:
                    continue
                part = ruler.at[0:size]
                copy = pltpu.make_async_remote_copy(
                    src_ref=part,
                    dst_ref=part,
                    send_sem=sem,
                    recv_sem=sem,
                    device_id={"gx": lax.rem(me_x + 1, count_x)},
                    device_id_type=MESH,
                )
                here = [h for h in (here_x, here_y) if h is not None]

                @pl.when(functools.reduce(both, here))
                def _():
                    if sending:
                        copy.wait_send()
                    else:
                        copy.wait_recv()

    fields = {
        "wide": (0, faces(wide, HALO, DIRS)),
        "static": (0, faces(static, HALO - 1, DIRS)),
        "north": (1, layer(hist, HALO, HALO - 1, 0, -1)),
        "south": (2, layer(hist, HALO, HALO - 1, 0, 1)),
        "across": (3, faces(hist, HALO, DIRS[:2])),
        "far": (3, layer(hist, HALO, HALO, HALO - 1, -1) + layer(hist, HALO, HALO, HALO - 1, 1)),
        "turn_north": (3, corners(hist, HALO, 1)),
        "turn_south": (3, corners(hist, HALO, -1)),
        "late": (3, faces(late, HALO, DIRS)),
    }
    odd = lax.rem(me_y, 2) == 1
    even = jnp.logical_not(odd)

    relayed = count_y == 4
    turns = ((1, 1, 3, 2), (-1, 2, 0, 1))
    bands = {"north": (HALO - 1, 0, 1), "south": (HALO - 1, 0, 1), "far": (HALO, HALO - 1, 0)}
    straight = depth - (2 * depth) // 5

    def start(name, piece):
        which = fields[name][0]
        ref, (sx, sy), side, (src_x, dst_x), (src_y, dst_y) = piece
        here = exists(sx, sy)
        if side != 0:
            here = both(here, exists(0, side))
        lead = (slice(None),) * (len(ref.shape) - 3)

        def go(lead):
            pltpu.make_async_remote_copy(
                src_ref=ref.at[lead + (src_x, src_y)],
                dst_ref=ref.at[lead + (dst_x, dst_y)],
                send_sem=send_sem,
                recv_sem=recv_sem.at[which],
                device_id=(me_x + sx, me_y + sy),
                device_id_type=MESH,
            ).start()

        if relayed and name in bands:
            turned = me_y == (1 if sy > 0 else 2)
            if bands[name][2]:

                @pl.when(turned)
                def _():
                    go((slice(0, straight), slice(None)))

            here = both(here, jnp.logical_not(turned))

        @pl.when(here)
        def _():
            go(lead)

    def passed(name, device, sy, stage):
        deep, skip, part = bands[name]
        src_y, dst_y = span_y(sy, deep, skip)
        group = slice(straight if part else 0, depth)
        inside = slice(HALO, HALO + cells_x)
        kept = passing.at[group, :, :, skip:deep]
        src = hist.at[group, :, inside, src_y] if stage == 0 else kept
        dst = kept if stage < 2 else hist.at[group, :, inside, dst_y]
        return pltpu.make_async_remote_copy(
            src_ref=src,
            dst_ref=dst,
            send_sem=send_sem,
            recv_sem=recv_sem.at[fields[name][0] if stage == 2 else 4 if part else 5],
            device_id=device,
            device_id_type=MESH,
        )

    def detour(names):
        for name, (sy, owner, relay, _) in zip(names, turns if relayed else ()):

            @pl.when(me_y == owner)
            def _():
                passed(name, (me_x, relay), sy, 0).start()

    def pass_on(names):
        for name, (sy, _, relay, target) in zip(names, turns if relayed else ()):

            @pl.when(me_y == relay)
            def _():
                passed(name, (me_x, target), sy, 1).wait_recv()
                passed(name, (me_x, target), sy, 2).start()

    def send(*names):
        for name in names:
            for piece in fields[name][1]:
                start(name, piece)

    def send_in_turn(*names):
        for here, first in ((odd, 1), (even, -1)):

            @pl.when(here)
            def _():
                for sy, kinds in ((first, (1, 0)), (0, (1,)), (-first, (1, 0))):
                    for kind in kinds:
                        for name in names:
                            for piece in fields[name][1]:
                                if piece[1][1] == sy and (piece[1][0] != 0) == (kind == 1):
                                    start(name, piece)

    def receive(which):
        pieces = [p for number, group in fields.values() if number == which for p in group]
        with jax.named_scope("recv" + str(which)):
            settle(pieces, recv_sem.at[which], False)

    def turn(which, name):
        receive(which)
        send(name)

    def along(slots, idx, k, sends, recvs, me, count, axis):
        return pltpu.make_async_remote_copy(
            src_ref=slots.at[idx, me],
            dst_ref=slots.at[idx, me],
            send_sem=sends.at[idx],
            recv_sem=recvs.at[idx],
            device_id={axis: lax.rem(me + k, count)},
            device_id_type=MESH,
        )

    count_all = count_x * count_y
    me_all = me_x * count_y + me_y
    if direct:
        slots_all, all_sem = shared
    else:
        slots_y, slots_x, ysend, yrecv, xsend, xrecv = shared
        lines = (
            (slots_y, ysend, yrecv, me_y, count_y, "gy"),
            (slots_x, xsend, xrecv, me_x, count_x, "gx"),
        )

    def spread(line, idx, row):
        slots, sends, recvs, me, count, axis = line
        slots[idx, me] = row
        for k in range(1, count):
            along(slots, idx, k, sends, recvs, me, count, axis).start()

    def whole(line, idx):
        slots, sends, recvs, me, count, axis = line
        part = slots.at[idx, 0 : count - 1]
        return pltpu.make_async_remote_copy(
            src_ref=part,
            dst_ref=part,
            send_sem=sends.at[idx],
            recv_sem=recvs.at[idx],
            device_id={axis: lax.rem(me + 1, count)},
            device_id_type=MESH,
        )

    def gather(line, idx):
        slots, sends, recvs, me, count, axis = line
        whole(line, idx).wait_recv()
        total = slots[idx, 0]
        for k in range(1, count):
            total = total + slots[idx, k]
        return total

    def give(idx, row):
        if not direct:
            spread(lines[1], idx, row)
            return
        slots_all[idx, me_all] = row
        for k in range(1, count_all):
            peer = lax.rem(me_all + k, count_all)
            pltpu.make_async_remote_copy(
                src_ref=slots_all.at[idx, me_all],
                dst_ref=slots_all.at[idx, me_all],
                send_sem=send_sem,
                recv_sem=all_sem.at[idx],
                device_id=(lax.div(peer, count_y), lax.rem(peer, count_y)),
                device_id_type=MESH,
            ).start()

    def halfway(idx):
        if not direct:
            spread(lines[0], idx, gather(lines[1], idx))

    def take(idx):
        if not direct:
            return gather(lines[0], idx)
        part = ruler.at[0 : count_all - 1]
        with jax.named_scope("take" + str(idx)):
            pltpu.make_async_remote_copy(
                src_ref=part,
                dst_ref=part,
                send_sem=all_sem.at[idx],
                recv_sem=all_sem.at[idx],
                device_id={"gx": lax.rem(me_x + 1, count_x)},
                device_id_type=MESH,
            ).wait_recv()
        return jnp.sum(slots_all[idx], axis=0)

    lane = lax.broadcasted_iota(jnp.int32, (cells_y, lanes), 1)

    def packed(parts):
        row = jnp.zeros((cells_y, lanes), jnp.float32)
        for j, part in enumerate(parts):
            row = jnp.where(lane == j, jnp.sum(part, axis=1, keepdims=True), row)
        return jnp.sum(row, axis=0, keepdims=True)

    def unpacked(row, count):
        return [jnp.broadcast_to(row[:, j : j + 1], (cells_y, lanes)) for j in range(count)]

    own = [(c, x) for c in range(3) for x in range(cells_x)]

    def factored(gram):
        trace = gram[0][0]
        for j in range(1, depth):
            trace = trace + gram[j][j]
        shift = (REG / depth) * trace + FLOOR * entries
        lower = [[None] * depth for _ in range(depth)]
        inverse = [None] * depth
        scaled = [[None] * depth for _ in range(depth)]
        for j in range(depth):
            pivot = gram[j][j] + shift
            for k in range(j):
                pivot = pivot - lower[j][k] * scaled[j][k]
            inverse[j] = 1.0 / pivot
            for i in range(j + 1, depth):
                value = gram[i][j]
                for k in range(j):
                    value = value - scaled[i][k] * lower[j][k]
                scaled[i][j] = value
                lower[i][j] = value * inverse[j]
        return lower, inverse

    def solved(factors, rhs):
        lower, inverse = factors
        part = list(rhs)
        for j in range(depth):
            for i in range(j + 1, depth):
                part[i] = part[i] - lower[i][j] * part[j]
        part = [p * inv for p, inv in zip(part, inverse)]
        for j in reversed(range(depth)):
            for i in range(j):
                part[i] = part[i] - lower[j][i] * part[j]
        return part

    zlane = lax.broadcasted_iota(jnp.int32, (rows, lanes), 1)
    has_below = jnp.where(zlane == 0, 0.0, 1.0)
    has_above = jnp.where(zlane == lanes - 1, 0.0, 1.0)

    def relax(src, dst, off, x, cut):
        cs = [coef[j, x + off][0:cut] for j in range(6)]
        for c in range(3):
            here = src(c, x)
            total = coef[6 + c, x + off][0:cut]
            total = total + cs[0] * src(c, x - 1)[0:cut] + cs[1] * src(c, x + 1)[0:cut]
            total = total + cs[2] * pltpu.roll(here, 1, 0)[0:cut]
            total = total + cs[3] * pltpu.roll(here, rows - 1, 0)[0:cut]
            total = total + cs[4] * pltpu.roll(here[0:cut], 1, 1)
            total = total + cs[5] * pltpu.roll(here[0:cut], lanes - 1, 1)
            dst(c, x, total)

    def picard(field, dst):
        for x in range(-2, cells_x + 2):
            vel = [field[c, x + HALO] for c in range(3)]
            visc = static[3, x + 2]
            diag = 1.0 + 6.0 * visc + jnp.abs(vel[0]) + jnp.abs(vel[1]) + jnp.abs(vel[2])
            inv = 1.0 / diag
            for a in range(3):
                lo = (visc + jnp.maximum(vel[a], 0.0)) * inv
                hi = (visc - jnp.minimum(vel[a], 0.0)) * inv
                if a == 2:
                    lo, hi = lo * has_below, hi * has_above
                coef[2 * a, x + 2] = lo
                coef[2 * a + 1, x + 2] = hi
            for c in range(3):
                coef[6 + c, x + 2] = (static[c, x + 2] + vel[c]) * inv

        def put(ref, off):
            def store(c, x, value):
                ref[c, x + off] = value

            return store

        for x in range(-2, cells_x + 2):
            relax(lambda c, i: field[c, i + HALO], put(first, 2), 2, x, rows)
        for x in range(-1, cells_x + 1):
            relax(lambda c, i: first[c, i + 2], put(second, 1), 2, x, rows)
        for x in range(cells_x):
            relax(lambda c, i: second[c, i + 1], dst, 2, x, cells_y)

    if direct:
        for k in range(1, count_x):

            @pl.when(me_x >= k)
            def _():
                pl.semaphore_signal(gate, inc=1, device_id=(me_x - k, me_y), device_id_type=MESH)

        for k in range(1, count_y):
            pl.semaphore_signal(
                gate, inc=1, device_id=(me_x, lax.rem(me_y + k, count_y)), device_id_type=MESH
            )

    def loaded(which, *refs):
        size = 0
        for ref in refs:
            part = 1
            for extent in ref.shape[:-1]:
                part = part * extent
            size = size + part
        part = ruler.at[0:size]
        pltpu.make_async_copy(part, part, in_sem.at[which]).wait()

    loaded(0, vel_hbm, forc_hbm, visc_hbm)
    send_in_turn("wide", "static")
    loaded(1, hval_hbm)
    detour(("south", "north"))
    detour(("far", "far"))
    send_in_turn("north", "south")
    send("across")
    send_in_turn("far")
    loaded(2, hres_hbm, rp_hbm, gp_hbm)

    pairs = [(i, j) for i in range(depth) for j in range(i + 1)]
    clear(hist, HALO)
    clear(late, HALO)
    sums = [None] * (len(pairs) + depth)

    def add(j, value):
        sums[j] = value if sums[j] is None else sums[j] + value

    for c, x in own:
        f = [fres[j, c, x] for j in range(depth)]
        r = past_res[c, x]
        for n, (i, j) in enumerate(pairs):
            add(n, f[i] * f[j])
        for j in range(depth):
            add(len(pairs) + j, f[j] * r)
    row = packed(sums)
    if direct:
        with jax.named_scope("gate"):
            pl.semaphore_wait(gate, count_x - 1 - me_x + count_y - 1)
    give(0, row)

    pass_on(("south", "north"))
    receive(0)

    def store_value(c, x, value):
        late[c, x + HALO, 0:cells_y] = value

    picard(wide, store_value)

    sums = [None] * (depth + 1)
    for c, x in own:
        resid = late[c, x + HALO, 0:cells_y] - wide[c, x + HALO, 0:cells_y]
        newest = resid - past_res[c, x]
        delta[c, x] = newest
        for j in range(depth):
            add(j, fres[j, c, x] * resid)
        add(depth, newest * newest)
    give(1, packed(sums))
    send_in_turn("late")
    pass_on(("far", "far"))

    @pl.when(odd)
    def _():
        turn(1, "turn_north")
        turn(2, "turn_south")

    @pl.when(even)
    def _():
        turn(2, "turn_south")
        turn(1, "turn_north")

    halfway(0)
    halfway(1)

    early = unpacked(take(0), len(pairs) + depth)
    gram = [[None] * depth for _ in range(depth)]
    for n, (i, j) in enumerate(pairs):
        gram[i][j] = gram[j][i] = early[n]
    factors = factored(gram)
    receive(3)
    for_rhs = unpacked(take(1), depth + 1)
    rhs, newest_sq = for_rhs[:depth], for_rhs[depth]
    gamma = solved(factors, rhs)
    wide_gamma = [jnp.concatenate([g, g], 0) for g in gamma]
    for c in range(3):
        for x in range(cells_x + 2 * HALO):
            value = late[c, x]
            for j in range(depth):
                value = value - wide_gamma[j] * hist[j, c, x]
            ahead[c, x] = value

    def store_out(c, x, value):
        out_ref[c, x] = value

    picard(ahead, store_out)

    sums = [None] * depth
    for c, x in own:
        resid = out_ref[c, x] - ahead[c, x + HALO, 0:cells_y]
        res_ref[c, x] = resid
        for j in range(1, depth):
            add(j - 1, fres[j, c, x] * resid)
        add(depth - 1, delta[c, x] * resid)
    give(2, packed(sums))

    gram2 = [[None] * depth for _ in range(depth)]
    for i in range(depth - 1):
        for j in range(depth - 1):
            gram2[i][j] = gram[i + 1][j + 1]
        cross = rhs[i + 1] - early[len(pairs) + i + 1]
        gram2[i][depth - 1] = gram2[depth - 1][i] = cross
    gram2[depth - 1][depth - 1] = newest_sq
    factors = factored(gram2)

    halfway(2)
    final = take(2)
    gamma = solved(factors, unpacked(final, depth))
    for c, x in own:
        value = out_ref[c, x]
        newest = late[c, x + HALO, 0:cells_y] - past_val[c, x]
        for j in range(1, depth):
            value = value - gamma[j - 1] * hist[j, c, x + HALO, 0:cells_y]
        out_ref[c, x] = value - gamma[depth - 1] * newest
    pieces = [piece for _, group in fields.values() for piece in group]
    settle(pieces, send_sem, True, 3 * (count_all - 1) if direct else 0)
    if not direct:
        for line in lines:
            for idx in range(3):
                whole(line, idx).wait_send()


def leave(vel_ref, res_ref, vel_hbm, res_hbm, sem):
    copies = [
        pltpu.make_async_copy(vel_ref, vel_hbm, sem.at[0]),
        pltpu.make_async_copy(res_ref, res_hbm, sem.at[1]),
    ]
    for copy in copies:
        copy.start()
    for copy in copies:
        copy.wait()


def local(velocity, forcing, viscosity, residual_prev, value_prev, hist_res, hist_val):
    depth, comps, cells_x, cells_y, lanes = hist_res.shape
    counts = (lax.axis_size("gx"), lax.axis_size("gy"))
    entries = 3.0 * cells_x * cells_y * lanes * counts[0] * counts[1]
    rows = 2 * cells_y
    count_all = counts[0] * counts[1]
    direct = count_all <= 64
    def vmem(*shape):
        return pltpu.VMEM(shape + (lanes,), jnp.float32)

    if direct:
        shared = [vmem(3, count_all, 1), pltpu.SemaphoreType.DMA((3,))]
    else:
        shared = [vmem(3, counts[1], 1), vmem(3, counts[0], 1)]
        shared += [pltpu.SemaphoreType.DMA((3,))] * 4
    length = 9 * (depth + 3) * (6 * (cells_x + cells_y) + 16) + 3 * count_all
    results = pl.pallas_call(
        functools.partial(kernel, counts, direct, entries),
        name="anderson",
        out_shape=(pltpu.VMEM(velocity.shape, jnp.float32),) * 2,
        in_specs=[pl.BlockSpec(memory_space=pl.ANY)] * 7,
        out_specs=(pl.BlockSpec(memory_space=pltpu.VMEM),) * 2,
        scratch_shapes=[
            vmem(3, cells_x + 6, rows),
            vmem(4, cells_x + 4, rows),
            vmem(depth, 3, cells_x + 6, rows),
            vmem(3, cells_x + 6, rows),
            vmem(3, cells_x + 6, rows),
            vmem(3, cells_x, cells_y),
            vmem(3, cells_x, cells_y),
            vmem(9, cells_x + 4, rows),
            vmem(3, cells_x + 4, rows),
            vmem(3, cells_x + 2, rows),
            vmem(depth, 3, cells_x, cells_y),
            vmem(3, cells_x, cells_y),
            vmem(depth, 3, cells_x, HALO),
            vmem(length, 1),
            pltpu.SemaphoreType.DMA((3,)),
            pltpu.SemaphoreType.DMA,
            pltpu.SemaphoreType.DMA((6,)),
            pltpu.SemaphoreType.REGULAR,
            *shared,
        ],
        compiler_params=pltpu.CompilerParams(collective_id=0, has_side_effects=True),
    )(velocity, forcing, viscosity, residual_prev, value_prev, hist_res, hist_val)
    return pl.pallas_call(
        leave,
        name="leave",
        out_shape=(jax.ShapeDtypeStruct(velocity.shape, jnp.float32),) * 2,
        in_specs=[pl.BlockSpec(memory_space=pl.ANY)] * 2,
        out_specs=(pl.BlockSpec(memory_space=pl.ANY),) * 2,
        scratch_shapes=[pltpu.SemaphoreType.DMA((2,))],
    )(*(pltpu.with_memory_space_constraint(r, pltpu.VMEM) for r in results))


def solution(mesh):
    field = P(None, "gx", "gy", None)
    history = P(None, None, "gx", "gy", None)
    return jax.shard_map(
        local,
        mesh=mesh,
        in_specs=(field, field, P("gx", "gy", None), field, field, history, history),
        out_specs=(field, field),
        check_vma=False,
    )
```

```python
import functools

import jax
import jax.numpy as jnp
from jax import lax
from jax.experimental import pallas as pl
from jax.experimental.pallas import tpu as pltpu
from jax.sharding import PartitionSpec as P

SWEEPS = 3
REG = 0.05
FLOOR = 0.001
MESH = pl.DeviceIdType.MESH
DIRS = ((-1, 0), (1, 0), (0, -1), (0, 1), (-1, -1), (-1, 1), (1, -1), (1, 1))
HALO = SWEEPS


def both(a, b):
    return jnp.logical_and(a, b)


def kernel(
    counts,
    direct,
    entries,
    vel_hbm, forc_hbm, visc_hbm, rp_hbm, gp_hbm, hres_hbm, hval_hbm,
    out_ref, res_ref,
    wide, static, hist, late, ahead, past_res, past_val, coef, first, second, fres, delta,
    passing, ruler, in_sem, send_sem, recv_sem, gate, *shared,
):
    depth, _, cells_x, cells_y, lanes = hres_hbm.shape
    count_x, count_y = counts
    me_x, me_y = lax.axis_index("gx"), lax.axis_index("gy")
    rows = 2 * cells_y

    def exists(sx, sy):
        ok = None
        for step, me, count in ((sx, me_x, count_x), (sy, me_y, count_y)):
            if step != 0:
                here = me > 0 if step < 0 else me < count - 1
                ok = here if ok is None else both(ok, here)
        return ok

    loads = [
        pltpu.make_async_copy(vel_hbm, wide.at[:, HALO : HALO + cells_x, 0:cells_y], in_sem.at[0]),
        pltpu.make_async_copy(forc_hbm, static.at[0:3, 2 : 2 + cells_x, 0:cells_y], in_sem.at[0]),
        pltpu.make_async_copy(visc_hbm, static.at[3, 2 : 2 + cells_x, 0:cells_y], in_sem.at[0]),
        pltpu.make_async_copy(hval_hbm, hist.at[:, :, HALO : HALO + cells_x, 0:cells_y], in_sem.at[1]),
        pltpu.make_async_copy(hres_hbm, fres, in_sem.at[2]),
        pltpu.make_async_copy(rp_hbm, past_res, in_sem.at[2]),
        pltpu.make_async_copy(gp_hbm, past_val, in_sem.at[2]),
    ]
    for load in loads[:4]:
        load.start()
    barrier = pltpu.get_barrier_semaphore()
    for k in range(1, count_y):
        pl.semaphore_signal(
            barrier, inc=1, device_id=(me_x, lax.rem(me_y + k, count_y)), device_id_type=MESH
        )
    for k in range(2, count_x):

        @pl.when(me_x + k < count_x)
        def _():
            pl.semaphore_signal(barrier, inc=1, device_id=(me_x + k, me_y), device_id_type=MESH)

    total = count_y - 1 + jnp.maximum(me_x - 1, 0)
    for sx, sy in DIRS[:2] + DIRS[4:]:
        here = exists(sx, sy)
        total = total + jnp.where(here, 1, 0)

        @pl.when(here)
        def _():
            pl.semaphore_signal(
                barrier, inc=1, device_id=(me_x + sx, me_y + sy), device_id_type=MESH
            )

    def clear(ref, off):
        lead = (slice(None),) * (len(ref.shape) - 3)
        for (sx, sy), part in (
            ((-1, 0), (slice(0, off), slice(None))),
            ((1, 0), (slice(off + cells_x, 2 * off + cells_x), slice(None))),
            ((0, -1), (slice(None), slice(rows - off, rows))),
            ((0, 1), (slice(None), slice(cells_y, cells_y + off))),
        ):

            @pl.when(jnp.logical_not(exists(sx, sy)))
            def _():
                where = lead + part
                ref[where] = jnp.zeros(ref.at[where].shape, jnp.float32)

    clear(wide, HALO)
    clear(static, HALO - 1)
    with jax.named_scope("barrier"):
        pl.semaphore_wait(barrier, total)

    def span_x(sx, off, deep, skip=0):
        if sx == 0:
            return (slice(off, off + cells_x),) * 2
        if sx < 0:
            return slice(off + skip, off + deep), slice(off + cells_x + skip, off + cells_x + deep)
        return slice(off + cells_x - deep, off + cells_x - skip), slice(off - deep, off - skip)

    def span_y(sy, deep, skip=0):
        if sy == 0:
            return (slice(0, cells_y),) * 2
        if sy < 0:
            return slice(skip, deep), slice(cells_y + skip, cells_y + deep)
        return slice(cells_y - deep, cells_y - skip), slice(rows - deep, rows - skip)

    def faces(ref, off, dirs):
        pieces = []
        for sx, sy in dirs:
            deep = off if sx == 0 or sy == 0 else off - 1
            pieces.append((ref, (sx, sy), 0, span_x(sx, off, deep), span_y(sy, deep)))
        return pieces

    def layer(ref, off, deep, skip, sy):
        return [(ref, (0, sy), 0, span_x(0, off, 0), span_y(sy, deep, skip))]

    def corners(ref, off, side):
        deep = off - 1
        part = slice(cells_y, cells_y + deep) if side > 0 else slice(rows - deep, rows)
        return [(ref, (sx, 0), side, span_x(sx, off, deep), (part, part)) for sx in (-1, 1)]

    def length(part):
        return part.stop - part.start

    def size_of(piece):
        ref, _, _, (src_x, _), (src_y, _) = piece
        size = length(src_x) * length(src_y)
        for extent in ref.shape[:-3]:
            size = size * extent
        return size

    def places(me, count):
        if count == 1:
            return [((0, 0), None)]
        ends = [((0, 1), me == 0), ((1, 0), me == count - 1)]
        return ends + [((1, 1), both(me > 0, me < count - 1))] if count > 2 else ends

    def settle(pieces, sem, sending, more=0):
        for sides_x, here_x in places(me_x, count_x):
            for sides_y, here_y in places(me_y, count_y):
                size = more
                for piece in pieces:
                    _, (sx, sy), side, _, _ = piece
                    there = 1
                    for step, sides in ((sx, sides_x), (sy, sides_y)):
                        if step != 0:
                            there = there * sides[step > 0 if sending else step < 0]
                    if side != 0:
                        there = there * sides_y[side > 0]
                    size = size + there * size_of(piece)
                if sending and relayed and sides_y != (1, 1):
                    near, far = fields["north"][1][0], fields["far"][1][0]
                    size = size + size_of(near) * (depth - straight) // depth + size_of(far)
                if size == 0:
                    continue
                part = ruler.at[0:size]
                copy = pltpu.make_async_remote_copy(
                    src_ref=part,
                    dst_ref=part,
                    send_sem=sem,
                    recv_sem=sem,
                    device_id={"gx": lax.rem(me_x + 1, count_x)},
                    device_id_type=MESH,
                )
                here = [h for h in (here_x, here_y) if h is not None]

                @pl.when(functools.reduce(both, here))
                def _():
                    if sending:
                        copy.wait_send()
                    else:
                        copy.wait_recv()

    fields = {
        "wide": (0, faces(wide, HALO, DIRS)),
        "static": (0, faces(static, HALO - 1, DIRS)),
        "north": (1, layer(hist, HALO, HALO - 1, 0, -1)),
        "south": (2, layer(hist, HALO, HALO - 1, 0, 1)),
        "across": (3, faces(hist, HALO, DIRS[:2])),
        "far": (3, layer(hist, HALO, HALO, HALO - 1, -1) + layer(hist, HALO, HALO, HALO - 1, 1)),
        "turn_north": (3, corners(hist, HALO, 1)),
        "turn_south": (3, corners(hist, HALO, -1)),
        "late": (3, faces(late, HALO, DIRS)),
    }
    odd = lax.rem(me_y, 2) == 1
    even = jnp.logical_not(odd)

    relayed = count_y == 4
    turns = ((1, 1, 3, 2), (-1, 2, 0, 1))
    bands = {"north": (HALO - 1, 0, 1), "south": (HALO - 1, 0, 1), "far": (HALO, HALO - 1, 0)}
    straight = depth - (3 * depth) // 5

    def start(name, piece):
        which = fields[name][0]
        ref, (sx, sy), side, (src_x, dst_x), (src_y, dst_y) = piece
        here = exists(sx, sy)
        if side != 0:
            here = both(here, exists(0, side))
        lead = (slice(None),) * (len(ref.shape) - 3)

        def go(lead):
            pltpu.make_async_remote_copy(
                src_ref=ref.at[lead + (src_x, src_y)],
                dst_ref=ref.at[lead + (dst_x, dst_y)],
                send_sem=send_sem,
                recv_sem=recv_sem.at[which],
                device_id=(me_x + sx, me_y + sy),
                device_id_type=MESH,
            ).start()

        if relayed and name in bands:
            turned = me_y == (1 if sy > 0 else 2)
            if bands[name][2]:

                @pl.when(turned)
                def _():
                    go((slice(0, straight), slice(None)))

            here = both(here, jnp.logical_not(turned))

        @pl.when(here)
        def _():
            go(lead)

    def passed(name, device, sy, stage):
        deep, skip, part = bands[name]
        src_y, dst_y = span_y(sy, deep, skip)
        group = slice(straight if part else 0, depth)
        inside = slice(HALO, HALO + cells_x)
        kept = passing.at[group, :, :, skip:deep]
        src = hist.at[group, :, inside, src_y] if stage == 0 else kept
        dst = kept if stage < 2 else hist.at[group, :, inside, dst_y]
        return pltpu.make_async_remote_copy(
            src_ref=src,
            dst_ref=dst,
            send_sem=send_sem,
            recv_sem=recv_sem.at[fields[name][0] if stage == 2 else 4 if part else 5],
            device_id=device,
            device_id_type=MESH,
        )

    def detour(names):
        for name, (sy, owner, relay, _) in zip(names, turns if relayed else ()):

            @pl.when(me_y == owner)
            def _():
                passed(name, (me_x, relay), sy, 0).start()

    def pass_on(names):
        for name, (sy, _, relay, target) in zip(names, turns if relayed else ()):

            @pl.when(me_y == relay)
            def _():
                passed(name, (me_x, target), sy, 1).wait_recv()
                passed(name, (me_x, target), sy, 2).start()

    def send(*names):
        for name in names:
            for piece in fields[name][1]:
                start(name, piece)

    def send_in_turn(*names):
        for here, first in ((odd, 1), (even, -1)):

            @pl.when(here)
            def _():
                for sy, kinds in ((first, (1, 0)), (0, (1,)), (-first, (1, 0))):
                    for kind in kinds:
                        for name in names:
                            for piece in fields[name][1]:
                                if piece[1][1] == sy and (piece[1][0] != 0) == (kind == 1):
                                    start(name, piece)

    def receive(which):
        pieces = [p for number, group in fields.values() if number == which for p in group]
        with jax.named_scope("recv" + str(which)):
            settle(pieces, recv_sem.at[which], False)

    def turn(which, name):
        receive(which)
        send(name)

    def along(slots, idx, k, sends, recvs, me, count, axis):
        return pltpu.make_async_remote_copy(
            src_ref=slots.at[idx, me],
            dst_ref=slots.at[idx, me],
            send_sem=sends.at[idx],
            recv_sem=recvs.at[idx],
            device_id={axis: lax.rem(me + k, count)},
            device_id_type=MESH,
        )

    count_all = count_x * count_y
    me_all = me_x * count_y + me_y
    if direct:
        slots_all, all_sem = shared
    else:
        slots_y, slots_x, ysend, yrecv, xsend, xrecv = shared
        lines = (
            (slots_y, ysend, yrecv, me_y, count_y, "gy"),
            (slots_x, xsend, xrecv, me_x, count_x, "gx"),
        )

    def spread(line, idx, row):
        slots, sends, recvs, me, count, axis = line
        slots[idx, me] = row
        for k in range(1, count):
            along(slots, idx, k, sends, recvs, me, count, axis).start()

    def whole(line, idx):
        slots, sends, recvs, me, count, axis = line
        part = slots.at[idx, 0 : count - 1]
        return pltpu.make_async_remote_copy(
            src_ref=part,
            dst_ref=part,
            send_sem=sends.at[idx],
            recv_sem=recvs.at[idx],
            device_id={axis: lax.rem(me + 1, count)},
            device_id_type=MESH,
        )

    def gather(line, idx):
        slots, sends, recvs, me, count, axis = line
        whole(line, idx).wait_recv()
        total = slots[idx, 0]
        for k in range(1, count):
            total = total + slots[idx, k]
        return total

    def others(me, count):
        order = []
        for k in range(count - 1):
            down = count - 1 - k
            down = jnp.where(down <= me, down - 1, down)
            order.append(jnp.where(2 * me < count, down, jnp.where(k >= me, k + 1, k)))
        return order

    if direct:
        far_x, far_y = others(me_x, count_x), others(me_y, count_y)
        ranked = [(kx + 2 * ky, x, y) for kx, x in enumerate(far_x) for ky, y in enumerate(far_y)]
        ranked += [(kx + 2 * count_y, x, me_y) for kx, x in enumerate(far_x)]
        ranked += [(count_x + 2 * ky, me_x, y) for ky, y in enumerate(far_y)]
        peers = [(x, y) for _, x, y in sorted(ranked, key=lambda entry: entry[0])]

    def give(idx, row):
        if not direct:
            spread(lines[1], idx, row)
            return
        slots_all[idx, me_all] = row
        for peer in peers:
            pltpu.make_async_remote_copy(
                src_ref=slots_all.at[idx, me_all],
                dst_ref=slots_all.at[idx, me_all],
                send_sem=send_sem,
                recv_sem=all_sem.at[idx],
                device_id=peer,
                device_id_type=MESH,
            ).start()

    def halfway(idx):
        if not direct:
            spread(lines[0], idx, gather(lines[1], idx))

    def take(idx):
        if not direct:
            return gather(lines[0], idx)
        part = ruler.at[0 : count_all - 1]
        with jax.named_scope("take" + str(idx)):
            pltpu.make_async_remote_copy(
                src_ref=part,
                dst_ref=part,
                send_sem=all_sem.at[idx],
                recv_sem=all_sem.at[idx],
                device_id={"gx": lax.rem(me_x + 1, count_x)},
                device_id_type=MESH,
            ).wait_recv()
        return jnp.sum(slots_all[idx], axis=0)

    lane = lax.broadcasted_iota(jnp.int32, (cells_y, lanes), 1)

    def packed(parts):
        row = jnp.zeros((cells_y, lanes), jnp.float32)
        for j, part in enumerate(parts):
            row = jnp.where(lane == j, jnp.sum(part, axis=1, keepdims=True), row)
        return jnp.sum(row, axis=0, keepdims=True)

    def unpacked(row, count):
        return [jnp.broadcast_to(row[:, j : j + 1], (cells_y, lanes)) for j in range(count)]

    own = [(c, x) for c in range(3) for x in range(cells_x)]

    def factored(gram):
        trace = gram[0][0]
        for j in range(1, depth):
            trace = trace + gram[j][j]
        shift = (REG / depth) * trace + FLOOR * entries
        lower = [[None] * depth for _ in range(depth)]
        inverse = [None] * depth
        scaled = [[None] * depth for _ in range(depth)]
        for j in range(depth):
            pivot = gram[j][j] + shift
            for k in range(j):
                pivot = pivot - lower[j][k] * scaled[j][k]
            inverse[j] = 1.0 / pivot
            for i in range(j + 1, depth):
                value = gram[i][j]
                for k in range(j):
                    value = value - scaled[i][k] * lower[j][k]
                scaled[i][j] = value
                lower[i][j] = value * inverse[j]
        return lower, inverse

    def solved(factors, rhs):
        lower, inverse = factors
        part = list(rhs)
        for j in range(depth):
            for i in range(j + 1, depth):
                part[i] = part[i] - lower[i][j] * part[j]
        part = [p * inv for p, inv in zip(part, inverse)]
        for j in reversed(range(depth)):
            for i in range(j):
                part[i] = part[i] - lower[j][i] * part[j]
        return part

    zlane = lax.broadcasted_iota(jnp.int32, (rows, lanes), 1)
    has_below = jnp.where(zlane == 0, 0.0, 1.0)
    has_above = jnp.where(zlane == lanes - 1, 0.0, 1.0)

    def relax(src, dst, off, x, cut):
        cs = [coef[j, x + off][0:cut] for j in range(6)]
        for c in range(3):
            here = src(c, x)
            total = coef[6 + c, x + off][0:cut]
            total = total + cs[0] * src(c, x - 1)[0:cut] + cs[1] * src(c, x + 1)[0:cut]
            total = total + cs[2] * pltpu.roll(here, 1, 0)[0:cut]
            total = total + cs[3] * pltpu.roll(here, rows - 1, 0)[0:cut]
            total = total + cs[4] * pltpu.roll(here[0:cut], 1, 1)
            total = total + cs[5] * pltpu.roll(here[0:cut], lanes - 1, 1)
            dst(c, x, total)

    def picard(field, dst):
        for x in range(-2, cells_x + 2):
            vel = [field[c, x + HALO] for c in range(3)]
            visc = static[3, x + 2]
            diag = 1.0 + 6.0 * visc + jnp.abs(vel[0]) + jnp.abs(vel[1]) + jnp.abs(vel[2])
            inv = 1.0 / diag
            for a in range(3):
                lo = (visc + jnp.maximum(vel[a], 0.0)) * inv
                hi = (visc - jnp.minimum(vel[a], 0.0)) * inv
                if a == 2:
                    lo, hi = lo * has_below, hi * has_above
                coef[2 * a, x + 2] = lo
                coef[2 * a + 1, x + 2] = hi
            for c in range(3):
                coef[6 + c, x + 2] = (static[c, x + 2] + vel[c]) * inv

        def put(ref, off):
            def store(c, x, value):
                ref[c, x + off] = value

            return store

        for x in range(-2, cells_x + 2):
            relax(lambda c, i: field[c, i + HALO], put(first, 2), 2, x, rows)
        for x in range(-1, cells_x + 1):
            relax(lambda c, i: first[c, i + 2], put(second, 1), 2, x, rows)
        for x in range(cells_x):
            relax(lambda c, i: second[c, i + 1], dst, 2, x, cells_y)

    if direct:
        for k in range(1, count_x):

            @pl.when(me_x >= k)
            def _():
                pl.semaphore_signal(gate, inc=1, device_id=(me_x - k, me_y), device_id_type=MESH)

        for k in range(1, count_y):
            pl.semaphore_signal(
                gate, inc=1, device_id=(me_x, lax.rem(me_y + k, count_y)), device_id_type=MESH
            )

    def loaded(which, *refs):
        size = 0
        for ref in refs:
            part = 1
            for extent in ref.shape[:-1]:
                part = part * extent
            size = size + part
        part = ruler.at[0:size]
        pltpu.make_async_copy(part, part, in_sem.at[which]).wait()

    loaded(0, vel_hbm, forc_hbm, visc_hbm)
    send_in_turn("wide", "static")
    for load in loads[4:]:
        load.start()
    loaded(1, hval_hbm)
    detour(("south", "north"))
    detour(("far", "far"))
    send_in_turn("north", "south")
    send("across")
    loaded(2, hres_hbm, rp_hbm, gp_hbm)

    pairs = [(i, j) for i in range(depth) for j in range(i + 1)]
    clear(hist, HALO)
    clear(late, HALO)
    sums = [None] * (len(pairs) + depth)

    def add(j, value):
        sums[j] = value if sums[j] is None else sums[j] + value

    for c, x in own:
        f = [fres[j, c, x] for j in range(depth)]
        r = past_res[c, x]
        for n, (i, j) in enumerate(pairs):
            add(n, f[i] * f[j])
        for j in range(depth):
            add(len(pairs) + j, f[j] * r)
    row = packed(sums)
    if direct:
        with jax.named_scope("gate"):
            pl.semaphore_wait(gate, count_x - 1 - me_x + count_y - 1)
    give(0, row)

    pass_on(("south", "north"))
    receive(0)

    def store_value(c, x, value):
        late[c, x + HALO, 0:cells_y] = value

    picard(wide, store_value)

    sums = [None] * (depth + 1)
    for c, x in own:
        resid = late[c, x + HALO, 0:cells_y] - wide[c, x + HALO, 0:cells_y]
        newest = resid - past_res[c, x]
        delta[c, x] = newest
        for j in range(depth):
            add(j, fres[j, c, x] * resid)
        add(depth, newest * newest)
    give(1, packed(sums))
    send_in_turn("far")
    send_in_turn("late")
    pass_on(("far", "far"))

    @pl.when(odd)
    def _():
        turn(1, "turn_north")
        turn(2, "turn_south")

    @pl.when(even)
    def _():
        turn(2, "turn_south")
        turn(1, "turn_north")

    halfway(0)
    halfway(1)

    early = unpacked(take(0), len(pairs) + depth)
    gram = [[None] * depth for _ in range(depth)]
    for n, (i, j) in enumerate(pairs):
        gram[i][j] = gram[j][i] = early[n]
    factors = factored(gram)
    receive(3)
    for_rhs = unpacked(take(1), depth + 1)
    rhs, newest_sq = for_rhs[:depth], for_rhs[depth]
    gamma = solved(factors, rhs)
    wide_gamma = [jnp.concatenate([g, g], 0) for g in gamma]
    for c in range(3):
        for x in range(cells_x + 2 * HALO):
            value = late[c, x]
            for j in range(depth):
                value = value - wide_gamma[j] * hist[j, c, x]
            ahead[c, x] = value

    def store_out(c, x, value):
        out_ref[c, x] = value

    picard(ahead, store_out)

    sums = [None] * depth
    for c, x in own:
        resid = out_ref[c, x] - ahead[c, x + HALO, 0:cells_y]
        res_ref[c, x] = resid
        for j in range(1, depth):
            add(j - 1, fres[j, c, x] * resid)
        add(depth - 1, delta[c, x] * resid)
    give(2, packed(sums))

    gram2 = [[None] * depth for _ in range(depth)]
    for i in range(depth - 1):
        for j in range(depth - 1):
            gram2[i][j] = gram[i + 1][j + 1]
        cross = rhs[i + 1] - early[len(pairs) + i + 1]
        gram2[i][depth - 1] = gram2[depth - 1][i] = cross
    gram2[depth - 1][depth - 1] = newest_sq
    factors = factored(gram2)

    halfway(2)
    pieces = [piece for _, group in fields.values() for piece in group]
    settle(pieces, send_sem, True, 3 * (count_all - 1) if direct else 0)
    if not direct:
        for line in lines:
            for idx in range(3):
                whole(line, idx).wait_send()
    final = take(2)
    gamma = solved(factors, unpacked(final, depth))
    for c, x in own:
        value = out_ref[c, x]
        newest = late[c, x + HALO, 0:cells_y] - past_val[c, x]
        for j in range(1, depth):
            value = value - gamma[j - 1] * hist[j, c, x + HALO, 0:cells_y]
        out_ref[c, x] = value - gamma[depth - 1] * newest


def leave(vel_ref, res_ref, vel_hbm, res_hbm, sem):
    copies = [
        pltpu.make_async_copy(vel_ref, vel_hbm, sem.at[0]),
        pltpu.make_async_copy(res_ref, res_hbm, sem.at[1]),
    ]
    for copy in copies:
        copy.start()
    for copy in copies:
        copy.wait()


def local(velocity, forcing, viscosity, residual_prev, value_prev, hist_res, hist_val):
    depth, comps, cells_x, cells_y, lanes = hist_res.shape
    counts = (lax.axis_size("gx"), lax.axis_size("gy"))
    entries = 3.0 * cells_x * cells_y * lanes * counts[0] * counts[1]
    rows = 2 * cells_y
    count_all = counts[0] * counts[1]
    direct = count_all <= 64
    def vmem(*shape):
        return pltpu.VMEM(shape + (lanes,), jnp.float32)

    if direct:
        shared = [vmem(3, count_all, 1), pltpu.SemaphoreType.DMA((3,))]
    else:
        shared = [vmem(3, counts[1], 1), vmem(3, counts[0], 1)]
        shared += [pltpu.SemaphoreType.DMA((3,))] * 4
    length = 9 * (depth + 3) * (6 * (cells_x + cells_y) + 16) + 3 * count_all
    results = pl.pallas_call(
        functools.partial(kernel, counts, direct, entries),
        name="anderson",
        out_shape=(pltpu.VMEM(velocity.shape, jnp.float32),) * 2,
        in_specs=[pl.BlockSpec(memory_space=pl.ANY)] * 7,
        out_specs=(pl.BlockSpec(memory_space=pltpu.VMEM),) * 2,
        scratch_shapes=[
            vmem(3, cells_x + 6, rows),
            vmem(4, cells_x + 4, rows),
            vmem(depth, 3, cells_x + 6, rows),
            vmem(3, cells_x + 6, rows),
            vmem(3, cells_x + 6, rows),
            vmem(3, cells_x, cells_y),
            vmem(3, cells_x, cells_y),
            vmem(9, cells_x + 4, rows),
            vmem(3, cells_x + 4, rows),
            vmem(3, cells_x + 2, rows),
            vmem(depth, 3, cells_x, cells_y),
            vmem(3, cells_x, cells_y),
            vmem(depth, 3, cells_x, HALO),
            vmem(length, 1),
            pltpu.SemaphoreType.DMA((3,)),
            pltpu.SemaphoreType.DMA,
            pltpu.SemaphoreType.DMA((6,)),
            pltpu.SemaphoreType.REGULAR,
            *shared,
        ],
        compiler_params=pltpu.CompilerParams(collective_id=0, has_side_effects=True),
    )(velocity, forcing, viscosity, residual_prev, value_prev, hist_res, hist_val)
    return pl.pallas_call(
        leave,
        name="leave",
        out_shape=(jax.ShapeDtypeStruct(velocity.shape, jnp.float32),) * 2,
        in_specs=[pl.BlockSpec(memory_space=pl.ANY)] * 2,
        out_specs=(pl.BlockSpec(memory_space=pl.ANY),) * 2,
        scratch_shapes=[pltpu.SemaphoreType.DMA((2,))],
    )(*(pltpu.with_memory_space_constraint(r, pltpu.VMEM) for r in results))


def solution(mesh):
    field = P(None, "gx", "gy", None)
    history = P(None, None, "gx", "gy", None)
    return jax.shard_map(
        local,
        mesh=mesh,
        in_specs=(field, field, P("gx", "gy", None), field, field, history, history),
        out_specs=(field, field),
        check_vma=False,
    )
```

```python
import functools

import jax
import jax.numpy as jnp
from jax import lax
from jax.experimental import pallas as pl
from jax.experimental.pallas import tpu as pltpu
from jax.sharding import PartitionSpec as P

SWEEPS = 3
REG = 0.05
FLOOR = 0.001
MESH = pl.DeviceIdType.MESH
DIRS = ((-1, 0), (1, 0), (0, -1), (0, 1), (-1, -1), (-1, 1), (1, -1), (1, 1))
HALO = SWEEPS


def both(a, b):
    return jnp.logical_and(a, b)


def kernel(
    counts,
    direct,
    entries,
    vel_hbm, forc_hbm, visc_hbm, rp_hbm, gp_hbm, hres_hbm, hval_hbm,
    out_ref, res_ref,
    wide, static, hist, late, ahead, past_res, past_val, coef, first, second, fres, delta,
    passing, ruler, in_sem, send_sem, recv_sem, gate, *shared,
):
    depth, _, cells_x, cells_y, lanes = hres_hbm.shape
    count_x, count_y = counts
    me_x, me_y = lax.axis_index("gx"), lax.axis_index("gy")
    rows = 2 * cells_y

    def exists(sx, sy):
        ok = None
        for step, me, count in ((sx, me_x, count_x), (sy, me_y, count_y)):
            if step != 0:
                here = me > 0 if step < 0 else me < count - 1
                ok = here if ok is None else both(ok, here)
        return ok

    loads = [
        pltpu.make_async_copy(vel_hbm, wide.at[:, HALO : HALO + cells_x, 0:cells_y], in_sem.at[0]),
        pltpu.make_async_copy(forc_hbm, static.at[0:3, 2 : 2 + cells_x, 0:cells_y], in_sem.at[0]),
        pltpu.make_async_copy(visc_hbm, static.at[3, 2 : 2 + cells_x, 0:cells_y], in_sem.at[0]),
        pltpu.make_async_copy(hval_hbm, hist.at[:, :, HALO : HALO + cells_x, 0:cells_y], in_sem.at[1]),
        pltpu.make_async_copy(hres_hbm, fres, in_sem.at[2]),
        pltpu.make_async_copy(rp_hbm, past_res, in_sem.at[2]),
        pltpu.make_async_copy(gp_hbm, past_val, in_sem.at[2]),
    ]
    for load in loads[:4]:
        load.start()
    barrier = pltpu.get_barrier_semaphore()
    for k in range(1, count_y):
        pl.semaphore_signal(
            barrier, inc=1, device_id=(me_x, lax.rem(me_y + k, count_y)), device_id_type=MESH
        )
    for k in range(2, count_x):

        @pl.when(me_x + k < count_x)
        def _():
            pl.semaphore_signal(barrier, inc=1, device_id=(me_x + k, me_y), device_id_type=MESH)

    total = count_y - 1 + jnp.maximum(me_x - 1, 0)
    for sx, sy in DIRS[:2] + DIRS[4:]:
        here = exists(sx, sy)
        total = total + jnp.where(here, 1, 0)

        @pl.when(here)
        def _():
            pl.semaphore_signal(
                barrier, inc=1, device_id=(me_x + sx, me_y + sy), device_id_type=MESH
            )

    def clear(ref, off):
        lead = (slice(None),) * (len(ref.shape) - 3)
        for (sx, sy), part in (
            ((-1, 0), (slice(0, off), slice(None))),
            ((1, 0), (slice(off + cells_x, 2 * off + cells_x), slice(None))),
            ((0, -1), (slice(None), slice(rows - off, rows))),
            ((0, 1), (slice(None), slice(cells_y, cells_y + off))),
        ):

            @pl.when(jnp.logical_not(exists(sx, sy)))
            def _():
                where = lead + part
                ref[where] = jnp.zeros(ref.at[where].shape, jnp.float32)

    clear(wide, HALO)
    clear(static, HALO - 1)
    with jax.named_scope("barrier"):
        pl.semaphore_wait(barrier, total)

    def span_x(sx, off, deep, skip=0):
        if sx == 0:
            return (slice(off, off + cells_x),) * 2
        if sx < 0:
            return slice(off + skip, off + deep), slice(off + cells_x + skip, off + cells_x + deep)
        return slice(off + cells_x - deep, off + cells_x - skip), slice(off - deep, off - skip)

    def span_y(sy, deep, skip=0):
        if sy == 0:
            return (slice(0, cells_y),) * 2
        if sy < 0:
            return slice(skip, deep), slice(cells_y + skip, cells_y + deep)
        return slice(cells_y - deep, cells_y - skip), slice(rows - deep, rows - skip)

    def faces(ref, off, dirs):
        pieces = []
        for sx, sy in dirs:
            deep = off if sx == 0 or sy == 0 else off - 1
            pieces.append((ref, (sx, sy), 0, span_x(sx, off, deep), span_y(sy, deep)))
        return pieces

    def layer(ref, off, deep, skip, sy):
        return [(ref, (0, sy), 0, span_x(0, off, 0), span_y(sy, deep, skip))]

    def corners(ref, off, side):
        deep = off - 1
        part = slice(cells_y, cells_y + deep) if side > 0 else slice(rows - deep, rows)
        return [(ref, (sx, 0), side, span_x(sx, off, deep), (part, part)) for sx in (-1, 1)]

    def length(part):
        return part.stop - part.start

    def size_of(piece):
        ref, _, _, (src_x, _), (src_y, _) = piece
        size = length(src_x) * length(src_y)
        for extent in ref.shape[:-3]:
            size = size * extent
        return size

    def places(me, count):
        if count == 1:
            return [((0, 0), None)]
        ends = [((0, 1), me == 0), ((1, 0), me == count - 1)]
        return ends + [((1, 1), both(me > 0, me < count - 1))] if count > 2 else ends

    def settle(pieces, sem, sending, more=0):
        for sides_x, here_x in places(me_x, count_x):
            for sides_y, here_y in places(me_y, count_y):
                size = more
                for piece in pieces:
                    _, (sx, sy), side, _, _ = piece
                    there = 1
                    for step, sides in ((sx, sides_x), (sy, sides_y)):
                        if step != 0:
                            there = there * sides[step > 0 if sending else step < 0]
                    if side != 0:
                        there = there * sides_y[side > 0]
                    size = size + there * size_of(piece)
                if sending and relayed and sides_y != (1, 1):
                    near, far = fields["north"][1][0], fields["far"][1][0]
                    size = size + size_of(near) * (depth - straight) // depth + size_of(far)
                if size == 0:
                    continue
                part = ruler.at[0:size]
                copy = pltpu.make_async_remote_copy(
                    src_ref=part,
                    dst_ref=part,
                    send_sem=sem,
                    recv_sem=sem,
                    device_id={"gx": lax.rem(me_x + 1, count_x)},
                    device_id_type=MESH,
                )
                here = [h for h in (here_x, here_y) if h is not None]

                @pl.when(functools.reduce(both, here))
                def _():
                    if sending:
                        copy.wait_send()
                    else:
                        copy.wait_recv()

    fields = {
        "wide": (0, faces(wide, HALO, DIRS)),
        "static": (0, faces(static, HALO - 1, DIRS)),
        "north": (1, layer(hist, HALO, HALO - 1, 0, -1)),
        "south": (2, layer(hist, HALO, HALO - 1, 0, 1)),
        "across": (3, faces(hist, HALO, DIRS[:2])),
        "far": (3, layer(hist, HALO, HALO, HALO - 1, -1) + layer(hist, HALO, HALO, HALO - 1, 1)),
        "turn_north": (3, corners(hist, HALO, 1)),
        "turn_south": (3, corners(hist, HALO, -1)),
        "late": (3, faces(late, HALO, DIRS)),
    }
    odd = lax.rem(me_y, 2) == 1
    even = jnp.logical_not(odd)

    relayed = count_y == 4
    turns = ((1, 1, 3, 2), (-1, 2, 0, 1))
    bands = {"north": (HALO - 1, 0, 1), "south": (HALO - 1, 0, 1), "far": (HALO, HALO - 1, 0)}
    straight = depth - (4 * depth) // 5

    def start(name, piece):
        which = fields[name][0]
        ref, (sx, sy), side, (src_x, dst_x), (src_y, dst_y) = piece
        here = exists(sx, sy)
        if side != 0:
            here = both(here, exists(0, side))
        lead = (slice(None),) * (len(ref.shape) - 3)

        def go(lead):
            pltpu.make_async_remote_copy(
                src_ref=ref.at[lead + (src_x, src_y)],
                dst_ref=ref.at[lead + (dst_x, dst_y)],
                send_sem=send_sem,
                recv_sem=recv_sem.at[which],
                device_id=(me_x + sx, me_y + sy),
                device_id_type=MESH,
            ).start()

        if relayed and name in bands:
            turned = me_y == (1 if sy > 0 else 2)
            if bands[name][2]:

                @pl.when(turned)
                def _():
                    go((slice(0, straight), slice(None)))

            here = both(here, jnp.logical_not(turned))

        @pl.when(here)
        def _():
            go(lead)

    middle = (straight + depth) // 2
    groups = {True: (slice(straight, middle), slice(middle, depth)), False: (slice(0, depth),)}

    def passed(name, device, sy, stage, which):
        deep, skip, part = bands[name]
        src_y, dst_y = span_y(sy, deep, skip)
        group = groups[part == 1][which]
        inside = slice(HALO, HALO + cells_x)
        kept = passing.at[group, :, :, skip:deep]
        src = hist.at[group, :, inside, src_y] if stage == 0 else kept
        dst = kept if stage < 2 else hist.at[group, :, inside, dst_y]
        return pltpu.make_async_remote_copy(
            src_ref=src,
            dst_ref=dst,
            send_sem=send_sem,
            recv_sem=recv_sem.at[fields[name][0] if stage == 2 else 4 + which if part else 6],
            device_id=device,
            device_id_type=MESH,
        )

    def detour(names):
        for name, (sy, owner, relay, _) in zip(names, turns if relayed else ()):

            @pl.when(me_y == owner)
            def _():
                for which in range(len(groups[bands[name][2] == 1])):
                    passed(name, (me_x, relay), sy, 0, which).start()

    def pass_on(names):
        for name, (sy, _, relay, target) in zip(names, turns if relayed else ()):

            @pl.when(me_y == relay)
            def _():
                for which in range(len(groups[bands[name][2] == 1])):
                    passed(name, (me_x, target), sy, 1, which).wait_recv()
                    passed(name, (me_x, target), sy, 2, which).start()

    def send(*names):
        for name in names:
            for piece in fields[name][1]:
                start(name, piece)

    def send_in_turn(*names):
        for here, first in ((odd, 1), (even, -1)):

            @pl.when(here)
            def _():
                for sy, kinds in ((first, (1, 0)), (0, (1,)), (-first, (1, 0))):
                    for kind in kinds:
                        for name in names:
                            for piece in fields[name][1]:
                                if piece[1][1] == sy and (piece[1][0] != 0) == (kind == 1):
                                    start(name, piece)

    def receive(which):
        pieces = [p for number, group in fields.values() if number == which for p in group]
        with jax.named_scope("recv" + str(which)):
            settle(pieces, recv_sem.at[which], False)

    def turn(which, name):
        receive(which)
        send(name)

    def along(slots, idx, k, sends, recvs, me, count, axis):
        return pltpu.make_async_remote_copy(
            src_ref=slots.at[idx, me],
            dst_ref=slots.at[idx, me],
            send_sem=sends.at[idx],
            recv_sem=recvs.at[idx],
            device_id={axis: lax.rem(me + k, count)},
            device_id_type=MESH,
        )

    count_all = count_x * count_y
    me_all = me_x * count_y + me_y
    if direct:
        slots_all, all_sem = shared
    else:
        slots_y, slots_x, ysend, yrecv, xsend, xrecv = shared
        lines = (
            (slots_y, ysend, yrecv, me_y, count_y, "gy"),
            (slots_x, xsend, xrecv, me_x, count_x, "gx"),
        )

    def spread(line, idx, row):
        slots, sends, recvs, me, count, axis = line
        slots[idx, me] = row
        for k in range(1, count):
            along(slots, idx, k, sends, recvs, me, count, axis).start()

    def whole(line, idx):
        slots, sends, recvs, me, count, axis = line
        part = slots.at[idx, 0 : count - 1]
        return pltpu.make_async_remote_copy(
            src_ref=part,
            dst_ref=part,
            send_sem=sends.at[idx],
            recv_sem=recvs.at[idx],
            device_id={axis: lax.rem(me + 1, count)},
            device_id_type=MESH,
        )

    def gather(line, idx):
        slots, sends, recvs, me, count, axis = line
        whole(line, idx).wait_recv()
        total = slots[idx, 0]
        for k in range(1, count):
            total = total + slots[idx, k]
        return total

    def others(me, count):
        order = []
        for k in range(count - 1):
            down = count - 1 - k
            down = jnp.where(down <= me, down - 1, down)
            order.append(jnp.where(2 * me < count, down, jnp.where(k >= me, k + 1, k)))
        return order

    if direct:
        far_x, far_y = others(me_x, count_x), others(me_y, count_y)
        ranked = [(kx + 2 * ky, x, y) for kx, x in enumerate(far_x) for ky, y in enumerate(far_y)]
        ranked += [(kx + 2 * count_y, x, me_y) for kx, x in enumerate(far_x)]
        ranked += [(count_x + 2 * ky, me_x, y) for ky, y in enumerate(far_y)]
        peers = [(x, y) for _, x, y in sorted(ranked, key=lambda entry: entry[0])]

    def give(idx, row):
        if not direct:
            spread(lines[1], idx, row)
            return
        slots_all[idx, me_all] = row
        for peer in peers:
            pltpu.make_async_remote_copy(
                src_ref=slots_all.at[idx, me_all],
                dst_ref=slots_all.at[idx, me_all],
                send_sem=send_sem,
                recv_sem=all_sem.at[idx],
                device_id=peer,
                device_id_type=MESH,
            ).start()

    def halfway(idx):
        if not direct:
            spread(lines[0], idx, gather(lines[1], idx))

    def take(idx):
        if not direct:
            return gather(lines[0], idx)
        part = ruler.at[0 : count_all - 1]
        with jax.named_scope("take" + str(idx)):
            pltpu.make_async_remote_copy(
                src_ref=part,
                dst_ref=part,
                send_sem=all_sem.at[idx],
                recv_sem=all_sem.at[idx],
                device_id={"gx": lax.rem(me_x + 1, count_x)},
                device_id_type=MESH,
            ).wait_recv()
        return jnp.sum(slots_all[idx], axis=0)

    lane = lax.broadcasted_iota(jnp.int32, (cells_y, lanes), 1)

    def packed(parts):
        row = jnp.zeros((cells_y, lanes), jnp.float32)
        for j, part in enumerate(parts):
            row = jnp.where(lane == j, jnp.sum(part, axis=1, keepdims=True), row)
        return jnp.sum(row, axis=0, keepdims=True)

    def unpacked(row, count):
        return [jnp.broadcast_to(row[:, j : j + 1], (cells_y, lanes)) for j in range(count)]

    own = [(c, x) for c in range(3) for x in range(cells_x)]

    def factored(gram):
        trace = gram[0][0]
        for j in range(1, depth):
            trace = trace + gram[j][j]
        shift = (REG / depth) * trace + FLOOR * entries
        lower = [[None] * depth for _ in range(depth)]
        inverse = [None] * depth
        scaled = [[None] * depth for _ in range(depth)]
        for j in range(depth):
            pivot = gram[j][j] + shift
            for k in range(j):
                pivot = pivot - lower[j][k] * scaled[j][k]
            inverse[j] = 1.0 / pivot
            for i in range(j + 1, depth):
                value = gram[i][j]
                for k in range(j):
                    value = value - scaled[i][k] * lower[j][k]
                scaled[i][j] = value
                lower[i][j] = value * inverse[j]
        return lower, inverse

    def solved(factors, rhs):
        lower, inverse = factors
        part = list(rhs)
        for j in range(depth):
            for i in range(j + 1, depth):
                part[i] = part[i] - lower[i][j] * part[j]
        part = [p * inv for p, inv in zip(part, inverse)]
        for j in reversed(range(depth)):
            for i in range(j):
                part[i] = part[i] - lower[j][i] * part[j]
        return part

    zlane = lax.broadcasted_iota(jnp.int32, (rows, lanes), 1)
    has_below = jnp.where(zlane == 0, 0.0, 1.0)
    has_above = jnp.where(zlane == lanes - 1, 0.0, 1.0)

    def relax(src, dst, off, x, cut):
        cs = [coef[j, x + off][0:cut] for j in range(6)]
        for c in range(3):
            here = src(c, x)
            total = coef[6 + c, x + off][0:cut]
            total = total + cs[0] * src(c, x - 1)[0:cut] + cs[1] * src(c, x + 1)[0:cut]
            total = total + cs[2] * pltpu.roll(here, 1, 0)[0:cut]
            total = total + cs[3] * pltpu.roll(here, rows - 1, 0)[0:cut]
            total = total + cs[4] * pltpu.roll(here[0:cut], 1, 1)
            total = total + cs[5] * pltpu.roll(here[0:cut], lanes - 1, 1)
            dst(c, x, total)

    def picard(field, dst):
        for x in range(-2, cells_x + 2):
            cut = cells_y if x in (-2, cells_x + 1) else rows
            vel = [field[c, x + HALO, 0:cut] for c in range(3)]
            visc = static[3, x + 2, 0:cut]
            diag = 1.0 + 6.0 * visc + jnp.abs(vel[0]) + jnp.abs(vel[1]) + jnp.abs(vel[2])
            inv = 1.0 / diag
            for a in range(3):
                lo = (visc + jnp.maximum(vel[a], 0.0)) * inv
                hi = (visc - jnp.minimum(vel[a], 0.0)) * inv
                if a == 2:
                    lo, hi = lo * has_below[0:cut], hi * has_above[0:cut]
                coef[2 * a, x + 2, 0:cut] = lo
                coef[2 * a + 1, x + 2, 0:cut] = hi
            for c in range(3):
                coef[6 + c, x + 2, 0:cut] = (static[c, x + 2, 0:cut] + vel[c]) * inv

        def put(ref, off):
            def store(c, x, value):
                ref[c, x + off, 0 : value.shape[0]] = value

            return store

        for x in range(-2, cells_x + 2):
            cut = cells_y if x in (-2, cells_x + 1) else rows
            relax(lambda c, i: field[c, i + HALO], put(first, 2), 2, x, cut)
        for x in range(-1, cells_x + 1):
            cut = cells_y if x in (-1, cells_x) else rows
            relax(lambda c, i: first[c, i + 2], put(second, 1), 2, x, cut)
        for x in range(cells_x):
            relax(lambda c, i: second[c, i + 1], dst, 2, x, cells_y)

    if direct:
        for k in range(1, count_x):

            @pl.when(me_x >= k)
            def _():
                pl.semaphore_signal(gate, inc=1, device_id=(me_x - k, me_y), device_id_type=MESH)

        for k in range(1, count_y):
            pl.semaphore_signal(
                gate, inc=1, device_id=(me_x, lax.rem(me_y + k, count_y)), device_id_type=MESH
            )

    def loaded(which, *refs):
        size = 0
        for ref in refs:
            part = 1
            for extent in ref.shape[:-1]:
                part = part * extent
            size = size + part
        part = ruler.at[0:size]
        pltpu.make_async_copy(part, part, in_sem.at[which]).wait()

    loaded(0, vel_hbm, forc_hbm, visc_hbm)
    send_in_turn("wide", "static")
    for load in loads[4:]:
        load.start()
    loaded(1, hval_hbm)
    detour(("south", "north"))
    detour(("far", "far"))
    send_in_turn("north", "south")
    send("across")
    loaded(2, hres_hbm, rp_hbm, gp_hbm)

    pairs = [(i, j) for i in range(depth) for j in range(i + 1)]
    clear(hist, HALO)
    clear(late, HALO)
    sums = [None] * (len(pairs) + depth)

    def add(j, value):
        sums[j] = value if sums[j] is None else sums[j] + value

    for c, x in own:
        f = [fres[j, c, x] for j in range(depth)]
        r = past_res[c, x]
        for n, (i, j) in enumerate(pairs):
            add(n, f[i] * f[j])
        for j in range(depth):
            add(len(pairs) + j, f[j] * r)
    row = packed(sums)
    pass_on(("south", "north"))
    if direct:
        with jax.named_scope("gate"):
            pl.semaphore_wait(gate, count_x - 1 - me_x + count_y - 1)
    give(0, row)

    receive(0)

    def store_value(c, x, value):
        late[c, x + HALO, 0:cells_y] = value

    picard(wide, store_value)

    sums = [None] * (depth + 1)
    for c, x in own:
        resid = late[c, x + HALO, 0:cells_y] - wide[c, x + HALO, 0:cells_y]
        newest = resid - past_res[c, x]
        delta[c, x] = newest
        for j in range(depth):
            add(j, fres[j, c, x] * resid)
        add(depth, newest * newest)
    give(1, packed(sums))
    send_in_turn("late")
    send_in_turn("far")
    pass_on(("far", "far"))

    @pl.when(odd)
    def _():
        turn(1, "turn_north")
        turn(2, "turn_south")

    @pl.when(even)
    def _():
        turn(2, "turn_south")
        turn(1, "turn_north")

    halfway(0)
    halfway(1)

    early = unpacked(take(0), len(pairs) + depth)
    gram = [[None] * depth for _ in range(depth)]
    for n, (i, j) in enumerate(pairs):
        gram[i][j] = gram[j][i] = early[n]
    factors = factored(gram)
    receive(3)
    for_rhs = unpacked(take(1), depth + 1)
    rhs, newest_sq = for_rhs[:depth], for_rhs[depth]
    gamma = solved(factors, rhs)
    wide_gamma = [jnp.concatenate([g, g], 0) for g in gamma]
    for c in range(3):
        for x in range(cells_x + 2 * HALO):
            cut = cells_y if x in (0, cells_x + 2 * HALO - 1) else rows
            value = late[c, x, 0:cut]
            for j in range(depth):
                value = value - wide_gamma[j][0:cut] * hist[j, c, x, 0:cut]
            ahead[c, x, 0:cut] = value

    def store_out(c, x, value):
        out_ref[c, x] = value

    picard(ahead, store_out)

    sums = [None] * depth
    for c, x in own:
        resid = out_ref[c, x] - ahead[c, x + HALO, 0:cells_y]
        res_ref[c, x] = resid
        for j in range(1, depth):
            add(j - 1, fres[j, c, x] * resid)
        add(depth - 1, delta[c, x] * resid)
    give(2, packed(sums))

    gram2 = [[None] * depth for _ in range(depth)]
    for i in range(depth - 1):
        for j in range(depth - 1):
            gram2[i][j] = gram[i + 1][j + 1]
        cross = rhs[i + 1] - early[len(pairs) + i + 1]
        gram2[i][depth - 1] = gram2[depth - 1][i] = cross
    gram2[depth - 1][depth - 1] = newest_sq
    factors = factored(gram2)

    halfway(2)
    pieces = [piece for _, group in fields.values() for piece in group]
    settle(pieces, send_sem, True, 3 * (count_all - 1) if direct else 0)
    if not direct:
        for line in lines:
            for idx in range(3):
                whole(line, idx).wait_send()
    final = take(2)
    gamma = solved(factors, unpacked(final, depth))
    for c, x in own:
        value = out_ref[c, x]
        newest = late[c, x + HALO, 0:cells_y] - past_val[c, x]
        for j in range(1, depth):
            value = value - gamma[j - 1] * hist[j, c, x + HALO, 0:cells_y]
        out_ref[c, x] = value - gamma[depth - 1] * newest


def leave(vel_ref, res_ref, vel_hbm, res_hbm, sem):
    copies = [
        pltpu.make_async_copy(vel_ref, vel_hbm, sem.at[0]),
        pltpu.make_async_copy(res_ref, res_hbm, sem.at[1]),
    ]
    for copy in copies:
        copy.start()
    for copy in copies:
        copy.wait()


def local(velocity, forcing, viscosity, residual_prev, value_prev, hist_res, hist_val):
    depth, comps, cells_x, cells_y, lanes = hist_res.shape
    counts = (lax.axis_size("gx"), lax.axis_size("gy"))
    entries = 3.0 * cells_x * cells_y * lanes * counts[0] * counts[1]
    rows = 2 * cells_y
    count_all = counts[0] * counts[1]
    direct = count_all <= 64
    def vmem(*shape):
        return pltpu.VMEM(shape + (lanes,), jnp.float32)

    if direct:
        shared = [vmem(3, count_all, 1), pltpu.SemaphoreType.DMA((3,))]
    else:
        shared = [vmem(3, counts[1], 1), vmem(3, counts[0], 1)]
        shared += [pltpu.SemaphoreType.DMA((3,))] * 4
    length = 9 * (depth + 3) * (6 * (cells_x + cells_y) + 16) + 3 * count_all
    results = pl.pallas_call(
        functools.partial(kernel, counts, direct, entries),
        name="anderson",
        out_shape=(pltpu.VMEM(velocity.shape, jnp.float32),) * 2,
        in_specs=[pl.BlockSpec(memory_space=pl.ANY)] * 7,
        out_specs=(pl.BlockSpec(memory_space=pltpu.VMEM),) * 2,
        scratch_shapes=[
            vmem(3, cells_x + 6, rows),
            vmem(4, cells_x + 4, rows),
            vmem(depth, 3, cells_x + 6, rows),
            vmem(3, cells_x + 6, rows),
            vmem(3, cells_x + 6, rows),
            vmem(3, cells_x, cells_y),
            vmem(3, cells_x, cells_y),
            vmem(9, cells_x + 4, rows),
            vmem(3, cells_x + 4, rows),
            vmem(3, cells_x + 2, rows),
            vmem(depth, 3, cells_x, cells_y),
            vmem(3, cells_x, cells_y),
            vmem(depth, 3, cells_x, HALO),
            vmem(length, 1),
            pltpu.SemaphoreType.DMA((3,)),
            pltpu.SemaphoreType.DMA,
            pltpu.SemaphoreType.DMA((7,)),
            pltpu.SemaphoreType.REGULAR,
            *shared,
        ],
        compiler_params=pltpu.CompilerParams(collective_id=0, has_side_effects=True),
    )(velocity, forcing, viscosity, residual_prev, value_prev, hist_res, hist_val)
    return pl.pallas_call(
        leave,
        name="leave",
        out_shape=(jax.ShapeDtypeStruct(velocity.shape, jnp.float32),) * 2,
        in_specs=[pl.BlockSpec(memory_space=pl.ANY)] * 2,
        out_specs=(pl.BlockSpec(memory_space=pl.ANY),) * 2,
        scratch_shapes=[pltpu.SemaphoreType.DMA((2,))],
    )(*(pltpu.with_memory_space_constraint(r, pltpu.VMEM) for r in results))


def solution(mesh):
    field = P(None, "gx", "gy", None)
    history = P(None, None, "gx", "gy", None)
    return jax.shard_map(
        local,
        mesh=mesh,
        in_specs=(field, field, P("gx", "gy", None), field, field, history, history),
        out_specs=(field, field),
        check_vma=False,
    )
```

```python
import functools

import jax
import jax.numpy as jnp
from jax import lax
from jax.experimental import pallas as pl
from jax.experimental.pallas import tpu as pltpu
from jax.sharding import PartitionSpec as P

SWEEPS = 3
REG = 0.05
FLOOR = 0.001
MESH = pl.DeviceIdType.MESH
DIRS = ((-1, 0), (1, 0), (0, -1), (0, 1), (-1, -1), (-1, 1), (1, -1), (1, 1))
HALO = SWEEPS


def both(a, b):
    return jnp.logical_and(a, b)


def kernel(
    counts,
    direct,
    entries,
    vel_hbm, forc_hbm, visc_hbm, rp_hbm, gp_hbm, hres_hbm, hval_hbm,
    out_ref, res_ref,
    wide, static, hist, late, ahead, past_res, past_val, coef, first, second, fres, delta,
    passing, ruler, in_sem, send_sem, recv_sem, gate, *shared,
):
    depth, _, cells_x, cells_y, lanes = hres_hbm.shape
    count_x, count_y = counts
    me_x, me_y = lax.axis_index("gx"), lax.axis_index("gy")
    rows = 2 * cells_y

    def exists(sx, sy):
        ok = None
        for step, me, count in ((sx, me_x, count_x), (sy, me_y, count_y)):
            if step != 0:
                here = me > 0 if step < 0 else me < count - 1
                ok = here if ok is None else both(ok, here)
        return ok

    loads = [
        pltpu.make_async_copy(vel_hbm, wide.at[:, HALO : HALO + cells_x, 0:cells_y], in_sem.at[0]),
        pltpu.make_async_copy(forc_hbm, static.at[0:3, 2 : 2 + cells_x, 0:cells_y], in_sem.at[0]),
        pltpu.make_async_copy(visc_hbm, static.at[3, 2 : 2 + cells_x, 0:cells_y], in_sem.at[0]),
        pltpu.make_async_copy(hval_hbm, hist.at[:, :, HALO : HALO + cells_x, 0:cells_y], in_sem.at[1]),
        pltpu.make_async_copy(hres_hbm, fres, in_sem.at[2]),
        pltpu.make_async_copy(rp_hbm, past_res, in_sem.at[2]),
        pltpu.make_async_copy(gp_hbm, past_val, in_sem.at[2]),
    ]
    for load in loads[:4]:
        load.start()
    barrier = pltpu.get_barrier_semaphore()
    for k in range(1, count_y):
        pl.semaphore_signal(
            barrier, inc=1, device_id=(me_x, lax.rem(me_y + k, count_y)), device_id_type=MESH
        )
    for k in range(2, count_x):

        @pl.when(me_x + k < count_x)
        def _():
            pl.semaphore_signal(barrier, inc=1, device_id=(me_x + k, me_y), device_id_type=MESH)

    total = count_y - 1 + jnp.maximum(me_x - 1, 0)
    for sx, sy in DIRS[:2] + DIRS[4:]:
        here = exists(sx, sy)
        total = total + jnp.where(here, 1, 0)

        @pl.when(here)
        def _():
            pl.semaphore_signal(
                barrier, inc=1, device_id=(me_x + sx, me_y + sy), device_id_type=MESH
            )

    def clear(ref, off):
        lead = (slice(None),) * (len(ref.shape) - 3)
        for (sx, sy), part in (
            ((-1, 0), (slice(0, off), slice(None))),
            ((1, 0), (slice(off + cells_x, 2 * off + cells_x), slice(None))),
            ((0, -1), (slice(None), slice(rows - off, rows))),
            ((0, 1), (slice(None), slice(cells_y, cells_y + off))),
        ):

            @pl.when(jnp.logical_not(exists(sx, sy)))
            def _():
                where = lead + part
                ref[where] = jnp.zeros(ref.at[where].shape, jnp.float32)

    clear(wide, HALO)
    clear(static, HALO - 1)
    with jax.named_scope("barrier"):
        pl.semaphore_wait(barrier, total)

    def span_x(sx, off, deep, skip=0):
        if sx == 0:
            return (slice(off, off + cells_x),) * 2
        if sx < 0:
            return slice(off + skip, off + deep), slice(off + cells_x + skip, off + cells_x + deep)
        return slice(off + cells_x - deep, off + cells_x - skip), slice(off - deep, off - skip)

    def span_y(sy, deep, skip=0):
        if sy == 0:
            return (slice(0, cells_y),) * 2
        if sy < 0:
            return slice(skip, deep), slice(cells_y + skip, cells_y + deep)
        return slice(cells_y - deep, cells_y - skip), slice(rows - deep, rows - skip)

    def faces(ref, off, dirs):
        pieces = []
        for sx, sy in dirs:
            deep = off if sx == 0 or sy == 0 else off - 1
            pieces.append((ref, (sx, sy), 0, span_x(sx, off, deep), span_y(sy, deep)))
        return pieces

    def layer(ref, off, deep, skip, sy):
        return [(ref, (0, sy), 0, span_x(0, off, 0), span_y(sy, deep, skip))]

    def corners(ref, off, side):
        deep = off - 1
        part = slice(cells_y, cells_y + deep) if side > 0 else slice(rows - deep, rows)
        return [(ref, (sx, 0), side, span_x(sx, off, deep), (part, part)) for sx in (-1, 1)]

    def length(part):
        return part.stop - part.start

    def size_of(piece):
        ref, _, _, (src_x, _), (src_y, _) = piece
        size = length(src_x) * length(src_y)
        for extent in ref.shape[:-3]:
            size = size * extent
        return size

    def places(me, count):
        if count == 1:
            return [((0, 0), None)]
        ends = [((0, 1), me == 0), ((1, 0), me == count - 1)]
        return ends + [((1, 1), both(me > 0, me < count - 1))] if count > 2 else ends

    def settle(pieces, sem, sending, more=0):
        for sides_x, here_x in places(me_x, count_x):
            for sides_y, here_y in places(me_y, count_y):
                size = more
                for piece in pieces:
                    _, (sx, sy), side, _, _ = piece
                    there = 1
                    for step, sides in ((sx, sides_x), (sy, sides_y)):
                        if step != 0:
                            there = there * sides[step > 0 if sending else step < 0]
                    if side != 0:
                        there = there * sides_y[side > 0]
                    size = size + there * size_of(piece)
                if sending and relayed and sides_y != (1, 1):
                    near, far = fields["north"][1][0], fields["far"][1][0]
                    size = size + size_of(near) * (depth - straight) // depth + size_of(far)
                if size == 0:
                    continue
                part = ruler.at[0:size]
                copy = pltpu.make_async_remote_copy(
                    src_ref=part,
                    dst_ref=part,
                    send_sem=sem,
                    recv_sem=sem,
                    device_id={"gx": lax.rem(me_x + 1, count_x)},
                    device_id_type=MESH,
                )
                here = [h for h in (here_x, here_y) if h is not None]

                @pl.when(functools.reduce(both, here))
                def _():
                    if sending:
                        copy.wait_send()
                    else:
                        copy.wait_recv()

    fields = {
        "wide": (0, faces(wide, HALO, DIRS)),
        "static": (0, faces(static, HALO - 1, DIRS)),
        "north": (1, layer(hist, HALO, HALO - 1, 0, -1)),
        "south": (2, layer(hist, HALO, HALO - 1, 0, 1)),
        "across": (3, faces(hist, HALO, DIRS[:2])),
        "far": (3, layer(hist, HALO, HALO, HALO - 1, -1) + layer(hist, HALO, HALO, HALO - 1, 1)),
        "turn_north": (3, corners(hist, HALO, 1)),
        "turn_south": (3, corners(hist, HALO, -1)),
        "late": (3, faces(late, HALO, DIRS)),
    }
    odd = lax.rem(me_y, 2) == 1
    even = jnp.logical_not(odd)

    relayed = count_y == 4
    turns = ((1, 1, 3, 2), (-1, 2, 0, 1))
    bands = {"north": (HALO - 1, 0, 1), "south": (HALO - 1, 0, 1), "far": (HALO, HALO - 1, 0)}
    straight = depth - (4 * depth) // 5

    def start(name, piece):
        which = fields[name][0]
        ref, (sx, sy), side, (src_x, dst_x), (src_y, dst_y) = piece
        here = exists(sx, sy)
        if side != 0:
            here = both(here, exists(0, side))
        lead = (slice(None),) * (len(ref.shape) - 3)

        def go(lead):
            pltpu.make_async_remote_copy(
                src_ref=ref.at[lead + (src_x, src_y)],
                dst_ref=ref.at[lead + (dst_x, dst_y)],
                send_sem=send_sem,
                recv_sem=recv_sem.at[which],
                device_id=(me_x + sx, me_y + sy),
                device_id_type=MESH,
            ).start()

        if relayed and name in bands:
            turned = me_y == (1 if sy > 0 else 2)
            if bands[name][2]:

                @pl.when(turned)
                def _():
                    go((slice(0, straight), slice(None)))

            here = both(here, jnp.logical_not(turned))

        @pl.when(here)
        def _():
            go(lead)

    middle = (straight + depth) // 2
    groups = {True: (slice(straight, middle), slice(middle, depth)), False: (slice(0, depth),)}

    def passed(name, device, sy, stage, which):
        deep, skip, part = bands[name]
        src_y, dst_y = span_y(sy, deep, skip)
        group = groups[part == 1][which]
        inside = slice(HALO, HALO + cells_x)
        kept = passing.at[group, :, :, skip:deep]
        src = hist.at[group, :, inside, src_y] if stage == 0 else kept
        dst = kept if stage < 2 else hist.at[group, :, inside, dst_y]
        return pltpu.make_async_remote_copy(
            src_ref=src,
            dst_ref=dst,
            send_sem=send_sem,
            recv_sem=recv_sem.at[fields[name][0] if stage == 2 else 4 + which if part else 6],
            device_id=device,
            device_id_type=MESH,
        )

    def detour(names):
        for name, (sy, owner, relay, _) in zip(names, turns if relayed else ()):

            @pl.when(me_y == owner)
            def _():
                for which in range(len(groups[bands[name][2] == 1])):
                    passed(name, (me_x, relay), sy, 0, which).start()

    def pass_on(names):
        for name, (sy, _, relay, target) in zip(names, turns if relayed else ()):

            @pl.when(me_y == relay)
            def _():
                for which in range(len(groups[bands[name][2] == 1])):
                    passed(name, (me_x, target), sy, 1, which).wait_recv()
                    passed(name, (me_x, target), sy, 2, which).start()

    def send(*names):
        for name in names:
            for piece in fields[name][1]:
                start(name, piece)

    def send_in_turn(*names):
        for here, first in ((odd, 1), (even, -1)):

            @pl.when(here)
            def _():
                for sy, kinds in ((first, (1, 0)), (0, (1,)), (-first, (1, 0))):
                    for kind in kinds:
                        for name in names:
                            for piece in fields[name][1]:
                                if piece[1][1] == sy and (piece[1][0] != 0) == (kind == 1):
                                    start(name, piece)

    def receive(which):
        pieces = [p for number, group in fields.values() if number == which for p in group]
        with jax.named_scope("recv" + str(which)):
            settle(pieces, recv_sem.at[which], False)

    def turn(which, name):
        receive(which)
        send(name)

    def along(slots, idx, k, sends, recvs, me, count, axis):
        return pltpu.make_async_remote_copy(
            src_ref=slots.at[idx, me],
            dst_ref=slots.at[idx, me],
            send_sem=sends.at[idx],
            recv_sem=recvs.at[idx],
            device_id={axis: lax.rem(me + k, count)},
            device_id_type=MESH,
        )

    count_all = count_x * count_y
    me_all = me_x * count_y + me_y
    if direct:
        slots_all, all_sem = shared
    else:
        slots_y, slots_x, ysend, yrecv, xsend, xrecv = shared
        lines = (
            (slots_y, ysend, yrecv, me_y, count_y, "gy"),
            (slots_x, xsend, xrecv, me_x, count_x, "gx"),
        )

    def spread(line, idx, row):
        slots, sends, recvs, me, count, axis = line
        slots[idx, me] = row
        for k in range(1, count):
            along(slots, idx, k, sends, recvs, me, count, axis).start()

    def whole(line, idx):
        slots, sends, recvs, me, count, axis = line
        part = slots.at[idx, 0 : count - 1]
        return pltpu.make_async_remote_copy(
            src_ref=part,
            dst_ref=part,
            send_sem=sends.at[idx],
            recv_sem=recvs.at[idx],
            device_id={axis: lax.rem(me + 1, count)},
            device_id_type=MESH,
        )

    def gather(line, idx):
        slots, sends, recvs, me, count, axis = line
        whole(line, idx).wait_recv()
        total = slots[idx, 0]
        for k in range(1, count):
            total = total + slots[idx, k]
        return total

    def others(me, count):
        order = []
        for k in range(count - 1):
            order.append(jnp.where(k >= me, k + 1, k))
        return order

    if direct:
        far_x, far_y = others(me_x, count_x), others(me_y, count_y)
        ranked = [(kx + 2 * ky, x, y) for kx, x in enumerate(far_x) for ky, y in enumerate(far_y)]
        ranked += [(kx + 2 * count_y, x, me_y) for kx, x in enumerate(far_x)]
        ranked += [(count_x + 2 * ky, me_x, y) for ky, y in enumerate(far_y)]
        peers = [(x, y) for _, x, y in sorted(ranked, key=lambda entry: entry[0])]

    def give(idx, row):
        if not direct:
            spread(lines[1], idx, row)
            return
        slots_all[idx, me_all] = row
        for peer in peers:
            pltpu.make_async_remote_copy(
                src_ref=slots_all.at[idx, me_all],
                dst_ref=slots_all.at[idx, me_all],
                send_sem=send_sem,
                recv_sem=all_sem.at[idx],
                device_id=peer,
                device_id_type=MESH,
            ).start()

    def halfway(idx):
        if not direct:
            spread(lines[0], idx, gather(lines[1], idx))

    def take(idx):
        if not direct:
            return gather(lines[0], idx)
        part = ruler.at[0 : count_all - 1]
        with jax.named_scope("take" + str(idx)):
            pltpu.make_async_remote_copy(
                src_ref=part,
                dst_ref=part,
                send_sem=all_sem.at[idx],
                recv_sem=all_sem.at[idx],
                device_id={"gx": lax.rem(me_x + 1, count_x)},
                device_id_type=MESH,
            ).wait_recv()
        return jnp.sum(slots_all[idx], axis=0)

    lane = lax.broadcasted_iota(jnp.int32, (cells_y, lanes), 1)

    def packed(parts):
        row = jnp.zeros((cells_y, lanes), jnp.float32)
        for j, part in enumerate(parts):
            row = jnp.where(lane == j, jnp.sum(part, axis=1, keepdims=True), row)
        return jnp.sum(row, axis=0, keepdims=True)

    def unpacked(row, count):
        return [jnp.broadcast_to(row[:, j : j + 1], (cells_y, lanes)) for j in range(count)]

    own = [(c, x) for c in range(3) for x in range(cells_x)]

    def factored(gram):
        trace = gram[0][0]
        for j in range(1, depth):
            trace = trace + gram[j][j]
        shift = (REG / depth) * trace + FLOOR * entries
        lower = [[None] * depth for _ in range(depth)]
        inverse = [None] * depth
        scaled = [[None] * depth for _ in range(depth)]
        for j in range(depth):
            pivot = gram[j][j] + shift
            for k in range(j):
                pivot = pivot - lower[j][k] * scaled[j][k]
            inverse[j] = 1.0 / pivot
            for i in range(j + 1, depth):
                value = gram[i][j]
                for k in range(j):
                    value = value - scaled[i][k] * lower[j][k]
                scaled[i][j] = value
                lower[i][j] = value * inverse[j]
        return lower, inverse

    def solved(factors, rhs):
        lower, inverse = factors
        part = list(rhs)
        for j in range(depth):
            for i in range(j + 1, depth):
                part[i] = part[i] - lower[i][j] * part[j]
        part = [p * inv for p, inv in zip(part, inverse)]
        for j in reversed(range(depth)):
            for i in range(j):
                part[i] = part[i] - lower[j][i] * part[j]
        return part

    zlane = lax.broadcasted_iota(jnp.int32, (rows, lanes), 1)
    has_below = jnp.where(zlane == 0, 0.0, 1.0)
    has_above = jnp.where(zlane == lanes - 1, 0.0, 1.0)

    def relax(src, dst, off, x, cut):
        cs = [coef[j, x + off][0:cut] for j in range(6)]
        for c in range(3):
            here = src(c, x)
            total = coef[6 + c, x + off][0:cut]
            total = total + cs[0] * src(c, x - 1)[0:cut] + cs[1] * src(c, x + 1)[0:cut]
            total = total + cs[2] * pltpu.roll(here, 1, 0)[0:cut]
            total = total + cs[3] * pltpu.roll(here, rows - 1, 0)[0:cut]
            total = total + cs[4] * pltpu.roll(here[0:cut], 1, 1)
            total = total + cs[5] * pltpu.roll(here[0:cut], lanes - 1, 1)
            dst(c, x, total)

    def picard(field, dst):
        for x in range(-2, cells_x + 2):
            cut = cells_y if x in (-2, cells_x + 1) else rows
            vel = [field[c, x + HALO, 0:cut] for c in range(3)]
            visc = static[3, x + 2, 0:cut]
            diag = 1.0 + 6.0 * visc + jnp.abs(vel[0]) + jnp.abs(vel[1]) + jnp.abs(vel[2])
            inv = 1.0 / diag
            for a in range(3):
                lo = (visc + jnp.maximum(vel[a], 0.0)) * inv
                hi = (visc - jnp.minimum(vel[a], 0.0)) * inv
                if a == 2:
                    lo, hi = lo * has_below[0:cut], hi * has_above[0:cut]
                coef[2 * a, x + 2, 0:cut] = lo
                coef[2 * a + 1, x + 2, 0:cut] = hi
            for c in range(3):
                coef[6 + c, x + 2, 0:cut] = (static[c, x + 2, 0:cut] + vel[c]) * inv

        def put(ref, off):
            def store(c, x, value):
                ref[c, x + off, 0 : value.shape[0]] = value

            return store

        for x in range(-2, cells_x + 2):
            cut = cells_y if x in (-2, cells_x + 1) else rows
            relax(lambda c, i: field[c, i + HALO], put(first, 2), 2, x, cut)
        for x in range(-1, cells_x + 1):
            cut = cells_y if x in (-1, cells_x) else rows
            relax(lambda c, i: first[c, i + 2], put(second, 1), 2, x, cut)
        for x in range(cells_x):
            relax(lambda c, i: second[c, i + 1], dst, 2, x, cells_y)

    if direct:
        for k in range(1, count_x):

            @pl.when(me_x >= k)
            def _():
                pl.semaphore_signal(gate, inc=1, device_id=(me_x - k, me_y), device_id_type=MESH)

        for k in range(1, count_y):
            pl.semaphore_signal(
                gate, inc=1, device_id=(me_x, lax.rem(me_y + k, count_y)), device_id_type=MESH
            )

    def loaded(which, *refs):
        size = 0
        for ref in refs:
            part = 1
            for extent in ref.shape[:-1]:
                part = part * extent
            size = size + part
        part = ruler.at[0:size]
        pltpu.make_async_copy(part, part, in_sem.at[which]).wait()

    loaded(0, vel_hbm, forc_hbm, visc_hbm)
    send_in_turn("wide", "static")
    for load in loads[4:]:
        load.start()
    loaded(1, hval_hbm)
    detour(("south", "north"))
    detour(("far", "far"))
    send_in_turn("north", "south")
    send("across")
    loaded(2, hres_hbm, rp_hbm, gp_hbm)

    pairs = [(i, j) for i in range(depth) for j in range(i + 1)]
    clear(hist, HALO)
    clear(late, HALO)
    sums = [None] * (len(pairs) + depth)

    def add(j, value):
        sums[j] = value if sums[j] is None else sums[j] + value

    for c, x in own:
        f = [fres[j, c, x] for j in range(depth)]
        r = past_res[c, x]
        for n, (i, j) in enumerate(pairs):
            add(n, f[i] * f[j])
        for j in range(depth):
            add(len(pairs) + j, f[j] * r)
    row = packed(sums)
    pass_on(("south", "north"))
    if direct:
        with jax.named_scope("gate"):
            pl.semaphore_wait(gate, count_x - 1 - me_x + count_y - 1)
    give(0, row)

    receive(0)

    def store_value(c, x, value):
        late[c, x + HALO, 0:cells_y] = value

    picard(wide, store_value)

    sums = [None] * (depth + 1)
    for c, x in own:
        resid = late[c, x + HALO, 0:cells_y] - wide[c, x + HALO, 0:cells_y]
        newest = resid - past_res[c, x]
        delta[c, x] = newest
        for j in range(depth):
            add(j, fres[j, c, x] * resid)
        add(depth, newest * newest)
    give(1, packed(sums))
    send_in_turn("late")
    send_in_turn("far")
    pass_on(("far", "far"))

    first_north = even if relayed else odd

    @pl.when(first_north)
    def _():
        turn(1, "turn_north")
        turn(2, "turn_south")

    @pl.when(jnp.logical_not(first_north))
    def _():
        turn(2, "turn_south")
        turn(1, "turn_north")

    halfway(0)
    halfway(1)

    early = unpacked(take(0), len(pairs) + depth)
    gram = [[None] * depth for _ in range(depth)]
    for n, (i, j) in enumerate(pairs):
        gram[i][j] = gram[j][i] = early[n]
    factors = factored(gram)
    for_rhs = unpacked(take(1), depth + 1)
    rhs, newest_sq = for_rhs[:depth], for_rhs[depth]
    gamma = solved(factors, rhs)
    receive(3)
    wide_gamma = [jnp.concatenate([g, g], 0) for g in gamma]
    for c in range(3):
        for x in range(cells_x + 2 * HALO):
            cut = cells_y if x in (0, cells_x + 2 * HALO - 1) else rows
            value = late[c, x, 0:cut]
            for j in range(depth):
                value = value - wide_gamma[j][0:cut] * hist[j, c, x, 0:cut]
            ahead[c, x, 0:cut] = value

    def store_out(c, x, value):
        out_ref[c, x] = value

    picard(ahead, store_out)

    sums = [None] * depth
    for c, x in own:
        resid = out_ref[c, x] - ahead[c, x + HALO, 0:cells_y]
        res_ref[c, x] = resid
        for j in range(1, depth):
            add(j - 1, fres[j, c, x] * resid)
        add(depth - 1, delta[c, x] * resid)
    give(2, packed(sums))

    gram2 = [[None] * depth for _ in range(depth)]
    for i in range(depth - 1):
        for j in range(depth - 1):
            gram2[i][j] = gram[i + 1][j + 1]
        cross = rhs[i + 1] - early[len(pairs) + i + 1]
        gram2[i][depth - 1] = gram2[depth - 1][i] = cross
    gram2[depth - 1][depth - 1] = newest_sq
    factors = factored(gram2)

    halfway(2)
    pieces = [piece for _, group in fields.values() for piece in group]
    settle(pieces, send_sem, True, 3 * (count_all - 1) if direct else 0)
    if not direct:
        for line in lines:
            for idx in range(3):
                whole(line, idx).wait_send()
    final = take(2)
    gamma = solved(factors, unpacked(final, depth))
    for c, x in own:
        value = out_ref[c, x]
        newest = late[c, x + HALO, 0:cells_y] - past_val[c, x]
        for j in range(1, depth):
            value = value - gamma[j - 1] * hist[j, c, x + HALO, 0:cells_y]
        out_ref[c, x] = value - gamma[depth - 1] * newest


def leave(vel_ref, res_ref, vel_hbm, res_hbm, sem):
    copies = [
        pltpu.make_async_copy(vel_ref, vel_hbm, sem.at[0]),
        pltpu.make_async_copy(res_ref, res_hbm, sem.at[1]),
    ]
    for copy in copies:
        copy.start()
    for copy in copies:
        copy.wait()


def local(velocity, forcing, viscosity, residual_prev, value_prev, hist_res, hist_val):
    depth, comps, cells_x, cells_y, lanes = hist_res.shape
    counts = (lax.axis_size("gx"), lax.axis_size("gy"))
    entries = 3.0 * cells_x * cells_y * lanes * counts[0] * counts[1]
    rows = 2 * cells_y
    count_all = counts[0] * counts[1]
    direct = count_all <= 64
    def vmem(*shape):
        return pltpu.VMEM(shape + (lanes,), jnp.float32)

    if direct:
        shared = [vmem(3, count_all, 1), pltpu.SemaphoreType.DMA((3,))]
    else:
        shared = [vmem(3, counts[1], 1), vmem(3, counts[0], 1)]
        shared += [pltpu.SemaphoreType.DMA((3,))] * 4
    length = 9 * (depth + 3) * (6 * (cells_x + cells_y) + 16) + 3 * count_all
    results = pl.pallas_call(
        functools.partial(kernel, counts, direct, entries),
        name="anderson",
        out_shape=(pltpu.VMEM(velocity.shape, jnp.float32),) * 2,
        in_specs=[pl.BlockSpec(memory_space=pl.ANY)] * 7,
        out_specs=(pl.BlockSpec(memory_space=pltpu.VMEM),) * 2,
        scratch_shapes=[
            vmem(3, cells_x + 6, rows),
            vmem(4, cells_x + 4, rows),
            vmem(depth, 3, cells_x + 6, rows),
            vmem(3, cells_x + 6, rows),
            vmem(3, cells_x + 6, rows),
            vmem(3, cells_x, cells_y),
            vmem(3, cells_x, cells_y),
            vmem(9, cells_x + 4, rows),
            vmem(3, cells_x + 4, rows),
            vmem(3, cells_x + 2, rows),
            vmem(depth, 3, cells_x, cells_y),
            vmem(3, cells_x, cells_y),
            vmem(depth, 3, cells_x, HALO),
            vmem(length, 1),
            pltpu.SemaphoreType.DMA((3,)),
            pltpu.SemaphoreType.DMA,
            pltpu.SemaphoreType.DMA((7,)),
            pltpu.SemaphoreType.REGULAR,
            *shared,
        ],
        compiler_params=pltpu.CompilerParams(collective_id=0, has_side_effects=True),
    )(velocity, forcing, viscosity, residual_prev, value_prev, hist_res, hist_val)
    return pl.pallas_call(
        leave,
        name="leave",
        out_shape=(jax.ShapeDtypeStruct(velocity.shape, jnp.float32),) * 2,
        in_specs=[pl.BlockSpec(memory_space=pl.ANY)] * 2,
        out_specs=(pl.BlockSpec(memory_space=pl.ANY),) * 2,
        scratch_shapes=[pltpu.SemaphoreType.DMA((2,))],
    )(*(pltpu.with_memory_space_constraint(r, pltpu.VMEM) for r in results))


def solution(mesh):
    field = P(None, "gx", "gy", None)
    history = P(None, None, "gx", "gy", None)
    return jax.shard_map(
        local,
        mesh=mesh,
        in_specs=(field, field, P("gx", "gy", None), field, field, history, history),
        out_specs=(field, field),
        check_vma=False,
    )
```

```python
import functools

import jax
import jax.numpy as jnp
from jax import lax
from jax.experimental import pallas as pl
from jax.experimental.pallas import tpu as pltpu
from jax.sharding import PartitionSpec as P

SWEEPS = 3
REG = 0.05
FLOOR = 0.001
MESH = pl.DeviceIdType.MESH
DIRS = ((-1, 0), (1, 0), (0, -1), (0, 1), (-1, -1), (-1, 1), (1, -1), (1, 1))
HALO = SWEEPS


def both(a, b):
    return jnp.logical_and(a, b)


def kernel(
    counts,
    direct,
    entries,
    vel_hbm, forc_hbm, visc_hbm, rp_hbm, gp_hbm, hres_hbm, hval_hbm,
    out_ref, res_ref,
    wide, static, hist, late, ahead, past_res, past_val, coef, first, second, fres, delta,
    passing, ruler, in_sem, send_sem, recv_sem, gate, *shared,
):
    depth, _, cells_x, cells_y, lanes = hres_hbm.shape
    count_x, count_y = counts
    me_x, me_y = lax.axis_index("gx"), lax.axis_index("gy")
    rows = 2 * cells_y

    def exists(sx, sy):
        ok = None
        for step, me, count in ((sx, me_x, count_x), (sy, me_y, count_y)):
            if step != 0:
                here = me > 0 if step < 0 else me < count - 1
                ok = here if ok is None else both(ok, here)
        return ok

    loads = [
        pltpu.make_async_copy(vel_hbm, wide.at[:, HALO : HALO + cells_x, 0:cells_y], in_sem.at[0]),
        pltpu.make_async_copy(forc_hbm, static.at[0:3, 2 : 2 + cells_x, 0:cells_y], in_sem.at[0]),
        pltpu.make_async_copy(visc_hbm, static.at[3, 2 : 2 + cells_x, 0:cells_y], in_sem.at[0]),
        pltpu.make_async_copy(hval_hbm, hist.at[:, :, HALO : HALO + cells_x, 0:cells_y], in_sem.at[1]),
        pltpu.make_async_copy(hres_hbm, fres, in_sem.at[2]),
        pltpu.make_async_copy(rp_hbm, past_res, in_sem.at[2]),
        pltpu.make_async_copy(gp_hbm, past_val, in_sem.at[2]),
    ]
    for load in loads[:4]:
        load.start()
    barrier = pltpu.get_barrier_semaphore()
    for k in range(1, count_y):
        pl.semaphore_signal(
            barrier, inc=1, device_id=(me_x, lax.rem(me_y + k, count_y)), device_id_type=MESH
        )
    for k in range(2, count_x):

        @pl.when(me_x + k < count_x)
        def _():
            pl.semaphore_signal(barrier, inc=1, device_id=(me_x + k, me_y), device_id_type=MESH)

    total = count_y - 1 + jnp.maximum(me_x - 1, 0)
    for sx, sy in DIRS[:2] + DIRS[4:]:
        here = exists(sx, sy)
        total = total + jnp.where(here, 1, 0)

        @pl.when(here)
        def _():
            pl.semaphore_signal(
                barrier, inc=1, device_id=(me_x + sx, me_y + sy), device_id_type=MESH
            )

    def clear(ref, off):
        lead = (slice(None),) * (len(ref.shape) - 3)
        for (sx, sy), part in (
            ((-1, 0), (slice(0, off), slice(None))),
            ((1, 0), (slice(off + cells_x, 2 * off + cells_x), slice(None))),
            ((0, -1), (slice(None), slice(rows - off, rows))),
            ((0, 1), (slice(None), slice(cells_y, cells_y + off))),
        ):

            @pl.when(jnp.logical_not(exists(sx, sy)))
            def _():
                where = lead + part
                ref[where] = jnp.zeros(ref.at[where].shape, jnp.float32)

    clear(wide, HALO)
    clear(static, HALO - 1)
    with jax.named_scope("barrier"):
        pl.semaphore_wait(barrier, total)

    def span_x(sx, off, deep, skip=0):
        if sx == 0:
            return (slice(off, off + cells_x),) * 2
        if sx < 0:
            return slice(off + skip, off + deep), slice(off + cells_x + skip, off + cells_x + deep)
        return slice(off + cells_x - deep, off + cells_x - skip), slice(off - deep, off - skip)

    def span_y(sy, deep, skip=0):
        if sy == 0:
            return (slice(0, cells_y),) * 2
        if sy < 0:
            return slice(skip, deep), slice(cells_y + skip, cells_y + deep)
        return slice(cells_y - deep, cells_y - skip), slice(rows - deep, rows - skip)

    def faces(ref, off, dirs):
        pieces = []
        for sx, sy in dirs:
            if sx == 0 or sy == 0:
                pieces.append((ref, (sx, sy), 0, span_x(sx, off, off), span_y(sy, off)))
            for deep in range(1, off) if sx != 0 and sy != 0 else ():
                at_x, at_y = span_x(sx, off, deep, deep - 1), span_y(sy, off - deep)
                pieces.append((ref, (sx, sy), 0, at_x, at_y))
        return pieces

    def layer(ref, off, deep, skip, sy):
        return [(ref, (0, sy), 0, span_x(0, off, 0), span_y(sy, deep, skip))]

    def corners(ref, off, side):
        deep = off - 1
        part = slice(cells_y, cells_y + deep) if side > 0 else slice(rows - deep, rows)
        return [(ref, (sx, 0), side, span_x(sx, off, deep), (part, part)) for sx in (-1, 1)]

    def length(part):
        return part.stop - part.start

    def size_of(piece):
        ref, _, _, (src_x, _), (src_y, _) = piece
        size = length(src_x) * length(src_y)
        for extent in ref.shape[:-3]:
            size = size * extent
        return size

    def places(me, count):
        if count == 1:
            return [((0, 0), None)]
        ends = [((0, 1), me == 0), ((1, 0), me == count - 1)]
        return ends + [((1, 1), both(me > 0, me < count - 1))] if count > 2 else ends

    def settle(pieces, sem, sending, more=0):
        for sides_x, here_x in places(me_x, count_x):
            for sides_y, here_y in places(me_y, count_y):
                size = more
                for piece in pieces:
                    _, (sx, sy), side, _, _ = piece
                    there = 1
                    for step, sides in ((sx, sides_x), (sy, sides_y)):
                        if step != 0:
                            there = there * sides[step > 0 if sending else step < 0]
                    if side != 0:
                        there = there * sides_y[side > 0]
                    size = size + there * size_of(piece)
                if sending and relayed and sides_y != (1, 1):
                    near, far = fields["north"][1][0], fields["far"][1][0]
                    size = size + size_of(near) * (depth - straight) // depth + size_of(far)
                if size == 0:
                    continue
                part = ruler.at[0:size]
                copy = pltpu.make_async_remote_copy(
                    src_ref=part,
                    dst_ref=part,
                    send_sem=sem,
                    recv_sem=sem,
                    device_id={"gx": lax.rem(me_x + 1, count_x)},
                    device_id_type=MESH,
                )
                here = [h for h in (here_x, here_y) if h is not None]

                @pl.when(functools.reduce(both, here))
                def _():
                    if sending:
                        copy.wait_send()
                    else:
                        copy.wait_recv()

    fields = {
        "wide": (0, faces(wide, HALO, DIRS)),
        "static": (0, faces(static, HALO - 1, DIRS)),
        "north": (1, layer(hist, HALO, HALO - 1, 0, -1)),
        "south": (2, layer(hist, HALO, HALO - 1, 0, 1)),
        "across": (3, faces(hist, HALO, DIRS[:2])),
        "far": (3, layer(hist, HALO, HALO, HALO - 1, -1) + layer(hist, HALO, HALO, HALO - 1, 1)),
        "turn_north": (3, corners(hist, HALO, 1)),
        "turn_south": (3, corners(hist, HALO, -1)),
        "late": (3, faces(late, HALO, DIRS)),
    }
    odd = lax.rem(me_y, 2) == 1
    even = jnp.logical_not(odd)

    relayed = count_y == 4
    turns = ((1, 1, 3, 2), (-1, 2, 0, 1))
    bands = {"north": (HALO - 1, 0, 1), "south": (HALO - 1, 0, 1), "far": (HALO, HALO - 1, 0)}
    straight = depth - (4 * depth) // 5

    def start(name, piece):
        which = fields[name][0]
        ref, (sx, sy), side, (src_x, dst_x), (src_y, dst_y) = piece
        here = exists(sx, sy)
        if side != 0:
            here = both(here, exists(0, side))
        lead = (slice(None),) * (len(ref.shape) - 3)

        def go(lead):
            pltpu.make_async_remote_copy(
                src_ref=ref.at[lead + (src_x, src_y)],
                dst_ref=ref.at[lead + (dst_x, dst_y)],
                send_sem=send_sem,
                recv_sem=recv_sem.at[which],
                device_id=(me_x + sx, me_y + sy),
                device_id_type=MESH,
            ).start()

        if relayed and name in bands:
            turned = me_y == (1 if sy > 0 else 2)
            if bands[name][2]:

                @pl.when(turned)
                def _():
                    go((slice(0, straight), slice(None)))

            here = both(here, jnp.logical_not(turned))

        @pl.when(here)
        def _():
            go(lead)

    middle = (straight + depth) // 2
    groups = {True: (slice(straight, middle), slice(middle, depth)), False: (slice(0, depth),)}

    def passed(name, device, sy, stage, which):
        deep, skip, part = bands[name]
        src_y, dst_y = span_y(sy, deep, skip)
        group = groups[part == 1][which]
        inside = slice(HALO, HALO + cells_x)
        kept = passing.at[group, :, :, skip:deep]
        src = hist.at[group, :, inside, src_y] if stage == 0 else kept
        dst = kept if stage < 2 else hist.at[group, :, inside, dst_y]
        return pltpu.make_async_remote_copy(
            src_ref=src,
            dst_ref=dst,
            send_sem=send_sem,
            recv_sem=recv_sem.at[fields[name][0] if stage == 2 else 4 + which if part else 6],
            device_id=device,
            device_id_type=MESH,
        )

    def detour(names):
        for name, (sy, owner, relay, _) in zip(names, turns if relayed else ()):

            @pl.when(me_y == owner)
            def _():
                for which in range(len(groups[bands[name][2] == 1])):
                    passed(name, (me_x, relay), sy, 0, which).start()

    def pass_on(names):
        for name, (sy, _, relay, target) in zip(names, turns if relayed else ()):

            @pl.when(me_y == relay)
            def _():
                for which in range(len(groups[bands[name][2] == 1])):
                    passed(name, (me_x, target), sy, 1, which).wait_recv()
                    passed(name, (me_x, target), sy, 2, which).start()

    def send(*names):
        for name in names:
            for piece in fields[name][1]:
                start(name, piece)

    def only(here):
        def run(body):
            lax.fori_loop(0, jnp.where(here, 1, 0), lambda i, c: (body(), c)[1], 0)

        return run

    def send_in_turn(*names):
        for here, first in ((odd, 1), (even, -1)):

            @only(here)
            def _():
                for sy, kinds in ((first, (1, 0)), (0, (1,)), (-first, (1, 0))):
                    for kind in kinds:
                        for name in names:
                            for piece in fields[name][1]:
                                if piece[1][1] == sy and (piece[1][0] != 0) == (kind == 1):
                                    start(name, piece)

    def receive(which):
        pieces = [p for number, group in fields.values() if number == which for p in group]
        with jax.named_scope("recv" + str(which)):
            settle(pieces, recv_sem.at[which], False)

    def turn(which, name):
        receive(which)
        send(name)

    def along(slots, idx, k, sends, recvs, me, count, axis):
        return pltpu.make_async_remote_copy(
            src_ref=slots.at[idx, me],
            dst_ref=slots.at[idx, me],
            send_sem=sends.at[idx],
            recv_sem=recvs.at[idx],
            device_id={axis: lax.rem(me + k, count)},
            device_id_type=MESH,
        )

    count_all = count_x * count_y
    me_all = me_x * count_y + me_y
    if direct:
        slots_all, all_sem = shared
    else:
        slots_y, slots_x, ysend, yrecv, xsend, xrecv = shared
        lines = (
            (slots_y, ysend, yrecv, me_y, count_y, "gy"),
            (slots_x, xsend, xrecv, me_x, count_x, "gx"),
        )

    def spread(line, idx, row):
        slots, sends, recvs, me, count, axis = line
        slots[idx, me] = row
        for k in range(1, count):
            along(slots, idx, k, sends, recvs, me, count, axis).start()

    def whole(line, idx):
        slots, sends, recvs, me, count, axis = line
        part = slots.at[idx, 0 : count - 1]
        return pltpu.make_async_remote_copy(
            src_ref=part,
            dst_ref=part,
            send_sem=sends.at[idx],
            recv_sem=recvs.at[idx],
            device_id={axis: lax.rem(me + 1, count)},
            device_id_type=MESH,
        )

    def gather(line, idx):
        slots, sends, recvs, me, count, axis = line
        whole(line, idx).wait_recv()
        total = slots[idx, 0]
        for k in range(1, count):
            total = total + slots[idx, k]
        return total

    def others(me, count):
        order = []
        for k in range(count - 1):
            order.append(jnp.where(k >= me, k + 1, k))
        return order

    if direct:
        far_x, far_y = others(me_x, count_x), others(me_y, count_y)
        ranked = [(kx + 2 * ky, x, y) for kx, x in enumerate(far_x) for ky, y in enumerate(far_y)]
        ranked += [(kx + 2 * count_y, x, me_y) for kx, x in enumerate(far_x)]
        ranked += [(count_x + 2 * ky, me_x, y) for ky, y in enumerate(far_y)]
        peers = [(x, y) for _, x, y in sorted(ranked, key=lambda entry: entry[0])]

    def give(idx, row):
        if not direct:
            spread(lines[1], idx, row)
            return
        slots_all[idx, me_all] = row
        for peer in peers:
            pltpu.make_async_remote_copy(
                src_ref=slots_all.at[idx, me_all],
                dst_ref=slots_all.at[idx, me_all],
                send_sem=send_sem,
                recv_sem=all_sem.at[idx],
                device_id=peer,
                device_id_type=MESH,
            ).start()

    def halfway(idx):
        if not direct:
            spread(lines[0], idx, gather(lines[1], idx))

    def take(idx):
        if not direct:
            return gather(lines[0], idx)
        part = ruler.at[0 : count_all - 1]
        with jax.named_scope("take" + str(idx)):
            pltpu.make_async_remote_copy(
                src_ref=part,
                dst_ref=part,
                send_sem=all_sem.at[idx],
                recv_sem=all_sem.at[idx],
                device_id={"gx": lax.rem(me_x + 1, count_x)},
                device_id_type=MESH,
            ).wait_recv()
        return jnp.sum(slots_all[idx], axis=0)

    lane = lax.broadcasted_iota(jnp.int32, (cells_y, lanes), 1)

    def packed(parts):
        row = jnp.zeros((cells_y, lanes), jnp.float32)
        for j, part in enumerate(parts):
            row = jnp.where(lane == j, jnp.sum(part, axis=1, keepdims=True), row)
        return jnp.sum(row, axis=0, keepdims=True)

    def unpacked(row, count):
        return [jnp.broadcast_to(row[:, j : j + 1], (cells_y, lanes)) for j in range(count)]

    own = [(c, x) for c in range(3) for x in range(cells_x)]

    def factored(gram):
        trace = gram[0][0]
        for j in range(1, depth):
            trace = trace + gram[j][j]
        shift = (REG / depth) * trace + FLOOR * entries
        lower = [[None] * depth for _ in range(depth)]
        inverse = [None] * depth
        scaled = [[None] * depth for _ in range(depth)]
        for j in range(depth):
            pivot = gram[j][j] + shift
            for k in range(j):
                pivot = pivot - lower[j][k] * scaled[j][k]
            inverse[j] = 1.0 / pivot
            for i in range(j + 1, depth):
                value = gram[i][j]
                for k in range(j):
                    value = value - scaled[i][k] * lower[j][k]
                scaled[i][j] = value
                lower[i][j] = value * inverse[j]
        return lower, inverse

    def solved(factors, rhs):
        lower, inverse = factors
        part = list(rhs)
        for j in range(depth):
            for i in range(j + 1, depth):
                part[i] = part[i] - lower[i][j] * part[j]
        part = [p * inv for p, inv in zip(part, inverse)]
        for j in reversed(range(depth)):
            for i in range(j):
                part[i] = part[i] - lower[j][i] * part[j]
        return part

    zlane = lax.broadcasted_iota(jnp.int32, (rows, lanes), 1)
    has_below = jnp.where(zlane == 0, 0.0, 1.0)
    has_above = jnp.where(zlane == lanes - 1, 0.0, 1.0)

    def relax(src, dst, off, x, cut):
        cs = [coef[j, x + off][0:cut] for j in range(6)]
        for c in range(3):
            here = src(c, x)
            total = coef[6 + c, x + off][0:cut]
            total = total + cs[0] * src(c, x - 1)[0:cut] + cs[1] * src(c, x + 1)[0:cut]
            total = total + cs[2] * pltpu.roll(here, 1, 0)[0:cut]
            total = total + cs[3] * pltpu.roll(here, rows - 1, 0)[0:cut]
            total = total + cs[4] * pltpu.roll(here[0:cut], 1, 1)
            total = total + cs[5] * pltpu.roll(here[0:cut], lanes - 1, 1)
            dst(c, x, total)

    def picard(field, dst):
        for x in range(-2, cells_x + 2):
            cut = cells_y if x in (-2, cells_x + 1) else rows
            vel = [field[c, x + HALO, 0:cut] for c in range(3)]
            visc = static[3, x + 2, 0:cut]
            diag = 1.0 + 6.0 * visc + jnp.abs(vel[0]) + jnp.abs(vel[1]) + jnp.abs(vel[2])
            inv = 1.0 / diag
            for a in range(3):
                lo = (visc + jnp.maximum(vel[a], 0.0)) * inv
                hi = (visc - jnp.minimum(vel[a], 0.0)) * inv
                if a == 2:
                    lo, hi = lo * has_below[0:cut], hi * has_above[0:cut]
                coef[2 * a, x + 2, 0:cut] = lo
                coef[2 * a + 1, x + 2, 0:cut] = hi
            for c in range(3):
                coef[6 + c, x + 2, 0:cut] = (static[c, x + 2, 0:cut] + vel[c]) * inv

        def put(ref, off):
            def store(c, x, value):
                ref[c, x + off, 0 : value.shape[0]] = value

            return store

        for x in range(-2, cells_x + 2):
            cut = cells_y if x in (-2, cells_x + 1) else rows
            relax(lambda c, i: field[c, i + HALO], put(first, 2), 2, x, cut)
        for x in range(-1, cells_x + 1):
            cut = cells_y if x in (-1, cells_x) else rows
            relax(lambda c, i: first[c, i + 2], put(second, 1), 2, x, cut)
        for x in range(cells_x):
            relax(lambda c, i: second[c, i + 1], dst, 2, x, cells_y)

    def loaded(which, *refs):
        size = 0
        for ref in refs:
            part = 1
            for extent in ref.shape[:-1]:
                part = part * extent
            size = size + part
        part = ruler.at[0:size]
        pltpu.make_async_copy(part, part, in_sem.at[which]).wait()

    loaded(0, vel_hbm, forc_hbm, visc_hbm)
    send_in_turn("wide", "static")
    for load in loads[4:]:
        load.start()
    if direct:
        for k in range(1, count_x):

            @pl.when(me_x >= k)
            def _():
                pl.semaphore_signal(gate, inc=1, device_id=(me_x - k, me_y), device_id_type=MESH)

        for k in range(1, count_y):
            pl.semaphore_signal(
                gate, inc=1, device_id=(me_x, lax.rem(me_y + k, count_y)), device_id_type=MESH
            )

    loaded(1, hval_hbm)
    detour(("south", "north"))
    detour(("far", "far"))
    send_in_turn("north", "south")
    send("across")
    loaded(2, hres_hbm, rp_hbm, gp_hbm)

    pairs = [(i, j) for i in range(depth) for j in range(i + 1)]
    clear(hist, HALO)
    clear(late, HALO)
    sums = [None] * (len(pairs) + depth)

    def add(j, value):
        sums[j] = value if sums[j] is None else sums[j] + value

    for c, x in own:
        f = [fres[j, c, x] for j in range(depth)]
        r = past_res[c, x]
        for n, (i, j) in enumerate(pairs):
            add(n, f[i] * f[j])
        for j in range(depth):
            add(len(pairs) + j, f[j] * r)
    row = packed(sums)
    pass_on(("south", "north"))
    if direct:
        with jax.named_scope("gate"):
            pl.semaphore_wait(gate, count_x - 1 - me_x + count_y - 1)
    give(0, row)

    receive(0)

    def store_value(c, x, value):
        late[c, x + HALO, 0:cells_y] = value

    picard(wide, store_value)

    sums = [None] * (depth + 1)
    for c, x in own:
        resid = late[c, x + HALO, 0:cells_y] - wide[c, x + HALO, 0:cells_y]
        newest = resid - past_res[c, x]
        delta[c, x] = newest
        for j in range(depth):
            add(j, fres[j, c, x] * resid)
        add(depth, newest * newest)
    give(1, packed(sums))
    send_in_turn("late")
    send_in_turn("far")
    pass_on(("far", "far"))

    first_north = even if relayed else odd

    @only(first_north)
    def _():
        turn(1, "turn_north")
        turn(2, "turn_south")

    @only(jnp.logical_not(first_north))
    def _():
        turn(2, "turn_south")
        turn(1, "turn_north")

    halfway(0)
    halfway(1)

    early = unpacked(take(0), len(pairs) + depth)
    gram = [[None] * depth for _ in range(depth)]
    for n, (i, j) in enumerate(pairs):
        gram[i][j] = gram[j][i] = early[n]
    factors = factored(gram)
    for_rhs = unpacked(take(1), depth + 1)
    rhs, newest_sq = for_rhs[:depth], for_rhs[depth]
    gamma = solved(factors, rhs)
    receive(3)
    wide_gamma = [jnp.concatenate([g, g], 0) for g in gamma]
    for c in range(3):
        for x in range(cells_x + 2 * HALO):
            cut = cells_y if x in (0, cells_x + 2 * HALO - 1) else rows
            value = late[c, x, 0:cut]
            for j in range(depth):
                value = value - wide_gamma[j][0:cut] * hist[j, c, x, 0:cut]
            ahead[c, x, 0:cut] = value

    def store_out(c, x, value):
        out_ref[c, x] = value

    picard(ahead, store_out)

    sums = [None] * depth
    for c, x in own:
        resid = out_ref[c, x] - ahead[c, x + HALO, 0:cells_y]
        res_ref[c, x] = resid
        for j in range(1, depth):
            add(j - 1, fres[j, c, x] * resid)
        add(depth - 1, delta[c, x] * resid)
    give(2, packed(sums))

    gram2 = [[None] * depth for _ in range(depth)]
    for i in range(depth - 1):
        for j in range(depth - 1):
            gram2[i][j] = gram[i + 1][j + 1]
        cross = rhs[i + 1] - early[len(pairs) + i + 1]
        gram2[i][depth - 1] = gram2[depth - 1][i] = cross
    gram2[depth - 1][depth - 1] = newest_sq
    factors = factored(gram2)

    halfway(2)
    pieces = [piece for _, group in fields.values() for piece in group]
    settle(pieces, send_sem, True, 3 * (count_all - 1) if direct else 0)
    if not direct:
        for line in lines:
            for idx in range(3):
                whole(line, idx).wait_send()
    final = take(2)
    gamma = solved(factors, unpacked(final, depth))
    for c, x in own:
        value = out_ref[c, x]
        newest = late[c, x + HALO, 0:cells_y] - past_val[c, x]
        for j in range(1, depth):
            value = value - gamma[j - 1] * hist[j, c, x + HALO, 0:cells_y]
        out_ref[c, x] = value - gamma[depth - 1] * newest


def leave(vel_ref, res_ref, vel_hbm, res_hbm, sem):
    copies = [
        pltpu.make_async_copy(vel_ref, vel_hbm, sem.at[0]),
        pltpu.make_async_copy(res_ref, res_hbm, sem.at[1]),
    ]
    for copy in copies:
        copy.start()
    for copy in copies:
        copy.wait()


def local(velocity, forcing, viscosity, residual_prev, value_prev, hist_res, hist_val):
    depth, comps, cells_x, cells_y, lanes = hist_res.shape
    counts = (lax.axis_size("gx"), lax.axis_size("gy"))
    entries = 3.0 * cells_x * cells_y * lanes * counts[0] * counts[1]
    rows = 2 * cells_y
    count_all = counts[0] * counts[1]
    direct = count_all <= 64
    def vmem(*shape):
        return pltpu.VMEM(shape + (lanes,), jnp.float32)

    if direct:
        shared = [vmem(3, count_all, 1), pltpu.SemaphoreType.DMA((3,))]
    else:
        shared = [vmem(3, counts[1], 1), vmem(3, counts[0], 1)]
        shared += [pltpu.SemaphoreType.DMA((3,))] * 4
    length = 9 * (depth + 3) * (6 * (cells_x + cells_y) + 16) + 3 * count_all
    results = pl.pallas_call(
        functools.partial(kernel, counts, direct, entries),
        name="anderson",
        out_shape=(pltpu.VMEM(velocity.shape, jnp.float32),) * 2,
        in_specs=[pl.BlockSpec(memory_space=pl.ANY)] * 7,
        out_specs=(pl.BlockSpec(memory_space=pltpu.VMEM),) * 2,
        scratch_shapes=[
            vmem(3, cells_x + 6, rows),
            vmem(4, cells_x + 4, rows),
            vmem(depth, 3, cells_x + 6, rows),
            vmem(3, cells_x + 6, rows),
            vmem(3, cells_x + 6, rows),
            vmem(3, cells_x, cells_y),
            vmem(3, cells_x, cells_y),
            vmem(9, cells_x + 4, rows),
            vmem(3, cells_x + 4, rows),
            vmem(3, cells_x + 2, rows),
            vmem(depth, 3, cells_x, cells_y),
            vmem(3, cells_x, cells_y),
            vmem(depth, 3, cells_x, HALO),
            vmem(length, 1),
            pltpu.SemaphoreType.DMA((3,)),
            pltpu.SemaphoreType.DMA,
            pltpu.SemaphoreType.DMA((7,)),
            pltpu.SemaphoreType.REGULAR,
            *shared,
        ],
        compiler_params=pltpu.CompilerParams(collective_id=0, has_side_effects=True),
    )(velocity, forcing, viscosity, residual_prev, value_prev, hist_res, hist_val)
    return pl.pallas_call(
        leave,
        name="leave",
        out_shape=(jax.ShapeDtypeStruct(velocity.shape, jnp.float32),) * 2,
        in_specs=[pl.BlockSpec(memory_space=pl.ANY)] * 2,
        out_specs=(pl.BlockSpec(memory_space=pl.ANY),) * 2,
        scratch_shapes=[pltpu.SemaphoreType.DMA((2,))],
    )(*(pltpu.with_memory_space_constraint(r, pltpu.VMEM) for r in results))


def solution(mesh):
    field = P(None, "gx", "gy", None)
    history = P(None, None, "gx", "gy", None)
    return jax.shard_map(
        local,
        mesh=mesh,
        in_specs=(field, field, P("gx", "gy", None), field, field, history, history),
        out_specs=(field, field),
        check_vma=False,
    )
```

```python
import functools

import jax
import jax.numpy as jnp
from jax import lax
from jax.experimental import pallas as pl
from jax.experimental.pallas import tpu as pltpu
from jax.sharding import PartitionSpec as P

SWEEPS = 3
REG = 0.05
FLOOR = 0.001
MESH = pl.DeviceIdType.MESH
DIRS = ((-1, 0), (1, 0), (0, -1), (0, 1), (-1, -1), (-1, 1), (1, -1), (1, 1))
HALO = SWEEPS


def both(a, b):
    return jnp.logical_and(a, b)


def kernel(
    counts,
    direct,
    entries,
    vel_hbm, forc_hbm, visc_hbm, rp_hbm, gp_hbm, hres_hbm, hval_hbm,
    out_ref, res_ref,
    wide, static, hist, late, ahead, past_res, past_val, coef, first, second, fres, delta,
    passing, ruler, in_sem, send_sem, recv_sem, gate, *shared,
):
    depth, _, cells_x, cells_y, lanes = hres_hbm.shape
    count_x, count_y = counts
    me_x, me_y = lax.axis_index("gx"), lax.axis_index("gy")
    rows = 2 * cells_y

    def exists(sx, sy):
        ok = None
        for step, me, count in ((sx, me_x, count_x), (sy, me_y, count_y)):
            if step != 0:
                here = me > 0 if step < 0 else me < count - 1
                ok = here if ok is None else both(ok, here)
        return ok

    loads = [
        pltpu.make_async_copy(vel_hbm, wide.at[:, HALO : HALO + cells_x, 0:cells_y], in_sem.at[0]),
        pltpu.make_async_copy(forc_hbm, static.at[0:3, 2 : 2 + cells_x, 0:cells_y], in_sem.at[0]),
        pltpu.make_async_copy(visc_hbm, static.at[3, 2 : 2 + cells_x, 0:cells_y], in_sem.at[0]),
        pltpu.make_async_copy(hval_hbm, hist.at[:, :, HALO : HALO + cells_x, 0:cells_y], in_sem.at[1]),
        pltpu.make_async_copy(hres_hbm, fres, in_sem.at[2]),
        pltpu.make_async_copy(rp_hbm, past_res, in_sem.at[2]),
        pltpu.make_async_copy(gp_hbm, past_val, in_sem.at[2]),
    ]
    for load in loads[:4]:
        load.start()
    barrier = pltpu.get_barrier_semaphore()
    for k in range(1, count_y):
        pl.semaphore_signal(
            barrier, inc=1, device_id=(me_x, lax.rem(me_y + k, count_y)), device_id_type=MESH
        )
    for k in range(2, count_x):

        @pl.when(me_x + k < count_x)
        def _():
            pl.semaphore_signal(barrier, inc=1, device_id=(me_x + k, me_y), device_id_type=MESH)

    total = count_y - 1 + jnp.maximum(me_x - 1, 0)
    for sx, sy in DIRS[:2] + DIRS[4:]:
        here = exists(sx, sy)
        total = total + jnp.where(here, 1, 0)

        @pl.when(here)
        def _():
            pl.semaphore_signal(
                barrier, inc=1, device_id=(me_x + sx, me_y + sy), device_id_type=MESH
            )

    def clear(ref, off):
        lead = (slice(None),) * (len(ref.shape) - 3)
        for (sx, sy), part in (
            ((-1, 0), (slice(0, off), slice(None))),
            ((1, 0), (slice(off + cells_x, 2 * off + cells_x), slice(None))),
            ((0, -1), (slice(None), slice(rows - off, rows))),
            ((0, 1), (slice(None), slice(cells_y, cells_y + off))),
        ):

            @pl.when(jnp.logical_not(exists(sx, sy)))
            def _():
                where = lead + part
                ref[where] = jnp.zeros(ref.at[where].shape, jnp.float32)

    clear(wide, HALO)
    clear(static, HALO - 1)
    with jax.named_scope("barrier"):
        pl.semaphore_wait(barrier, total)

    def span_x(sx, off, deep, skip=0):
        if sx == 0:
            return (slice(off, off + cells_x),) * 2
        if sx < 0:
            return slice(off + skip, off + deep), slice(off + cells_x + skip, off + cells_x + deep)
        return slice(off + cells_x - deep, off + cells_x - skip), slice(off - deep, off - skip)

    def span_y(sy, deep, skip=0):
        if sy == 0:
            return (slice(0, cells_y),) * 2
        if sy < 0:
            return slice(skip, deep), slice(cells_y + skip, cells_y + deep)
        return slice(cells_y - deep, cells_y - skip), slice(rows - deep, rows - skip)

    def faces(ref, off, dirs):
        pieces = []
        for sx, sy in dirs:
            if sx == 0 or sy == 0:
                pieces.append((ref, (sx, sy), 0, span_x(sx, off, off), span_y(sy, off)))
            for deep in range(1, off) if sx != 0 and sy != 0 else ():
                at_x, at_y = span_x(sx, off, deep, deep - 1), span_y(sy, off - deep)
                pieces.append((ref, (sx, sy), 0, at_x, at_y))
        return pieces

    def layer(ref, off, deep, skip, sy):
        return [(ref, (0, sy), 0, span_x(0, off, 0), span_y(sy, deep, skip))]

    def corners(ref, off, side):
        deep = off - 1
        part = slice(cells_y, cells_y + deep) if side > 0 else slice(rows - deep, rows)
        return [(ref, (sx, 0), side, span_x(sx, off, deep), (part, part)) for sx in (-1, 1)]

    def length(part):
        return part.stop - part.start

    def size_of(piece):
        ref, _, _, (src_x, _), (src_y, _) = piece
        size = length(src_x) * length(src_y)
        for extent in ref.shape[:-3]:
            size = size * extent
        return size

    def places(me, count):
        if count == 1:
            return [((0, 0), None)]
        ends = [((0, 1), me == 0), ((1, 0), me == count - 1)]
        return ends + [((1, 1), both(me > 0, me < count - 1))] if count > 2 else ends

    def settle(pieces, sem, sending, more=0):
        for sides_x, here_x in places(me_x, count_x):
            for sides_y, here_y in places(me_y, count_y):
                size = more
                for piece in pieces:
                    _, (sx, sy), side, _, _ = piece
                    there = 1
                    for step, sides in ((sx, sides_x), (sy, sides_y)):
                        if step != 0:
                            there = there * sides[step > 0 if sending else step < 0]
                    if side != 0:
                        there = there * sides_y[side > 0]
                    size = size + there * size_of(piece)
                if sending and relayed and sides_y != (1, 1):
                    near, far = fields["north"][1][0], fields["far"][1][0]
                    size = size + size_of(near) * (depth - straight) // depth + size_of(far)
                if size == 0:
                    continue
                part = ruler.at[0:size]
                copy = pltpu.make_async_remote_copy(
                    src_ref=part,
                    dst_ref=part,
                    send_sem=sem,
                    recv_sem=sem,
                    device_id={"gx": lax.rem(me_x + 1, count_x)},
                    device_id_type=MESH,
                )
                here = [h for h in (here_x, here_y) if h is not None]

                @pl.when(functools.reduce(both, here))
                def _():
                    if sending:
                        copy.wait_send()
                    else:
                        copy.wait_recv()

    fields = {
        "wide": (0, faces(wide, HALO, DIRS)),
        "static": (0, faces(static, HALO - 1, DIRS)),
        "north": (1, layer(hist, HALO, HALO - 1, 0, -1)),
        "south": (2, layer(hist, HALO, HALO - 1, 0, 1)),
        "across": (3, faces(hist, HALO, DIRS[:2])),
        "far": (3, layer(hist, HALO, HALO, HALO - 1, -1) + layer(hist, HALO, HALO, HALO - 1, 1)),
        "turn_north": (3, corners(hist, HALO, 1)),
        "turn_south": (3, corners(hist, HALO, -1)),
        "late": (3, faces(late, HALO, DIRS)),
    }
    odd = lax.rem(me_y, 2) == 1
    even = jnp.logical_not(odd)

    relayed = count_y == 4
    turns = ((1, 1, 3, 2), (-1, 2, 0, 1))
    bands = {"north": (HALO - 1, 0, 1), "south": (HALO - 1, 0, 1), "far": (HALO, HALO - 1, 0)}
    straight = depth - (4 * depth) // 5

    def start(name, piece):
        which = fields[name][0]
        ref, (sx, sy), side, (src_x, dst_x), (src_y, dst_y) = piece
        here = exists(sx, sy)
        if side != 0:
            here = both(here, exists(0, side))
        lead = (slice(None),) * (len(ref.shape) - 3)

        def go(lead):
            pltpu.make_async_remote_copy(
                src_ref=ref.at[lead + (src_x, src_y)],
                dst_ref=ref.at[lead + (dst_x, dst_y)],
                send_sem=send_sem,
                recv_sem=recv_sem.at[which],
                device_id=(me_x + sx, me_y + sy),
                device_id_type=MESH,
            ).start()

        if relayed and name in bands:
            turned = me_y == (1 if sy > 0 else 2)
            if bands[name][2]:

                @pl.when(turned)
                def _():
                    go((slice(0, straight), slice(None)))

            here = both(here, jnp.logical_not(turned))

        @pl.when(here)
        def _():
            go(lead)

    middle = (straight + depth) // 2
    groups = {True: (slice(straight, middle), slice(middle, depth)), False: (slice(0, depth),)}

    def passed(name, device, sy, stage, which):
        deep, skip, part = bands[name]
        src_y, dst_y = span_y(sy, deep, skip)
        group = groups[part == 1][which]
        inside = slice(HALO, HALO + cells_x)
        kept = passing.at[group, :, :, skip:deep]
        src = hist.at[group, :, inside, src_y] if stage == 0 else kept
        dst = kept if stage < 2 else hist.at[group, :, inside, dst_y]
        return pltpu.make_async_remote_copy(
            src_ref=src,
            dst_ref=dst,
            send_sem=send_sem,
            recv_sem=recv_sem.at[fields[name][0] if stage == 2 else 4 + which if part else 6],
            device_id=device,
            device_id_type=MESH,
        )

    def detour(names):
        for name, (sy, owner, relay, _) in zip(names, turns if relayed else ()):

            @pl.when(me_y == owner)
            def _():
                for which in range(len(groups[bands[name][2] == 1])):
                    passed(name, (me_x, relay), sy, 0, which).start()

    def pass_on(names):
        for name, (sy, _, relay, target) in zip(names, turns if relayed else ()):

            @pl.when(me_y == relay)
            def _():
                for which in range(len(groups[bands[name][2] == 1])):
                    passed(name, (me_x, target), sy, 1, which).wait_recv()
                    passed(name, (me_x, target), sy, 2, which).start()

    def send(*names):
        for name in names:
            for piece in fields[name][1]:
                start(name, piece)

    def only(here):
        def run(body):
            lax.fori_loop(0, jnp.where(here, 1, 0), lambda i, c: (body(), c)[1], 0)

        return run

    def send_in_turn(*names):
        for here, first in ((odd, 1), (even, -1)):

            @only(here)
            def _():
                for sy, kinds in ((first, (1, 0)), (0, (1,)), (-first, (1, 0))):
                    for kind in kinds:
                        for name in names:
                            for piece in fields[name][1]:
                                if piece[1][1] == sy and (piece[1][0] != 0) == (kind == 1):
                                    start(name, piece)

    def receive(which):
        pieces = [p for number, group in fields.values() if number == which for p in group]
        with jax.named_scope("recv" + str(which)):
            settle(pieces, recv_sem.at[which], False)

    def turn(which, name):
        receive(which)
        send(name)

    def along(slots, idx, k, sends, recvs, me, count, axis):
        return pltpu.make_async_remote_copy(
            src_ref=slots.at[idx, me],
            dst_ref=slots.at[idx, me],
            send_sem=sends.at[idx],
            recv_sem=recvs.at[idx],
            device_id={axis: lax.rem(me + k, count)},
            device_id_type=MESH,
        )

    count_all = count_x * count_y
    me_all = me_x * count_y + me_y
    if direct:
        slots_all, all_sem = shared
    else:
        slots_y, slots_x, ysend, yrecv, xsend, xrecv = shared
        lines = (
            (slots_y, ysend, yrecv, me_y, count_y, "gy"),
            (slots_x, xsend, xrecv, me_x, count_x, "gx"),
        )

    def spread(line, idx, row):
        slots, sends, recvs, me, count, axis = line
        slots[idx, me] = row
        for k in range(1, count):
            along(slots, idx, k, sends, recvs, me, count, axis).start()

    def whole(line, idx):
        slots, sends, recvs, me, count, axis = line
        part = slots.at[idx, 0 : count - 1]
        return pltpu.make_async_remote_copy(
            src_ref=part,
            dst_ref=part,
            send_sem=sends.at[idx],
            recv_sem=recvs.at[idx],
            device_id={axis: lax.rem(me + 1, count)},
            device_id_type=MESH,
        )

    def gather(line, idx):
        slots, sends, recvs, me, count, axis = line
        whole(line, idx).wait_recv()
        total = slots[idx, 0]
        for k in range(1, count):
            total = total + slots[idx, k]
        return total

    def others(me, count, upward):
        order = []
        for k in range(count - 1):
            up = jnp.where(k >= me, k + 1, k)
            down = jnp.where(count - 1 - k <= me, count - 2 - k, count - 1 - k)
            order.append(up if upward else jnp.where(2 * me < count, down, up))
        return order

    def ranking(upward):
        far_x, far_y = others(me_x, count_x, upward), others(me_y, count_y, upward)
        ranked = [(kx + 2 * ky, x, y) for kx, x in enumerate(far_x) for ky, y in enumerate(far_y)]
        ranked += [(kx + 2 * count_y, x, me_y) for kx, x in enumerate(far_x)]
        ranked += [(count_x + 2 * ky, me_x, y) for ky, y in enumerate(far_y)]
        return [(x, y) for _, x, y in sorted(ranked, key=lambda entry: entry[0])]

    peers = [ranking(False), ranking(True)] if direct else None

    def give(idx, row):
        if not direct:
            spread(lines[1], idx, row)
            return
        slots_all[idx, me_all] = row
        for peer in peers[idx == 2]:
            pltpu.make_async_remote_copy(
                src_ref=slots_all.at[idx, me_all],
                dst_ref=slots_all.at[idx, me_all],
                send_sem=send_sem,
                recv_sem=all_sem.at[idx],
                device_id=peer,
                device_id_type=MESH,
            ).start()

    def halfway(idx):
        if not direct:
            spread(lines[0], idx, gather(lines[1], idx))

    def take(idx):
        if not direct:
            return gather(lines[0], idx)
        part = ruler.at[0 : count_all - 1]
        with jax.named_scope("take" + str(idx)):
            pltpu.make_async_remote_copy(
                src_ref=part,
                dst_ref=part,
                send_sem=all_sem.at[idx],
                recv_sem=all_sem.at[idx],
                device_id={"gx": lax.rem(me_x + 1, count_x)},
                device_id_type=MESH,
            ).wait_recv()
        return jnp.sum(slots_all[idx], axis=0)

    lane = lax.broadcasted_iota(jnp.int32, (cells_y, lanes), 1)

    def packed(parts):
        row = jnp.zeros((cells_y, lanes), jnp.float32)
        for j, part in enumerate(parts):
            row = jnp.where(lane == j, jnp.sum(part, axis=1, keepdims=True), row)
        return jnp.sum(row, axis=0, keepdims=True)

    def unpacked(row, count):
        return [jnp.broadcast_to(row[:, j : j + 1], (cells_y, lanes)) for j in range(count)]

    own = [(c, x) for c in range(3) for x in range(cells_x)]

    def factored(gram):
        trace = gram[0][0]
        for j in range(1, depth):
            trace = trace + gram[j][j]
        shift = (REG / depth) * trace + FLOOR * entries
        lower = [[None] * depth for _ in range(depth)]
        inverse = [None] * depth
        scaled = [[None] * depth for _ in range(depth)]
        for j in range(depth):
            pivot = gram[j][j] + shift
            for k in range(j):
                pivot = pivot - lower[j][k] * scaled[j][k]
            inverse[j] = 1.0 / pivot
            for i in range(j + 1, depth):
                value = gram[i][j]
                for k in range(j):
                    value = value - scaled[i][k] * lower[j][k]
                scaled[i][j] = value
                lower[i][j] = value * inverse[j]
        return lower, inverse

    def solved(factors, rhs):
        lower, inverse = factors
        part = list(rhs)
        for j in range(depth):
            for i in range(j + 1, depth):
                part[i] = part[i] - lower[i][j] * part[j]
        part = [p * inv for p, inv in zip(part, inverse)]
        for j in reversed(range(depth)):
            for i in range(j):
                part[i] = part[i] - lower[j][i] * part[j]
        return part

    zlane = lax.broadcasted_iota(jnp.int32, (rows, lanes), 1)
    has_below = jnp.where(zlane == 0, 0.0, 1.0)
    has_above = jnp.where(zlane == lanes - 1, 0.0, 1.0)

    def relax(src, dst, off, x, cut):
        cs = [coef[j, x + off][0:cut] for j in range(6)]
        for c in range(3):
            here = src(c, x)
            total = coef[6 + c, x + off][0:cut]
            total = total + cs[0] * src(c, x - 1)[0:cut] + cs[1] * src(c, x + 1)[0:cut]
            total = total + cs[2] * pltpu.roll(here, 1, 0)[0:cut]
            total = total + cs[3] * pltpu.roll(here, rows - 1, 0)[0:cut]
            total = total + cs[4] * pltpu.roll(here[0:cut], 1, 1)
            total = total + cs[5] * pltpu.roll(here[0:cut], lanes - 1, 1)
            dst(c, x, total)

    def picard(field, dst):
        for x in range(-2, cells_x + 2):
            cut = cells_y if x in (-2, cells_x + 1) else rows
            vel = [field[c, x + HALO, 0:cut] for c in range(3)]
            visc = static[3, x + 2, 0:cut]
            diag = 1.0 + 6.0 * visc + jnp.abs(vel[0]) + jnp.abs(vel[1]) + jnp.abs(vel[2])
            inv = 1.0 / diag
            for a in range(3):
                lo = (visc + jnp.maximum(vel[a], 0.0)) * inv
                hi = (visc - jnp.minimum(vel[a], 0.0)) * inv
                if a == 2:
                    lo, hi = lo * has_below[0:cut], hi * has_above[0:cut]
                coef[2 * a, x + 2, 0:cut] = lo
                coef[2 * a + 1, x + 2, 0:cut] = hi
            for c in range(3):
                coef[6 + c, x + 2, 0:cut] = (static[c, x + 2, 0:cut] + vel[c]) * inv

        def put(ref, off):
            def store(c, x, value):
                ref[c, x + off, 0 : value.shape[0]] = value

            return store

        for x in range(-2, cells_x + 2):
            cut = cells_y if x in (-2, cells_x + 1) else rows
            relax(lambda c, i: field[c, i + HALO], put(first, 2), 2, x, cut)
        for x in range(-1, cells_x + 1):
            cut = cells_y if x in (-1, cells_x) else rows
            relax(lambda c, i: first[c, i + 2], put(second, 1), 2, x, cut)
        for x in range(cells_x):
            relax(lambda c, i: second[c, i + 1], dst, 2, x, cells_y)

    def loaded(which, *refs):
        size = 0
        for ref in refs:
            part = 1
            for extent in ref.shape[:-1]:
                part = part * extent
            size = size + part
        part = ruler.at[0:size]
        pltpu.make_async_copy(part, part, in_sem.at[which]).wait()

    loaded(0, vel_hbm, forc_hbm, visc_hbm)
    send_in_turn("wide", "static")
    for load in loads[4:]:
        load.start()
    if direct:
        for k in range(1, count_x):

            @pl.when(me_x >= k)
            def _():
                pl.semaphore_signal(gate, inc=1, device_id=(me_x - k, me_y), device_id_type=MESH)

        for k in range(1, count_y):
            pl.semaphore_signal(
                gate, inc=1, device_id=(me_x, lax.rem(me_y + k, count_y)), device_id_type=MESH
            )

    loaded(1, hval_hbm)
    detour(("south", "north"))
    detour(("far", "far"))
    send_in_turn("north", "south")
    send("across")
    loaded(2, hres_hbm, rp_hbm, gp_hbm)

    pairs = [(i, j) for i in range(depth) for j in range(i + 1)]
    clear(hist, HALO)
    clear(late, HALO)
    sums = [None] * (len(pairs) + depth)

    def add(j, value):
        sums[j] = value if sums[j] is None else sums[j] + value

    for c, x in own:
        f = [fres[j, c, x] for j in range(depth)]
        r = past_res[c, x]
        for n, (i, j) in enumerate(pairs):
            add(n, f[i] * f[j])
        for j in range(depth):
            add(len(pairs) + j, f[j] * r)
    row = packed(sums)
    pass_on(("south", "north"))
    if direct:
        with jax.named_scope("gate"):
            pl.semaphore_wait(gate, count_x - 1 - me_x + count_y - 1)
    give(0, row)

    receive(0)

    def store_value(c, x, value):
        late[c, x + HALO, 0:cells_y] = value

    picard(wide, store_value)

    sums = [None] * (depth + 1)
    for c, x in own:
        resid = late[c, x + HALO, 0:cells_y] - wide[c, x + HALO, 0:cells_y]
        newest = resid - past_res[c, x]
        delta[c, x] = newest
        for j in range(depth):
            add(j, fres[j, c, x] * resid)
        add(depth, newest * newest)
    give(1, packed(sums))
    send_in_turn("late")
    send_in_turn("far")
    pass_on(("far", "far"))

    first_north = even if relayed else odd

    @only(first_north)
    def _():
        turn(1, "turn_north")
        turn(2, "turn_south")

    @only(jnp.logical_not(first_north))
    def _():
        turn(2, "turn_south")
        turn(1, "turn_north")

    halfway(0)
    halfway(1)

    early = unpacked(take(0), len(pairs) + depth)
    gram = [[None] * depth for _ in range(depth)]
    for n, (i, j) in enumerate(pairs):
        gram[i][j] = gram[j][i] = early[n]
    factors = factored(gram)
    for_rhs = unpacked(take(1), depth + 1)
    rhs, newest_sq = for_rhs[:depth], for_rhs[depth]
    gamma = solved(factors, rhs)
    receive(3)
    wide_gamma = [jnp.concatenate([g, g], 0) for g in gamma]
    for c in range(3):
        for x in range(cells_x + 2 * HALO):
            cut = cells_y if x in (0, cells_x + 2 * HALO - 1) else rows
            value = late[c, x, 0:cut]
            for j in range(depth):
                value = value - wide_gamma[j][0:cut] * hist[j, c, x, 0:cut]
            ahead[c, x, 0:cut] = value

    def store_out(c, x, value):
        out_ref[c, x] = value

    picard(ahead, store_out)

    sums = [None] * depth
    for c, x in own:
        resid = out_ref[c, x] - ahead[c, x + HALO, 0:cells_y]
        res_ref[c, x] = resid
        for j in range(1, depth):
            add(j - 1, fres[j, c, x] * resid)
        add(depth - 1, delta[c, x] * resid)
    give(2, packed(sums))

    gram2 = [[None] * depth for _ in range(depth)]
    for i in range(depth - 1):
        for j in range(depth - 1):
            gram2[i][j] = gram[i + 1][j + 1]
        cross = rhs[i + 1] - early[len(pairs) + i + 1]
        gram2[i][depth - 1] = gram2[depth - 1][i] = cross
    gram2[depth - 1][depth - 1] = newest_sq
    factors = factored(gram2)

    halfway(2)
    pieces = [piece for _, group in fields.values() for piece in group]
    settle(pieces, send_sem, True, 3 * (count_all - 1) if direct else 0)
    if not direct:
        for line in lines:
            for idx in range(3):
                whole(line, idx).wait_send()
    final = take(2)
    gamma = solved(factors, unpacked(final, depth))
    for c, x in own:
        value = out_ref[c, x]
        newest = late[c, x + HALO, 0:cells_y] - past_val[c, x]
        for j in range(1, depth):
            value = value - gamma[j - 1] * hist[j, c, x + HALO, 0:cells_y]
        out_ref[c, x] = value - gamma[depth - 1] * newest


def leave(vel_ref, res_ref, vel_hbm, res_hbm, sem):
    copies = [
        pltpu.make_async_copy(vel_ref, vel_hbm, sem.at[0]),
        pltpu.make_async_copy(res_ref, res_hbm, sem.at[1]),
    ]
    for copy in copies:
        copy.start()
    for copy in copies:
        copy.wait()


def local(velocity, forcing, viscosity, residual_prev, value_prev, hist_res, hist_val):
    depth, comps, cells_x, cells_y, lanes = hist_res.shape
    counts = (lax.axis_size("gx"), lax.axis_size("gy"))
    entries = 3.0 * cells_x * cells_y * lanes * counts[0] * counts[1]
    rows = 2 * cells_y
    count_all = counts[0] * counts[1]
    direct = count_all <= 64
    def vmem(*shape):
        return pltpu.VMEM(shape + (lanes,), jnp.float32)

    if direct:
        shared = [vmem(3, count_all, 1), pltpu.SemaphoreType.DMA((3,))]
    else:
        shared = [vmem(3, counts[1], 1), vmem(3, counts[0], 1)]
        shared += [pltpu.SemaphoreType.DMA((3,))] * 4
    length = 9 * (depth + 3) * (6 * (cells_x + cells_y) + 16) + 3 * count_all
    results = pl.pallas_call(
        functools.partial(kernel, counts, direct, entries),
        name="anderson",
        out_shape=(pltpu.VMEM(velocity.shape, jnp.float32),) * 2,
        in_specs=[pl.BlockSpec(memory_space=pl.ANY)] * 7,
        out_specs=(pl.BlockSpec(memory_space=pltpu.VMEM),) * 2,
        scratch_shapes=[
            vmem(3, cells_x + 6, rows),
            vmem(4, cells_x + 4, rows),
            vmem(depth, 3, cells_x + 6, rows),
            vmem(3, cells_x + 6, rows),
            vmem(3, cells_x + 6, rows),
            vmem(3, cells_x, cells_y),
            vmem(3, cells_x, cells_y),
            vmem(9, cells_x + 4, rows),
            vmem(3, cells_x + 4, rows),
            vmem(3, cells_x + 2, rows),
            vmem(depth, 3, cells_x, cells_y),
            vmem(3, cells_x, cells_y),
            vmem(depth, 3, cells_x, HALO),
            vmem(length, 1),
            pltpu.SemaphoreType.DMA((3,)),
            pltpu.SemaphoreType.DMA,
            pltpu.SemaphoreType.DMA((7,)),
            pltpu.SemaphoreType.REGULAR,
            *shared,
        ],
        compiler_params=pltpu.CompilerParams(collective_id=0, has_side_effects=True),
    )(velocity, forcing, viscosity, residual_prev, value_prev, hist_res, hist_val)
    return pl.pallas_call(
        leave,
        name="leave",
        out_shape=(jax.ShapeDtypeStruct(velocity.shape, jnp.float32),) * 2,
        in_specs=[pl.BlockSpec(memory_space=pl.ANY)] * 2,
        out_specs=(pl.BlockSpec(memory_space=pl.ANY),) * 2,
        scratch_shapes=[pltpu.SemaphoreType.DMA((2,))],
    )(*(pltpu.with_memory_space_constraint(r, pltpu.VMEM) for r in results))


def solution(mesh):
    field = P(None, "gx", "gy", None)
    history = P(None, None, "gx", "gy", None)
    return jax.shard_map(
        local,
        mesh=mesh,
        in_specs=(field, field, P("gx", "gy", None), field, field, history, history),
        out_specs=(field, field),
        check_vma=False,
    )
```

```python
import functools

import jax
import jax.numpy as jnp
from jax import lax
from jax.experimental import pallas as pl
from jax.experimental.pallas import tpu as pltpu
from jax.sharding import PartitionSpec as P

SWEEPS = 3
REG = 0.05
FLOOR = 0.001
MESH = pl.DeviceIdType.MESH
DIRS = ((-1, 0), (1, 0), (0, -1), (0, 1), (-1, -1), (-1, 1), (1, -1), (1, 1))
HALO = SWEEPS


def both(a, b):
    return jnp.logical_and(a, b)


def kernel(
    counts,
    direct,
    entries,
    vel_hbm, forc_hbm, visc_hbm, rp_hbm, gp_hbm, hres_hbm, hval_hbm,
    out_ref, res_ref,
    wide, static, hist, late, ahead, past_res, past_val, coef, first, second, fres, delta,
    passing, ruler, in_sem, send_sem, recv_sem, gate, *shared,
):
    depth, _, cells_x, cells_y, lanes = hres_hbm.shape
    count_x, count_y = counts
    me_x, me_y = lax.axis_index("gx"), lax.axis_index("gy")
    rows = 2 * cells_y

    def exists(sx, sy):
        ok = None
        for step, me, count in ((sx, me_x, count_x), (sy, me_y, count_y)):
            if step != 0:
                here = me > 0 if step < 0 else me < count - 1
                ok = here if ok is None else both(ok, here)
        return ok

    loads = [
        pltpu.make_async_copy(vel_hbm, wide.at[:, HALO : HALO + cells_x, 0:cells_y], in_sem.at[0]),
        pltpu.make_async_copy(forc_hbm, static.at[0:3, 2 : 2 + cells_x, 0:cells_y], in_sem.at[0]),
        pltpu.make_async_copy(visc_hbm, static.at[3, 2 : 2 + cells_x, 0:cells_y], in_sem.at[0]),
        pltpu.make_async_copy(hval_hbm, hist.at[:, :, HALO : HALO + cells_x, 0:cells_y], in_sem.at[1]),
        pltpu.make_async_copy(hres_hbm, fres, in_sem.at[2]),
        pltpu.make_async_copy(rp_hbm, past_res, in_sem.at[2]),
        pltpu.make_async_copy(gp_hbm, past_val, in_sem.at[2]),
    ]
    for load in loads[:4]:
        load.start()
    barrier = pltpu.get_barrier_semaphore()
    for k in range(1, count_y):
        pl.semaphore_signal(
            barrier, inc=1, device_id=(me_x, lax.rem(me_y + k, count_y)), device_id_type=MESH
        )
    for k in range(2, count_x):

        @pl.when(me_x + k < count_x)
        def _():
            pl.semaphore_signal(barrier, inc=1, device_id=(me_x + k, me_y), device_id_type=MESH)

    total = count_y - 1 + jnp.maximum(me_x - 1, 0)
    for sx, sy in DIRS[:2] + DIRS[4:]:
        here = exists(sx, sy)
        total = total + jnp.where(here, 1, 0)

        @pl.when(here)
        def _():
            pl.semaphore_signal(
                barrier, inc=1, device_id=(me_x + sx, me_y + sy), device_id_type=MESH
            )

    def clear(ref, off):
        lead = (slice(None),) * (len(ref.shape) - 3)
        for (sx, sy), part in (
            ((-1, 0), (slice(0, off), slice(None))),
            ((1, 0), (slice(off + cells_x, 2 * off + cells_x), slice(None))),
            ((0, -1), (slice(None), slice(rows - off, rows))),
            ((0, 1), (slice(None), slice(cells_y, cells_y + off))),
        ):

            @pl.when(jnp.logical_not(exists(sx, sy)))
            def _():
                where = lead + part
                ref[where] = jnp.zeros(ref.at[where].shape, jnp.float32)

    clear(wide, HALO)
    clear(static, HALO - 1)
    with jax.named_scope("barrier"):
        pl.semaphore_wait(barrier, total)

    def span_x(sx, off, deep, skip=0):
        if sx == 0:
            return (slice(off, off + cells_x),) * 2
        if sx < 0:
            return slice(off + skip, off + deep), slice(off + cells_x + skip, off + cells_x + deep)
        return slice(off + cells_x - deep, off + cells_x - skip), slice(off - deep, off - skip)

    def span_y(sy, deep, skip=0):
        if sy == 0:
            return (slice(0, cells_y),) * 2
        if sy < 0:
            return slice(skip, deep), slice(cells_y + skip, cells_y + deep)
        return slice(cells_y - deep, cells_y - skip), slice(rows - deep, rows - skip)

    def faces(ref, off, dirs):
        pieces = []
        for sx, sy in dirs:
            if sx == 0 or sy == 0:
                pieces.append((ref, (sx, sy), 0, span_x(sx, off, off), span_y(sy, off)))
            for deep in range(1, off) if sx != 0 and sy != 0 else ():
                at_x, at_y = span_x(sx, off, deep, deep - 1), span_y(sy, off - deep)
                pieces.append((ref, (sx, sy), 0, at_x, at_y))
        return pieces

    def layer(ref, off, deep, skip, sy):
        return [(ref, (0, sy), 0, span_x(0, off, 0), span_y(sy, deep, skip))]

    def corners(ref, off, side):
        deep = off - 1
        part = slice(cells_y, cells_y + deep) if side > 0 else slice(rows - deep, rows)
        return [(ref, (sx, 0), side, span_x(sx, off, deep), (part, part)) for sx in (-1, 1)]

    def length(part):
        return part.stop - part.start

    def size_of(piece):
        ref, _, _, (src_x, _), (src_y, _) = piece
        size = length(src_x) * length(src_y)
        for extent in ref.shape[:-3]:
            size = size * extent
        return size

    def places(me, count):
        if count == 1:
            return [((0, 0), None)]
        ends = [((0, 1), me == 0), ((1, 0), me == count - 1)]
        return ends + [((1, 1), both(me > 0, me < count - 1))] if count > 2 else ends

    def settle(pieces, sem, sending, more=0):
        for sides_x, here_x in places(me_x, count_x):
            for sides_y, here_y in places(me_y, count_y):
                size = more
                for piece in pieces:
                    _, (sx, sy), side, _, _ = piece
                    there = 1
                    for step, sides in ((sx, sides_x), (sy, sides_y)):
                        if step != 0:
                            there = there * sides[step > 0 if sending else step < 0]
                    if side != 0:
                        there = there * sides_y[side > 0]
                    size = size + there * size_of(piece)
                if sending and relayed and sides_y != (1, 1):
                    near, far = fields["north"][1][0], fields["far"][1][0]
                    size = size + size_of(near) * (depth - straight) // depth + size_of(far)
                if size == 0:
                    continue
                part = ruler.at[0:size]
                copy = pltpu.make_async_remote_copy(
                    src_ref=part,
                    dst_ref=part,
                    send_sem=sem,
                    recv_sem=sem,
                    device_id={"gx": lax.rem(me_x + 1, count_x)},
                    device_id_type=MESH,
                )
                here = [h for h in (here_x, here_y) if h is not None]

                @pl.when(functools.reduce(both, here))
                def _():
                    if sending:
                        copy.wait_send()
                    else:
                        copy.wait_recv()

    fields = {
        "wide": (0, faces(wide, HALO, DIRS)),
        "static": (0, faces(static, HALO - 1, DIRS)),
        "north": (1, layer(hist, HALO, HALO - 1, 0, -1)),
        "south": (2, layer(hist, HALO, HALO - 1, 0, 1)),
        "across": (3, faces(hist, HALO, DIRS[:2])),
        "far": (3, layer(hist, HALO, HALO, HALO - 1, -1) + layer(hist, HALO, HALO, HALO - 1, 1)),
        "turn_north": (3, corners(hist, HALO, 1)),
        "turn_south": (3, corners(hist, HALO, -1)),
        "late": (3, faces(late, HALO, DIRS)),
    }
    odd = lax.rem(me_y, 2) == 1
    even = jnp.logical_not(odd)

    relayed = count_y == 4
    turns = ((1, 1, 3, 2), (-1, 2, 0, 1))
    bands = {"north": (HALO - 1, 0, 1), "south": (HALO - 1, 0, 1), "far": (HALO, HALO - 1, 0)}
    straight = depth - (4 * depth) // 5

    def start(name, piece):
        which = fields[name][0]
        ref, (sx, sy), side, (src_x, dst_x), (src_y, dst_y) = piece
        here = exists(sx, sy)
        if side != 0:
            here = both(here, exists(0, side))
        lead = (slice(None),) * (len(ref.shape) - 3)

        def go(lead):
            pltpu.make_async_remote_copy(
                src_ref=ref.at[lead + (src_x, src_y)],
                dst_ref=ref.at[lead + (dst_x, dst_y)],
                send_sem=send_sem,
                recv_sem=recv_sem.at[which],
                device_id=(me_x + sx, me_y + sy),
                device_id_type=MESH,
            ).start()

        if relayed and name in bands:
            turned = me_y == (1 if sy > 0 else 2)
            if bands[name][2]:

                @pl.when(turned)
                def _():
                    go((slice(0, straight), slice(None)))

            here = both(here, jnp.logical_not(turned))

        @pl.when(here)
        def _():
            go(lead)

    middle = (straight + depth) // 2
    groups = {True: (slice(straight, middle), slice(middle, depth)), False: (slice(0, depth),)}

    def passed(name, device, sy, stage, which):
        deep, skip, part = bands[name]
        src_y, dst_y = span_y(sy, deep, skip)
        group = groups[part == 1][which]
        inside = slice(HALO, HALO + cells_x)
        kept = passing.at[group, :, :, skip:deep]
        src = hist.at[group, :, inside, src_y] if stage == 0 else kept
        dst = kept if stage < 2 else hist.at[group, :, inside, dst_y]
        return pltpu.make_async_remote_copy(
            src_ref=src,
            dst_ref=dst,
            send_sem=send_sem,
            recv_sem=recv_sem.at[fields[name][0] if stage == 2 else 4 + which if part else 6],
            device_id=device,
            device_id_type=MESH,
        )

    def detour(names):
        for name, (sy, owner, relay, _) in zip(names, turns if relayed else ()):

            @pl.when(me_y == owner)
            def _():
                for which in range(len(groups[bands[name][2] == 1])):
                    passed(name, (me_x, relay), sy, 0, which).start()

    def pass_on(names):
        for name, (sy, _, relay, target) in zip(names, turns if relayed else ()):

            @pl.when(me_y == relay)
            def _():
                for which in range(len(groups[bands[name][2] == 1])):
                    passed(name, (me_x, target), sy, 1, which).wait_recv()
                    passed(name, (me_x, target), sy, 2, which).start()

    def send(*names):
        for name in names:
            for piece in fields[name][1]:
                start(name, piece)

    def only(here):
        def run(body):
            lax.fori_loop(0, jnp.where(here, 1, 0), lambda i, c: (body(), c)[1], 0)

        return run

    def send_in_turn(*names):
        for here, first in ((odd, 1), (even, -1)):

            @only(here)
            def _():
                for sy, kinds in ((first, (1, 0)), (0, (1,)), (-first, (1, 0))):
                    for kind in kinds:
                        for name in names:
                            for piece in fields[name][1]:
                                if piece[1][1] == sy and (piece[1][0] != 0) == (kind == 1):
                                    start(name, piece)

    def receive(which):
        pieces = [p for number, group in fields.values() if number == which for p in group]
        with jax.named_scope("recv" + str(which)):
            settle(pieces, recv_sem.at[which], False)

    def turn(which, name):
        receive(which)
        send(name)

    def along(slots, idx, k, sends, recvs, me, count, axis):
        return pltpu.make_async_remote_copy(
            src_ref=slots.at[idx, me],
            dst_ref=slots.at[idx, me],
            send_sem=sends.at[idx],
            recv_sem=recvs.at[idx],
            device_id={axis: lax.rem(me + k, count)},
            device_id_type=MESH,
        )

    count_all = count_x * count_y
    me_all = me_x * count_y + me_y
    if direct:
        slots_all, all_sem = shared
    else:
        slots_y, slots_x, ysend, yrecv, xsend, xrecv = shared
        lines = (
            (slots_y, ysend, yrecv, me_y, count_y, "gy"),
            (slots_x, xsend, xrecv, me_x, count_x, "gx"),
        )

    def spread(line, idx, row):
        slots, sends, recvs, me, count, axis = line
        slots[idx, me] = row
        for k in range(1, count):
            along(slots, idx, k, sends, recvs, me, count, axis).start()

    def whole(line, idx):
        slots, sends, recvs, me, count, axis = line
        part = slots.at[idx, 0 : count - 1]
        return pltpu.make_async_remote_copy(
            src_ref=part,
            dst_ref=part,
            send_sem=sends.at[idx],
            recv_sem=recvs.at[idx],
            device_id={axis: lax.rem(me + 1, count)},
            device_id_type=MESH,
        )

    def gather(line, idx):
        slots, sends, recvs, me, count, axis = line
        whole(line, idx).wait_recv()
        total = slots[idx, 0]
        for k in range(1, count):
            total = total + slots[idx, k]
        return total

    def others(me, count, upward):
        order = []
        for k in range(count - 1):
            up = jnp.where(k >= me, k + 1, k)
            down = jnp.where(count - 1 - k <= me, count - 2 - k, count - 1 - k)
            order.append(up if upward else jnp.where(2 * me < count, down, up))
        return order

    def ranking(upward):
        far_x, far_y = others(me_x, count_x, upward), others(me_y, count_y, upward)
        ranked = [(kx + 2 * ky, x, y) for kx, x in enumerate(far_x) for ky, y in enumerate(far_y)]
        ranked += [(kx + 2 * count_y, x, me_y) for kx, x in enumerate(far_x)]
        ranked += [(count_x + 2 * ky, me_x, y) for ky, y in enumerate(far_y)]
        return [(x, y) for _, x, y in sorted(ranked, key=lambda entry: entry[0])]

    peers = [ranking(False), ranking(True)] if direct else None

    def give(idx, row):
        if not direct:
            spread(lines[1], idx, row)
            return
        slots_all[idx, me_all] = row
        for peer in peers[idx == 2]:
            pltpu.make_async_remote_copy(
                src_ref=slots_all.at[idx, me_all],
                dst_ref=slots_all.at[idx, me_all],
                send_sem=send_sem,
                recv_sem=all_sem.at[idx],
                device_id=peer,
                device_id_type=MESH,
            ).start()

    def halfway(idx):
        if not direct:
            spread(lines[0], idx, gather(lines[1], idx))

    def take(idx):
        if not direct:
            return gather(lines[0], idx)
        part = ruler.at[0 : count_all - 1]
        with jax.named_scope("take" + str(idx)):
            pltpu.make_async_remote_copy(
                src_ref=part,
                dst_ref=part,
                send_sem=all_sem.at[idx],
                recv_sem=all_sem.at[idx],
                device_id={"gx": lax.rem(me_x + 1, count_x)},
                device_id_type=MESH,
            ).wait_recv()
        return jnp.sum(slots_all[idx], axis=0)

    lane = lax.broadcasted_iota(jnp.int32, (cells_y, lanes), 1)

    def packed(parts):
        row = jnp.zeros((cells_y, lanes), jnp.float32)
        for j, part in enumerate(parts):
            row = jnp.where(lane == j, jnp.sum(part, axis=1, keepdims=True), row)
        return jnp.sum(row, axis=0, keepdims=True)

    def unpacked(row, count):
        return [jnp.broadcast_to(row[:, j : j + 1], (cells_y, lanes)) for j in range(count)]

    own = [(c, x) for c in range(3) for x in range(cells_x)]

    def factored(gram):
        trace = gram[0][0]
        for j in range(1, depth):
            trace = trace + gram[j][j]
        shift = (REG / depth) * trace + FLOOR * entries
        lower = [[None] * depth for _ in range(depth)]
        inverse = [None] * depth
        scaled = [[None] * depth for _ in range(depth)]
        for j in range(depth):
            pivot = gram[j][j] + shift
            for k in range(j):
                pivot = pivot - lower[j][k] * scaled[j][k]
            inverse[j] = 1.0 / pivot
            for i in range(j + 1, depth):
                value = gram[i][j]
                for k in range(j):
                    value = value - scaled[i][k] * lower[j][k]
                scaled[i][j] = value
                lower[i][j] = value * inverse[j]
        return lower, inverse

    def solved(factors, rhs):
        lower, inverse = factors
        part = list(rhs)
        for j in range(depth):
            for i in range(j + 1, depth):
                part[i] = part[i] - lower[i][j] * part[j]
        part = [p * inv for p, inv in zip(part, inverse)]
        for j in reversed(range(depth)):
            for i in range(j):
                part[i] = part[i] - lower[j][i] * part[j]
        return part

    zlane = lax.broadcasted_iota(jnp.int32, (rows, lanes), 1)
    has_below = jnp.where(zlane == 0, 0.0, 1.0)
    has_above = jnp.where(zlane == lanes - 1, 0.0, 1.0)

    def relax(src, dst, off, x, cut):
        cs = [coef[j, x + off][0:cut] for j in range(6)]
        for c in range(3):
            here = src(c, x)
            total = coef[6 + c, x + off][0:cut]
            total = total + cs[0] * src(c, x - 1)[0:cut] + cs[1] * src(c, x + 1)[0:cut]
            total = total + cs[2] * pltpu.roll(here, 1, 0)[0:cut]
            total = total + cs[3] * pltpu.roll(here, rows - 1, 0)[0:cut]
            total = total + cs[4] * pltpu.roll(here[0:cut], 1, 1)
            total = total + cs[5] * pltpu.roll(here[0:cut], lanes - 1, 1)
            dst(c, x, total)

    def picard(field, dst):
        for x in range(-2, cells_x + 2):
            cut = cells_y if x in (-2, cells_x + 1) else rows
            vel = [field[c, x + HALO, 0:cut] for c in range(3)]
            visc = static[3, x + 2, 0:cut]
            diag = 1.0 + 6.0 * visc + jnp.abs(vel[0]) + jnp.abs(vel[1]) + jnp.abs(vel[2])
            inv = 1.0 / diag
            for a in range(3):
                lo = (visc + jnp.maximum(vel[a], 0.0)) * inv
                hi = (visc - jnp.minimum(vel[a], 0.0)) * inv
                if a == 2:
                    lo, hi = lo * has_below[0:cut], hi * has_above[0:cut]
                coef[2 * a, x + 2, 0:cut] = lo
                coef[2 * a + 1, x + 2, 0:cut] = hi
            for c in range(3):
                coef[6 + c, x + 2, 0:cut] = (static[c, x + 2, 0:cut] + vel[c]) * inv

        def put(ref, off):
            def store(c, x, value):
                ref[c, x + off, 0 : value.shape[0]] = value

            return store

        for x in range(-2, cells_x + 2):
            cut = cells_y if x in (-2, cells_x + 1) else rows
            relax(lambda c, i: field[c, i + HALO], put(first, 2), 2, x, cut)
        for x in range(-1, cells_x + 1):
            cut = cells_y if x in (-1, cells_x) else rows
            relax(lambda c, i: first[c, i + 2], put(second, 1), 2, x, cut)
        for x in range(cells_x):
            relax(lambda c, i: second[c, i + 1], dst, 2, x, cells_y)

    def loaded(which, *refs):
        size = 0
        for ref in refs:
            part = 1
            for extent in ref.shape[:-1]:
                part = part * extent
            size = size + part
        part = ruler.at[0:size]
        pltpu.make_async_copy(part, part, in_sem.at[which]).wait()

    loaded(0, vel_hbm, forc_hbm, visc_hbm)
    send_in_turn("wide", "static")
    for load in loads[4:]:
        load.start()
    if direct:
        for k in range(1, count_x):

            @pl.when(me_x >= k)
            def _():
                pl.semaphore_signal(gate, inc=1, device_id=(me_x - k, me_y), device_id_type=MESH)

        for k in range(1, count_y):
            pl.semaphore_signal(
                gate, inc=1, device_id=(me_x, lax.rem(me_y + k, count_y)), device_id_type=MESH
            )

    loaded(1, hval_hbm)
    detour(("south", "north"))
    detour(("far", "far"))
    send_in_turn("north", "south")
    send("across")
    loaded(2, hres_hbm, rp_hbm, gp_hbm)

    pairs = [(i, j) for i in range(depth) for j in range(i + 1)]
    clear(hist, HALO)
    clear(late, HALO)
    sums = [None] * (len(pairs) + depth)

    def add(j, value):
        sums[j] = value if sums[j] is None else sums[j] + value

    for c, x in own:
        f = [fres[j, c, x] for j in range(depth)]
        r = past_res[c, x]
        for n, (i, j) in enumerate(pairs):
            add(n, f[i] * f[j])
        for j in range(depth):
            add(len(pairs) + j, f[j] * r)
    row = packed(sums)
    pass_on(("south", "north"))
    if direct:
        with jax.named_scope("gate"):
            pl.semaphore_wait(gate, count_x - 1 - me_x + count_y - 1)
    give(0, row)

    receive(0)

    def store_value(c, x, value):
        late[c, x + HALO, 0:cells_y] = value

    picard(wide, store_value)

    sums = [None] * (depth + 1)
    for c, x in own:
        resid = late[c, x + HALO, 0:cells_y] - wide[c, x + HALO, 0:cells_y]
        newest = resid - past_res[c, x]
        delta[c, x] = newest
        for j in range(depth):
            add(j, fres[j, c, x] * resid)
        add(depth, newest * newest)
    give(1, packed(sums))
    send_in_turn("far")
    send_in_turn("late")
    pass_on(("far", "far"))

    first_north = even if relayed else odd

    @only(first_north)
    def _():
        turn(1, "turn_north")
        turn(2, "turn_south")

    @only(jnp.logical_not(first_north))
    def _():
        turn(2, "turn_south")
        turn(1, "turn_north")

    halfway(0)
    halfway(1)

    early = unpacked(take(0), len(pairs) + depth)
    gram = [[None] * depth for _ in range(depth)]
    for n, (i, j) in enumerate(pairs):
        gram[i][j] = gram[j][i] = early[n]
    factors = factored(gram)
    for_rhs = unpacked(take(1), depth + 1)
    rhs, newest_sq = for_rhs[:depth], for_rhs[depth]
    gamma = solved(factors, rhs)
    receive(3)
    wide_gamma = [jnp.concatenate([g, g], 0) for g in gamma]
    for c in range(3):
        for x in range(cells_x + 2 * HALO):
            cut = cells_y if x in (0, cells_x + 2 * HALO - 1) else rows
            value = late[c, x, 0:cut]
            for j in range(depth):
                value = value - wide_gamma[j][0:cut] * hist[j, c, x, 0:cut]
            ahead[c, x, 0:cut] = value

    def store_out(c, x, value):
        out_ref[c, x] = value

    picard(ahead, store_out)

    sums = [None] * depth
    for c, x in own:
        resid = out_ref[c, x] - ahead[c, x + HALO, 0:cells_y]
        res_ref[c, x] = resid
        for j in range(1, depth):
            add(j - 1, fres[j, c, x] * resid)
        add(depth - 1, delta[c, x] * resid)
    give(2, packed(sums))

    gram2 = [[None] * depth for _ in range(depth)]
    for i in range(depth - 1):
        for j in range(depth - 1):
            gram2[i][j] = gram[i + 1][j + 1]
        cross = rhs[i + 1] - early[len(pairs) + i + 1]
        gram2[i][depth - 1] = gram2[depth - 1][i] = cross
    gram2[depth - 1][depth - 1] = newest_sq
    factors = factored(gram2)

    halfway(2)
    pieces = [piece for _, group in fields.values() for piece in group]
    settle(pieces, send_sem, True, 3 * (count_all - 1) if direct else 0)
    if not direct:
        for line in lines:
            for idx in range(3):
                whole(line, idx).wait_send()
    final = take(2)
    gamma = solved(factors, unpacked(final, depth))
    for c, x in own:
        value = out_ref[c, x]
        newest = late[c, x + HALO, 0:cells_y] - past_val[c, x]
        for j in range(1, depth):
            value = value - gamma[j - 1] * hist[j, c, x + HALO, 0:cells_y]
        out_ref[c, x] = value - gamma[depth - 1] * newest


def leave(vel_ref, res_ref, vel_hbm, res_hbm, sem):
    copies = [
        pltpu.make_async_copy(vel_ref, vel_hbm, sem.at[0]),
        pltpu.make_async_copy(res_ref, res_hbm, sem.at[1]),
    ]
    for copy in copies:
        copy.start()
    for copy in copies:
        copy.wait()


def local(velocity, forcing, viscosity, residual_prev, value_prev, hist_res, hist_val):
    depth, comps, cells_x, cells_y, lanes = hist_res.shape
    counts = (lax.axis_size("gx"), lax.axis_size("gy"))
    entries = 3.0 * cells_x * cells_y * lanes * counts[0] * counts[1]
    rows = 2 * cells_y
    count_all = counts[0] * counts[1]
    direct = count_all <= 64
    def vmem(*shape):
        return pltpu.VMEM(shape + (lanes,), jnp.float32)

    if direct:
        shared = [vmem(3, count_all, 1), pltpu.SemaphoreType.DMA((3,))]
    else:
        shared = [vmem(3, counts[1], 1), vmem(3, counts[0], 1)]
        shared += [pltpu.SemaphoreType.DMA((3,))] * 4
    length = 9 * (depth + 3) * (6 * (cells_x + cells_y) + 16) + 3 * count_all
    results = pl.pallas_call(
        functools.partial(kernel, counts, direct, entries),
        name="anderson",
        out_shape=(pltpu.VMEM(velocity.shape, jnp.float32),) * 2,
        in_specs=[pl.BlockSpec(memory_space=pl.ANY)] * 7,
        out_specs=(pl.BlockSpec(memory_space=pltpu.VMEM),) * 2,
        scratch_shapes=[
            vmem(3, cells_x + 6, rows),
            vmem(4, cells_x + 4, rows),
            vmem(depth, 3, cells_x + 6, rows),
            vmem(3, cells_x + 6, rows),
            vmem(3, cells_x + 6, rows),
            vmem(3, cells_x, cells_y),
            vmem(3, cells_x, cells_y),
            vmem(9, cells_x + 4, rows),
            vmem(3, cells_x + 4, rows),
            vmem(3, cells_x + 2, rows),
            vmem(depth, 3, cells_x, cells_y),
            vmem(3, cells_x, cells_y),
            vmem(depth, 3, cells_x, HALO),
            vmem(length, 1),
            pltpu.SemaphoreType.DMA((3,)),
            pltpu.SemaphoreType.DMA,
            pltpu.SemaphoreType.DMA((7,)),
            pltpu.SemaphoreType.REGULAR,
            *shared,
        ],
        compiler_params=pltpu.CompilerParams(collective_id=0, has_side_effects=True),
    )(velocity, forcing, viscosity, residual_prev, value_prev, hist_res, hist_val)
    return pl.pallas_call(
        leave,
        name="leave",
        out_shape=(jax.ShapeDtypeStruct(velocity.shape, jnp.float32),) * 2,
        in_specs=[pl.BlockSpec(memory_space=pl.ANY)] * 2,
        out_specs=(pl.BlockSpec(memory_space=pl.ANY),) * 2,
        scratch_shapes=[pltpu.SemaphoreType.DMA((2,))],
    )(*(pltpu.with_memory_space_constraint(r, pltpu.VMEM) for r in results))


def solution(mesh):
    field = P(None, "gx", "gy", None)
    history = P(None, None, "gx", "gy", None)
    return jax.shard_map(
        local,
        mesh=mesh,
        in_specs=(field, field, P("gx", "gy", None), field, field, history, history),
        out_specs=(field, field),
        check_vma=False,
    )
```
